32 devices in a mesh: seq: 8 (over y, x, core), fsdp: 4 (over z).
Axes of the slice: x: 2, y: 2, z: 4, core: 2. Of those that a mesh axis runs over, the one named last changes fastest.
Arguments:
- tokens: bfloat16 [4, 2048, 2048], P('fsdp', 'seq'), may hold values from -6 to 6
- layer_norm_gain: bfloat16 [2048], P(('seq', 'fsdp')), may hold values from 0.5 to 1.5
- layer_norm_bias: bfloat16 [2048], P(('seq', 'fsdp')), may hold values from -1.5 to 1.5
- qkv_weight: bfloat16 [2048, 3, 2048], P(None, None, ('seq', 'fsdp')), as said below
- qkv_bias: bfloat16 [3, 2048], P(None, ('seq', 'fsdp')), may hold values from -2.5 to 2.5
- dense_weight: bfloat16 [2048, 2048], P(('seq', 'fsdp')), may hold values from -4 to 4
- dense_bias: bfloat16 [2048], P(('seq', 'fsdp')), may hold values from -2.5 to 2.5
- fc1_weight: bfloat16 [2048, 8192], P(None, ('seq', 'fsdp')), may hold values from -0.125 to 0.125
- fc1_bias: bfloat16 [8192], P(('seq', 'fsdp')), may hold values from -2.5 to 2.5
- fc2_weight: bfloat16 [8192, 2048], P(('seq', 'fsdp')), may hold values from -0.0625 to 0.0625
- fc2_bias: bfloat16 [2048], P(('seq', 'fsdp')), may hold values from -2.5 to 2.5
- cotangent: bfloat16 [4, 2048, 2048], P('fsdp', 'seq'), may hold values from -6 to 6
Outputs:
- output: bfloat16 [4, 2048, 2048], P('fsdp', 'seq')
- tokens_grad: bfloat16 [4, 2048, 2048], P('fsdp', 'seq')
- ln_gain_grad: float32 [2048], P(('seq', 'fsdp'))
- ln_bias_grad: float32 [2048], P(('seq', 'fsdp'))
- qkv_weight_grad: float32 [2048, 3, 2048], P(None, None, ('seq', 'fsdp'))
- qkv_bias_grad: float32 [3, 2048], P(None, ('seq', 'fsdp'))
- dense_weight_grad: float32 [2048, 2048], P(('seq', 'fsdp'))
- dense_bias_grad: float32 [2048], P(('seq', 'fsdp'))
- fc1_weight_grad: float32 [2048, 8192], P(None, ('seq', 'fsdp'))
- fc1_bias_grad: float32 [8192], P(('seq', 'fsdp'))
- fc2_weight_grad: float32 [8192, 2048], P(('seq', 'fsdp'))
- fc2_bias_grad: float32 [2048], P(('seq', 'fsdp'))
The draws below stay inside these ranges and needn't reach their ends.
Inputs may be any that keep to these rules, and one draw needn't show every extreme that they name: `qkv_weight`: each entry is a projection weight no larger in magnitude than 24 times 2048 ** -0.5.
All inputs are finite; a program needn't handle non-finite values.
Results may differ from the reference program's by a relative error of at most 0.034.
The reference program's roundings to bfloat16 on the way count: a program that leaves them out, or rounds other values in their place, can miss the bound.
Values may be sent and summed in bfloat16 or wider, within the bound.
A program may use at most 192 MiB of HBM per device.

```python
import math
import jax
import jax.numpy as jnp
from jax import lax

D = 2048
HEADS = 32
ROT = 32
FF = 8192
LEN = 2048
SEQS = 4


def draw_qkv_weight(key, part):
    normal_vals = jnp.clip(jax.random.normal(key, (D, 3, D), jnp.float32), -6.0, 6.0) * D ** (-0.5)
    return normal_vals.astype(jnp.bfloat16)


def block_levels(rng, extent, split, smallest, top_value):
    level = 1.0
    for axis_at, shards_of in split:
        steps = jax.random.uniform(jax.random.fold_in(jax.random.fold_in(rng, 6), axis_at), (shards_of,), jnp.float32, smallest / len(split), top_value / len(split))
        level = level * jnp.repeat(jnp.exp(steps), extent[axis_at] // shards_of).reshape((-1,) + (1,) * (len(extent) - 1 - axis_at))
    return level


def bell_draw(own_key, dims, scale, bound, shards=(), held_as=jnp.bfloat16):
    result = scale * jax.random.normal(own_key, dims, jnp.float32)
    if shards:
        result = result * block_levels(own_key, dims, shards, -0.22, 0.18)
    return jnp.clip(result, -bound, bound).astype(held_as)


def setup_inputs(seed: int = 0) -> dict:
    key_of = jax.random.split(jax.random.key(seed), 13)
    return {
        "tokens": bell_draw(key_of[0], (SEQS, LEN, D), 1.0, 6.0, ((0, 4), (1, 8))),
        "layer_norm_gain": jnp.clip(1.0 + 0.1 * jax.random.normal(key_of[1], (D,), jnp.float32), 0.5, 1.5).astype(jnp.bfloat16),
        "layer_norm_bias": bell_draw(key_of[2], (D,), 0.3, 1.5, ((0, 32),)),
        "qkv_weight": draw_qkv_weight(jax.random.fold_in(key_of[12], 71), 0),
        "qkv_bias": bell_draw(key_of[4], (3, D), 0.5, 2.5, ((1, 32),)),
        "dense_weight": bell_draw(key_of[5], (D, D), (max(1, 2 * D // LEN)) ** -0.5, 4.0, ((0, 32),)),
        "dense_bias": bell_draw(key_of[6], (D,), 0.5, 2.5, ((0, 32),)),
        "fc1_weight": bell_draw(key_of[7], (D, FF), D ** -0.5, 0.125, ((1, 32),)),
        "fc1_bias": bell_draw(key_of[8], (FF,), 0.5, 2.5, ((0, 32),)),
        "fc2_weight": bell_draw(key_of[9], (FF, D), FF ** -0.5, 0.0625, ((0, 32),)),
        "fc2_bias": bell_draw(key_of[10], (D,), 0.5, 2.5, ((0, 32),)),
        "cotangent": bell_draw(key_of[11], (SEQS, LEN, D), 1.0, 6.0, ((0, 4), (1, 8))),
    }


EPSILON = 1e-05
GELU_C = math.sqrt(2.0 / math.pi)
BASE_LOG = math.log(10000.0)

def normalize_rows(input_rows, gain_vector, bias_vec):
    row_mean = lax.optimization_barrier(jnp.mean(input_rows, -1, keepdims=True))
    centred = input_rows - row_mean
    variance = lax.optimization_barrier(jnp.mean(centred * centred, -1, keepdims=True))
    inverse_deviation = lax.rsqrt(variance + EPSILON)
    normed = centred * inverse_deviation
    return (normed * gain_vector + bias_vec, normed, inverse_deviation)

def angle_tables(positions, rot_dims):
    half_dims = rot_dims // 2
    inverse = jnp.exp(-(jnp.arange(half_dims).astype(jnp.float32) * 2.0 / rot_dims) * BASE_LOG)
    angles = positions.astype(jnp.float32)[:, None] * inverse[None, :]
    return (jnp.cos(angles)[:, None, :], jnp.sin(angles)[:, None, :])

def rotate_heads(values, cos_tab, sin_tab, rot_dims):
    half_dims = rot_dims // 2
    first = values[..., :half_dims]
    second = values[..., half_dims:rot_dims]
    return jnp.concatenate([first * cos_tab - second * sin_tab, second * cos_tab + first * sin_tab, values[..., rot_dims:]], -1)

def unrotate_heads(grads, cos_tab, sin_tab, rot_dims):
    half_dims = rot_dims // 2
    first = grads[..., :half_dims]
    second = grads[..., half_dims:rot_dims]
    return jnp.concatenate([first * cos_tab + second * sin_tab, second * cos_tab - first * sin_tab, grads[..., rot_dims:]], -1)

def gelu_value(input_rows):
    inner = GELU_C * (input_rows + 0.044715 * input_rows * input_rows * input_rows)
    return 0.5 * input_rows * (1.0 + jnp.tanh(inner))

def gelu_slope(input_rows):
    tanh_val = jnp.tanh(GELU_C * (input_rows + 0.044715 * input_rows * input_rows * input_rows))
    return 0.5 * (1.0 + tanh_val) + 0.5 * input_rows * (1.0 - tanh_val * tanh_val) * GELU_C * (1.0 + 3.0 * 0.044715 * input_rows * input_rows)

def attend_forward(queries, key_rows, values, block_len):
    length, groups, width = queries.shape
    scaling = width ** (-0.5)
    count = length // block_len
    key_pos = jnp.arange(length)
    key_wide = key_rows.astype(jnp.float32)
    value_wide = values.astype(jnp.float32)

    def one_block(carry, block_id):
        start = block_id * block_len
        q_blk = lax.dynamic_slice_in_dim(queries, start, block_len, 0).astype(jnp.float32)
        scores = jnp.einsum('qgd,kgd->gqk', q_blk, key_wide) * scaling
        row_pos = start + jnp.arange(block_len)
        allowed = key_pos[None, :] <= row_pos[:, None]
        scores = jnp.where(allowed[None], scores, -1e+30)
        row_max = lax.optimization_barrier(jnp.max(scores, -1, keepdims=True))
        exp_terms = jnp.exp(scores - row_max)
        row_sum = lax.optimization_barrier(jnp.sum(exp_terms, -1, keepdims=True))
        probs_low = (exp_terms / row_sum).astype(jnp.bfloat16)
        out_blk = jnp.einsum('gqk,kgd->qgd', probs_low.astype(jnp.float32), value_wide).astype(jnp.bfloat16)
        return (carry, (out_blk, (row_max + jnp.log(row_sum))[..., 0]))
    _, (outs, log_sums) = lax.scan(one_block, 0, jnp.arange(count))
    return (outs.reshape(length, groups, width), jnp.transpose(log_sums, (1, 0, 2)).reshape(groups, length))

def attend_backward(queries, key_rows, values, outputs, grad_out, log_sums, block_len):
    length, groups, width = queries.shape
    scaling = width ** (-0.5)
    count = length // block_len
    key_pos = jnp.arange(length)
    key_wide = key_rows.astype(jnp.float32)
    value_wide = values.astype(jnp.float32)
    deltas = lax.optimization_barrier(jnp.sum(grad_out.astype(jnp.float32) * outputs.astype(jnp.float32), -1))

    def one_block(carry, block_id):
        grad_keys, grad_values = carry
        start = block_id * block_len
        q_blk = lax.dynamic_slice_in_dim(queries, start, block_len, 0).astype(jnp.float32)
        do_blk = lax.dynamic_slice_in_dim(grad_out, start, block_len, 0).astype(jnp.float32)
        lse_blk = lax.dynamic_slice_in_dim(log_sums, start, block_len, 1)
        delta_blk = lax.dynamic_slice_in_dim(deltas, start, block_len, 0)
        scores = jnp.einsum('qgd,kgd->gqk', q_blk, key_wide) * scaling
        row_pos = start + jnp.arange(block_len)
        allowed = key_pos[None, :] <= row_pos[:, None]
        scores = jnp.where(allowed[None], scores, -1e+30)
        probs = jnp.exp(scores - lse_blk[..., None])
        probs_low = probs.astype(jnp.bfloat16).astype(jnp.float32)
        grad_values = grad_values + jnp.einsum('gqk,qgd->kgd', probs_low, do_blk)
        grad_probs = jnp.einsum('qgd,kgd->gqk', do_blk, value_wide)
        grad_scores = probs * (grad_probs - jnp.transpose(delta_blk)[..., None]) * scaling
        grad_low = grad_scores.astype(jnp.bfloat16).astype(jnp.float32)
        grad_query = jnp.einsum('gqk,kgd->qgd', grad_low, key_wide)
        grad_keys = grad_keys + jnp.einsum('gqk,qgd->kgd', grad_low, q_blk)
        return ((grad_keys, grad_values), grad_query)
    zero_heads = jnp.zeros((length, groups, width), jnp.float32)
    (grad_keys, grad_values), grad_queries = lax.scan(one_block, (zero_heads, zero_heads), jnp.arange(count))
    return (grad_queries.reshape(length, groups, width), grad_keys, grad_values)

def one_sequence(seq_tokens, seq_cot, params):
    layer_norm_gain, layer_norm_bias, qkv_three, qkv_bias_three, dense_weight, dense_bias, fc1_weight, fc1_bias, fc2_weight, fc2_bias = params
    qkv_weight = qkv_three.reshape(D, 3 * D)
    qkv_bias = qkv_bias_three.reshape(3 * D)
    rows_all = seq_tokens.shape[0]
    head_dim = D // HEADS
    block_len = min(512, rows_all)
    input_rows = seq_tokens.astype(jnp.float32)
    normalized_rows_float, centered_normalized, inverse_deviation = normalize_rows(input_rows, layer_norm_gain.astype(jnp.float32), layer_norm_bias.astype(jnp.float32))
    normed = normalized_rows_float.astype(jnp.bfloat16)
    qkv = jnp.dot(normed, qkv_weight, preferred_element_type=jnp.float32) + qkv_bias.astype(jnp.float32)
    qkv_four = qkv.reshape(rows_all, 3, HEADS, head_dim)
    cos_tab, sin_tab = angle_tables(jnp.arange(rows_all), ROT)
    queries = rotate_heads(qkv_four[:, 0], cos_tab, sin_tab, ROT).astype(jnp.bfloat16)
    key_rows = rotate_heads(qkv_four[:, 1], cos_tab, sin_tab, ROT).astype(jnp.bfloat16)
    values = qkv_four[:, 2].astype(jnp.bfloat16)
    outputs, log_sums = attend_forward(queries, key_rows, values, block_len)
    attn_heads = outputs.reshape(rows_all, D)
    attn = jnp.dot(attn_heads, dense_weight, preferred_element_type=jnp.float32) + dense_bias.astype(jnp.float32)
    pre = jnp.dot(normed, fc1_weight, preferred_element_type=jnp.float32) + fc1_bias.astype(jnp.float32)
    act = gelu_value(pre).astype(jnp.bfloat16)
    mlp = jnp.dot(act, fc2_weight, preferred_element_type=jnp.float32) + fc2_bias.astype(jnp.float32)
    output = (input_rows + attn + mlp).astype(jnp.bfloat16)
    cotangent_expanded = seq_cot.astype(jnp.float32)
    fc2_w_grad = jnp.dot(act.T, seq_cot, preferred_element_type=jnp.float32)
    fc2_b_grad = lax.optimization_barrier(jnp.sum(cotangent_expanded, 0))
    pre_grad = jnp.dot(seq_cot, fc2_weight.T, preferred_element_type=jnp.float32) * gelu_slope(pre)
    fc1_b_grad = lax.optimization_barrier(jnp.sum(pre_grad, 0))
    pre_low = pre_grad.astype(jnp.bfloat16)
    fc1_w_grad = jnp.dot(normed.T, pre_low, preferred_element_type=jnp.float32)
    normed_grad_mlp = jnp.dot(pre_low, fc1_weight.T, preferred_element_type=jnp.float32)
    dense_w_grad = jnp.dot(attn_heads.T, seq_cot, preferred_element_type=jnp.float32)
    dense_b_grad = lax.optimization_barrier(jnp.sum(cotangent_expanded, 0))
    heads_grad = jnp.dot(seq_cot, dense_weight.T, preferred_element_type=jnp.float32).astype(jnp.bfloat16)
    grad_q, grad_k, grad_v = attend_backward(queries, key_rows, values, outputs, heads_grad.reshape(rows_all, HEADS, head_dim), log_sums, block_len)
    grad_q = unrotate_heads(grad_q.astype(jnp.bfloat16).astype(jnp.float32), cos_tab, sin_tab, ROT)
    grad_k = unrotate_heads(grad_k.astype(jnp.bfloat16).astype(jnp.float32), cos_tab, sin_tab, ROT)
    grad_v = grad_v.astype(jnp.bfloat16).astype(jnp.float32)
    qkv_grad = jnp.stack([grad_q, grad_k, grad_v], 1).reshape(rows_all, 3 * D)
    qkv_b_grad = lax.optimization_barrier(jnp.sum(qkv_grad, 0))
    qkv_low = qkv_grad.astype(jnp.bfloat16)
    qkv_w_grad = jnp.dot(normed.T, qkv_low, preferred_element_type=jnp.float32)
    normalized_gradient = jnp.dot(qkv_low, qkv_weight.T, preferred_element_type=jnp.float32) + normed_grad_mlp
    gain_gradient = lax.optimization_barrier(jnp.sum(normalized_gradient * centered_normalized, 0))
    shift_grad = lax.optimization_barrier(jnp.sum(normalized_gradient, 0))
    scaled_rows = normalized_gradient * layer_norm_gain.astype(jnp.float32)
    inner_gradient = inverse_deviation * (scaled_rows - lax.optimization_barrier(jnp.mean(scaled_rows, -1, keepdims=True)) - centered_normalized * lax.optimization_barrier(jnp.mean(scaled_rows * centered_normalized, -1, keepdims=True)))
    tokens_grad = (cotangent_expanded + inner_gradient).astype(jnp.bfloat16)
    grads = (gain_gradient, shift_grad, qkv_w_grad.reshape(D, 3, D), qkv_b_grad.reshape(3, D), dense_w_grad, dense_b_grad, fc1_w_grad, fc1_b_grad, fc2_w_grad, fc2_b_grad)
    return (output, tokens_grad, grads)

def reference(tokens, layer_norm_gain, layer_norm_bias, qkv_weight, qkv_bias, dense_weight, dense_bias, fc1_weight, fc1_bias, fc2_weight, fc2_bias, cotangent):
    params = (layer_norm_gain, layer_norm_bias, qkv_weight, qkv_bias, dense_weight, dense_bias, fc1_weight, fc1_bias, fc2_weight, fc2_bias)
    zero_grads = tuple((jnp.zeros(item.shape, jnp.float32) for item in params))

    def step_seq(carry, pair):
        output, tokens_grad, grads = one_sequence(pair[0], pair[1], params)
        return (tuple((left + right for left, right in zip(carry, grads))), (output, tokens_grad))
    totals, (outputs, token_grads) = lax.scan(step_seq, zero_grads, (tokens, cotangent))
    return (outputs, token_grads, totals[0], totals[1], totals[2], totals[3], totals[4], totals[5], totals[6], totals[7], totals[8], totals[9])
```

```python
import functools
import math

import jax
import jax.numpy as jnp
from jax import lax
from jax.experimental import pallas as pl
from jax.experimental.pallas import tpu as pltpu
from jax.sharding import PartitionSpec as P

HEADS = 32
ROT = 32
EPSILON = 1e-05
GELU_C = math.sqrt(2.0 / math.pi)
BASE_LOG = math.log(10000.0)
F32 = jnp.float32
BF16 = jnp.bfloat16


def dot_nn(left, right):
    return lax.dot_general(left, right, (((1,), (0,)), ((), ())), preferred_element_type=F32)


def dot_nt(left, right):
    return lax.dot_general(left, right, (((1,), (1,)), ((), ())), preferred_element_type=F32)


def dot_tn(left, right):
    return lax.dot_general(left, right, (((0,), (0,)), ((), ())), preferred_element_type=F32)


def gelu_pair(pre):
    t = jnp.tanh(GELU_C * (pre + 0.044715 * pre * pre * pre))
    value = 0.5 * pre * (1.0 + t)
    slope = 0.5 * (1.0 + t) + 0.5 * pre * (1.0 - t * t) * GELU_C * (1.0 + 3.0 * 0.044715 * pre * pre)
    return value, slope


def xor_perm(size, mask):
    return [(i, i ^ mask) for i in range(size)]


def swap(x, axis, mask):
    return lax.ppermute(x, axis, xor_perm(lax.axis_size(axis), mask))


def bit_orders(ways):
    upper = list(range(1, ways.bit_length() - 1))
    last = [0] if ways > 1 else []
    return upper + last, upper[::-1] + last


def masks_of(order):
    masks = [0]
    for b in order:
        masks = masks + [m ^ (1 << b) for m in masks]
    return masks


def gather_half(x, order):
    parts = [x]
    for b in order:
        parts = parts + [swap(p, "seq", 1 << b) for p in parts]
    return parts


def scatter_half(x, order):
    for at, b in enumerate(reversed(order)):
        n = x.shape[0] // 2
        total = x[:n].astype(F32) + swap(x[n:], "seq", 1 << b).astype(F32)
        x = total if at == len(order) - 1 else total.astype(BF16)
    return x


def gather_small(x):
    for axis in ("fsdp", "seq"):
        ways = lax.axis_size(axis)
        place = lax.axis_index(axis)
        for b in range(ways.bit_length() - 1):
            other = swap(x, axis, 1 << b)
            mine_high = (place >> b) & 1
            x = jnp.where(mine_high == 1, jnp.concatenate([other, x], 1), jnp.concatenate([x, other], 1))
    return x


def scatter_small(x):
    for axis in ("seq", "fsdp"):
        ways = lax.axis_size(axis)
        place = lax.axis_index(axis)
        for b in reversed(range(ways.bit_length() - 1)):
            n = x.shape[1] // 2
            mine_high = (place >> b) & 1
            keep = jnp.where(mine_high == 1, x[:, n:], x[:, :n])
            send = jnp.where(mine_high == 1, x[:, :n], x[:, n:])
            x = keep + swap(send, axis, 1 << b)
    return x


def group_gather(x, dim, half):
    return [x] + [swap(x, "fsdp", k) for k in range(1, half)]


def ordered(parts, dim, half, relative):
    if relative:
        return jnp.concatenate(parts, dim)
    place = lax.rem(lax.axis_index("fsdp"), half)
    stacked = jnp.stack(parts, 0)[jnp.arange(half) ^ place]
    return jnp.concatenate([stacked[k] for k in range(half)], dim)


def group_scatter(x, dim, half, relative):
    n = x.shape[dim] // half
    pieces = [lax.slice_in_dim(x, k * n, (k + 1) * n, axis=dim) for k in range(half)]
    if not relative:
        place = lax.rem(lax.axis_index("fsdp"), half)
        stacked = jnp.stack(pieces, 0)[jnp.arange(half) ^ place]
        pieces = [stacked[k] for k in range(half)]
    total = pieces[0]
    for k in range(1, half):
        total = total + swap(pieces[k].astype(BF16), "fsdp", k).astype(F32)
    return total


def rotation_tables(length, head_dim, heads):
    half = ROT // 2
    inverse = jnp.exp(-(jnp.arange(half).astype(F32) * 2.0 / ROT) * BASE_LOG)
    angles = jnp.arange(length).astype(F32)[:, None] * inverse[None, :]
    cos, sin = jnp.cos(angles), jnp.sin(angles)
    zero = jnp.zeros_like(sin)
    rest = jnp.zeros((length, head_dim - ROT), F32)
    one_head = (
        jnp.concatenate([cos, cos, rest + 1.0], 1),
        jnp.concatenate([-sin, zero, rest], 1),
        jnp.concatenate([zero, sin, rest], 1),
    )
    return tuple(jnp.tile(t, (1, heads)) for t in one_head)


def attention_kernel(
    heads, head_dim, block, chunks, chunk,
    place, q_in, k_in, v_in, g_in, cos_ref, neg_ref, pos_ref,
    o_out, dq_out, dk_out, dv_out, bias_out,
    stage, q, k, v, g, kt, vt, gt, dk, dv, dq, o, scores, in_sem, out_sem,
):
    length, width = q.shape
    half = ROT // 2
    scale = head_dim ** (-0.5)
    count = length // block
    loads = []
    for r in range(chunks):
        rows = pl.ds(pl.multiple_of(place[r] * chunk, chunk), chunk)
        for n, src in enumerate((q_in, k_in, v_in)):
            loads.append(pltpu.make_async_copy(src.at[pl.ds(r * chunk, chunk), :], stage.at[n, rows, :], in_sem.at[r, n]))
        loads.append(pltpu.make_async_copy(g_in.at[pl.ds(r * chunk, chunk), :], g.at[rows, :], in_sem.at[r, 3]))
    for c in loads:
        c.start()
    for c in loads:
        c.wait()

    def prepare(at, _):
        rows = pl.ds(pl.multiple_of(at * block, block), block)
        cos, neg, pos = cos_ref[rows, :], neg_ref[rows, :], pos_ref[rows, :]

        def rotate(x):
            return x * cos + pltpu.roll(x, width - half, 1) * neg + pltpu.roll(x, half, 1) * pos

        q[rows, :] = rotate(stage[0, rows, :]).astype(BF16) * scale
        kb = rotate(stage[1, rows, :]).astype(BF16)
        vb = stage[2, rows, :].astype(BF16)
        k[rows, :] = kb
        v[rows, :] = vb
        kt[:, rows] = kb.T
        vt[:, rows] = vb.T
        gt[:, rows] = g[rows, :].T
        dk[rows, :] = jnp.zeros((block, width), F32)
        dv[rows, :] = jnp.zeros((block, width), F32)
        return 0

    lax.fori_loop(0, count, prepare, 0)
    lane = lax.broadcasted_iota(jnp.int32, (block, width), 1)

    def only(x, h):
        if heads == 1:
            return x
        keep = (lane >= h * head_dim) & (lane < (h + 1) * head_dim)
        return jnp.where(keep, x.astype(F32), 0.0).astype(BF16)

    def one_block(i, _):
        mine = pl.ds(pl.multiple_of(i * block, block), block)
        qi, gi = q[mine, :], g[mine, :]
        ob = jnp.zeros((width, block), F32)
        dqb = jnp.zeros((width, block), F32)
        row = lax.broadcasted_iota(jnp.int32, (width, block), 0)
        for h in range(heads):
            qh, gh = only(qi, h), only(gi, h)

            def first(j, top):
                cols = pl.ds(pl.multiple_of(j * block, block), block)
                s = dot_nt(k[cols, :], qh)
                scores[cols, :] = s
                return jnp.maximum(top, jnp.max(s, 0, keepdims=True))

            top = lax.fori_loop(0, i, first, jnp.full((1, block), -1e30, F32))
            s = dot_nt(k[mine, :], qh)
            key_at = lax.broadcasted_iota(jnp.int32, (block, block), 0)
            query_at = lax.broadcasted_iota(jnp.int32, (block, block), 1)
            s = jnp.where(key_at <= query_at, s, -1e30)
            scores[mine, :] = s
            top = jnp.maximum(top, jnp.max(s, 0, keepdims=True))

            def second(j, carry):
                total, acc = carry
                cols = pl.ds(pl.multiple_of(j * block, block), block)
                e = jnp.exp(scores[cols, :] - top)
                scores[cols, :] = e
                return total + jnp.sum(e, 0, keepdims=True), acc + dot_nn(vt[:, cols], e.astype(BF16))

            total, acc = lax.fori_loop(
                0, i + 1, second, (jnp.zeros((1, block), F32), jnp.zeros((width, block), F32))
            )
            inv = 1.0 / total
            acc = (acc * inv).astype(BF16).astype(F32)
            here = (row >= h * head_dim) & (row < (h + 1) * head_dim)
            acc = jnp.where(here, acc, 0.0)
            delta = jnp.sum(acc * gt[:, mine].astype(F32), 0, keepdims=True)
            ob = ob + acc

            def third(j, acc_q):
                cols = pl.ds(pl.multiple_of(j * block, block), block)
                p = scores[cols, :] * inv
                dv[cols, :] += dot_nn(p.astype(BF16), gh)
                dp = dot_nt(v[cols, :], gh)
                ds = (p * (dp - delta)).astype(BF16)
                dk[cols, :] += dot_nn(ds, qh)
                return acc_q + dot_nn(kt[:, cols], ds)

            acc_q = lax.fori_loop(0, i + 1, third, jnp.zeros((width, block), F32))
            dqb = dqb + jnp.where(here, acc_q, 0.0)
        o[mine, :] = ob.T.astype(BF16)
        dq[mine, :] = dqb.T * scale
        return 0

    lax.fori_loop(0, count, one_block, 0)

    def finish(at, sums):
        rows = pl.ds(pl.multiple_of(at * block, block), block)
        cos, neg, pos = cos_ref[rows, :], neg_ref[rows, :], pos_ref[rows, :]

        def unrotate(x):
            return x * cos - pltpu.roll(x, width - half, 1) * neg - pltpu.roll(x, half, 1) * pos

        a = unrotate(dq[rows, :].astype(BF16).astype(F32))
        b = unrotate(dk[rows, :].astype(BF16).astype(F32))
        c = dv[rows, :].astype(BF16).astype(F32)
        q[rows, :] = a.astype(BF16)
        k[rows, :] = b.astype(BF16)
        v[rows, :] = c.astype(BF16)
        return tuple(s + jnp.sum(x, 0, keepdims=True) for s, x in zip(sums, (a, b, c)))

    sums = lax.fori_loop(0, count, finish, tuple(jnp.zeros((1, width), F32) for _ in range(3)))
    bias_out[...] = jnp.concatenate(list(sums), 0)
    stores = []
    for r in range(chunks):
        rows = pl.ds(pl.multiple_of(place[r] * chunk, chunk), chunk)
        for n, (src, dst) in enumerate(((q, dq_out), (k, dk_out), (v, dv_out), (o, o_out))):
            stores.append(pltpu.make_async_copy(src.at[rows, :], dst.at[pl.ds(r * chunk, chunk), :], out_sem.at[r, n]))
    for c in stores:
        c.start()
    for c in stores:
        c.wait()


def attention(q, k, v, grad, tables, place, heads, head_dim):
    length, width = q.shape
    block = min(512, length)
    chunks = place.shape[0]
    chunk = length // chunks
    low = jax.ShapeDtypeStruct((length, width), BF16)
    hbm = pl.BlockSpec(memory_space=pl.ANY)
    vmem = pl.BlockSpec(memory_space=pltpu.VMEM)
    pairs = heads * length * (length + block) // 2
    return pl.pallas_call(
        functools.partial(attention_kernel, heads, head_dim, block, chunks, chunk),
        out_shape=(low, low, low, low, jax.ShapeDtypeStruct((3, width), F32)),
        in_specs=[pl.BlockSpec(memory_space=pltpu.SMEM)] + [hbm] * 4 + [vmem] * 3,
        out_specs=(hbm, hbm, hbm, hbm, vmem),
        scratch_shapes=[
            pltpu.VMEM((3, length, width), F32),
            pltpu.VMEM((length, width), BF16),
            pltpu.VMEM((length, width), BF16),
            pltpu.VMEM((length, width), BF16),
            pltpu.VMEM((length, width), BF16),
            pltpu.VMEM((width, length), BF16),
            pltpu.VMEM((width, length), BF16),
            pltpu.VMEM((width, length), BF16),
            pltpu.VMEM((length, width), F32),
            pltpu.VMEM((length, width), F32),
            pltpu.VMEM((length, width), F32),
            pltpu.VMEM((length, width), BF16),
            pltpu.VMEM((length, block), F32),
            pltpu.SemaphoreType.DMA((chunks, 4)),
            pltpu.SemaphoreType.DMA((chunks, 4)),
        ],
        compiler_params=pltpu.CompilerParams(vmem_limit_bytes=48 << 20),
        cost_estimate=pl.CostEstimate(flops=pairs * 4 * 6 * 128, bytes_accessed=length * width * 24, transcendentals=pairs),
        name="attention",
    )(place, q, k, v, grad, *tables)


def normalize(rows):
    mean = jnp.mean(rows, -1, keepdims=True)
    centred = rows - mean
    inv = lax.rsqrt(jnp.mean(centred * centred, -1, keepdims=True) + EPSILON)
    return centred * inv, inv


def local(
    tokens, layer_norm_gain, layer_norm_bias, qkv_weight, qkv_bias, dense_weight, dense_bias,
    fc1_weight, fc1_bias, fc2_weight, fc2_bias, cotangent,
):
    shape = tokens.shape
    rows, width = shape[0] * shape[1], shape[2]
    head_dim = width // HEADS
    ways = lax.axis_size("seq")
    spread = lax.axis_size("fsdp")
    half = spread // 2
    length = rows * ways
    heads = HEADS // (2 * ways)
    part = heads * head_dim
    relative = qkv_weight.shape[2] % head_dim == 0
    orders = bit_orders(ways)
    masks = [masks_of(o) for o in orders]
    me = lax.axis_index("seq")
    hb = rows // 2
    place = jnp.stack([2 * (me ^ m) + h for h in range(2) for m in masks[h]]).astype(jnp.int32)

    own = jnp.stack([tokens.reshape(rows, width), cotangent.reshape(rows, width)])
    own_halves = [own[:, :hb], own[:, hb:]]
    gathered = [[gather_half(x, o) for x, o in zip(own_halves, orders)]]
    qkv_parts = group_gather(qkv_weight, 2, half)
    fc1_parts = group_gather(fc1_weight, 1, half)
    far_halves = [swap(x, "fsdp", half) for x in own_halves]
    fc2_parts = group_gather(fc2_weight, 0, half)
    dense_parts = group_gather(dense_weight, 0, half)
    qkv_bias_parts = group_gather(qkv_bias, 1, half)
    fc1_bias_parts = group_gather(fc1_bias, 0, half)
    gathered.append([gather_half(x, o) for x, o in zip(far_halves, orders)])
    small = gather_small(jnp.stack([layer_norm_gain, layer_norm_bias, dense_bias, fc2_bias])).astype(F32)
    gain, shift = small[0], small[1]

    qkv_w = ordered(qkv_parts, 2, half, relative).reshape(width, 3 * part)
    qkv_b = ordered(qkv_bias_parts, 1, half, relative).astype(F32)
    dense_w = ordered(dense_parts, 0, half, relative)
    fc1_w = ordered(fc1_parts, 1, half, True)
    fc1_b = ordered(fc1_bias_parts, 0, half, True).astype(F32)
    fc2_w = ordered(fc2_parts, 0, half, True)
    tables = rotation_tables(length, head_dim, heads)

    outs, grads = [], []
    sums = None
    for seq in range(2):
        parts = gathered[seq][0] + gathered[seq][1]
        toks = jnp.concatenate([p[0] for p in parts], 0)
        cot = jnp.concatenate([p[1] for p in parts], 0)
        xhat_all, _ = normalize(toks.astype(F32))
        normed = (xhat_all * gain + shift).astype(BF16)
        qkv = dot_nn(normed, qkv_w)
        q, k, v = (qkv[:, n * part : (n + 1) * part] + qkv_b[n] for n in range(3))
        grad_heads = dot_nt(cot, dense_w).astype(BF16)
        heads_low, dq, dk, dv, qkv_b_sum = attention(q, k, v, grad_heads, tables, place, heads, head_dim)
        pre = dot_nn(normed, fc1_w) + fc1_b
        act, slope = gelu_pair(pre)
        act = act.astype(BF16)
        pre_grad = dot_nt(cot, fc2_w) * slope
        pre_low = pre_grad.astype(BF16)
        qkv_low = jnp.concatenate([dq, dk, dv], 1)
        out_part = (dot_nn(heads_low, dense_w) + dot_nn(act, fc2_w)).astype(BF16)
        grad_part = (dot_nt(qkv_low, qkv_w) + dot_nt(pre_low, fc1_w)).astype(BF16)
        here = (
            dot_tn(normed, qkv_low),
            qkv_b_sum,
            dot_tn(heads_low, cot),
            dot_tn(normed, pre_low),
            jnp.sum(pre_grad, 0),
            dot_tn(act, cot),
        )
        sums = here if sums is None else tuple(a + b for a, b in zip(sums, here))
        for part_rows, into in ((out_part, outs), (grad_part, grads)):
            n = part_rows.shape[0] // 2
            done = jnp.concatenate([scatter_half(x, o) for x, o in zip((part_rows[:n], part_rows[n:]), orders)], 0)
            into.append(done)

    out_far = swap(outs[1].astype(BF16), "fsdp", half).astype(F32)
    grad_far = swap(grads[1].astype(BF16), "fsdp", half).astype(F32)
    rows_f32 = tokens.reshape(rows, width).astype(F32)
    cot_f32 = cotangent.reshape(rows, width).astype(F32)
    output = (rows_f32 + outs[0] + out_far + small[2] + small[3]).astype(BF16).reshape(shape)
    normed_grad = grads[0] + grad_far
    xhat, inv = normalize(rows_f32)
    scaled = normed_grad * gain
    inner = inv * (
        scaled
        - jnp.mean(scaled, -1, keepdims=True)
        - xhat * jnp.mean(scaled * xhat, -1, keepdims=True)
    )
    tokens_grad = (cot_f32 + inner).astype(BF16).reshape(shape)
    vectors = jnp.stack([jnp.sum(normed_grad * xhat, 0), jnp.sum(normed_grad, 0), jnp.sum(cot_f32, 0)])
    vectors = scatter_small(vectors)

    qkv_w_grad = group_scatter(sums[0].reshape(width, 3, part), 2, half, relative)
    qkv_b_grad = group_scatter(sums[1], 1, half, relative)
    dense_w_grad = group_scatter(sums[2], 0, half, relative)
    fc1_w_grad = group_scatter(sums[3], 1, half, True)
    fc1_b_grad = group_scatter(sums[4], 0, half, True)
    fc2_w_grad = group_scatter(sums[5], 0, half, True)
    return (
        output, tokens_grad, vectors[0], vectors[1], qkv_w_grad, qkv_b_grad, dense_w_grad, vectors[2],
        fc1_w_grad, fc1_b_grad, fc2_w_grad, vectors[2],
    )


def solution(mesh):
    both = ("seq", "fsdp")
    rows = P("fsdp", "seq", None)
    return jax.shard_map(
        local,
        mesh=mesh,
        in_specs=(
            rows, P(both), P(both), P(None, None, both), P(None, both), P(both, None), P(both),
            P(None, both), P(both), P(both, None), P(both), rows,
        ),
        out_specs=(
            rows, rows, P(both), P(both), P(None, None, both), P(None, both), P(both, None), P(both),
            P(None, both), P(both), P(both, None), P(both),
        ),
        check_vma=False,
    )
```

```python
import functools
import math

import jax
import jax.numpy as jnp
from jax import lax
from jax.experimental import pallas as pl
from jax.experimental.pallas import tpu as pltpu
from jax.sharding import PartitionSpec as P

HEADS = 32
ROT = 32
EPSILON = 1e-05
GELU_C = math.sqrt(2.0 / math.pi)
BASE_LOG = math.log(10000.0)
F32 = jnp.float32
BF16 = jnp.bfloat16
MESH = pl.DeviceIdType.MESH


def dot_nn(left, right):
    return lax.dot_general(left, right, (((1,), (0,)), ((), ())), preferred_element_type=F32)


def dot_nt(left, right):
    return lax.dot_general(left, right, (((1,), (1,)), ((), ())), preferred_element_type=F32)


def dot_tn(left, right):
    return lax.dot_general(left, right, (((0,), (0,)), ((), ())), preferred_element_type=F32)


def gelu_pair(pre):
    t = jnp.tanh(GELU_C * (pre + 0.044715 * pre * pre * pre))
    value = 0.5 * pre * (1.0 + t)
    slope = 0.5 * (1.0 + t) + 0.5 * pre * (1.0 - t * t) * GELU_C * (1.0 + 3.0 * 0.044715 * pre * pre)
    return value, slope


def xor_perm(size, mask):
    return [(i, i ^ mask) for i in range(size)]


def swap(x, axis, mask):
    return lax.ppermute(x, axis, xor_perm(lax.axis_size(axis), mask))


def bit_orders(ways):
    upper = list(range(1, ways.bit_length() - 1))
    last = [0] if ways > 1 else []
    return upper + last, upper[::-1] + last


def masks_of(order):
    masks = [0]
    for b in order:
        masks = masks + [m ^ (1 << b) for m in masks]
    return masks


def gather_half(x, order):
    parts = [x]
    for b in order:
        parts = parts + [swap(p, "seq", 1 << b) for p in parts]
    return parts


def scatter_half(x, order):
    for at, b in enumerate(reversed(order)):
        n = x.shape[0] // 2
        total = x[:n].astype(F32) + swap(x[n:], "seq", 1 << b).astype(F32)
        x = total if at == len(order) - 1 else total.astype(BF16)
    return x


def gather_small(x):
    for axis in ("fsdp", "seq"):
        ways = lax.axis_size(axis)
        place = lax.axis_index(axis)
        for b in range(ways.bit_length() - 1):
            other = swap(x, axis, 1 << b)
            mine_high = (place >> b) & 1
            x = jnp.where(mine_high == 1, jnp.concatenate([other, x], 1), jnp.concatenate([x, other], 1))
    return x


def scatter_small(x):
    for axis in ("seq", "fsdp"):
        ways = lax.axis_size(axis)
        place = lax.axis_index(axis)
        for b in reversed(range(ways.bit_length() - 1)):
            n = x.shape[1] // 2
            mine_high = (place >> b) & 1
            keep = jnp.where(mine_high == 1, x[:, n:], x[:, :n])
            send = jnp.where(mine_high == 1, x[:, :n], x[:, n:])
            x = keep + swap(send, axis, 1 << b)
    return x


def group_gather(x, dim, half):
    return [x] + [swap(x, "fsdp", k) for k in range(1, half)]


def ordered(parts, dim, half, relative):
    if relative:
        return jnp.concatenate(parts, dim)
    place = lax.rem(lax.axis_index("fsdp"), half)
    stacked = jnp.stack(parts, 0)[jnp.arange(half) ^ place]
    return jnp.concatenate([stacked[k] for k in range(half)], dim)


def group_scatter(x, dim, half, relative):
    n = x.shape[dim] // half
    pieces = [lax.slice_in_dim(x, k * n, (k + 1) * n, axis=dim) for k in range(half)]
    if not relative:
        place = lax.rem(lax.axis_index("fsdp"), half)
        stacked = jnp.stack(pieces, 0)[jnp.arange(half) ^ place]
        pieces = [stacked[k] for k in range(half)]
    total = pieces[0]
    for k in range(1, half):
        total = total + swap(pieces[k].astype(BF16), "fsdp", k).astype(F32)
    return total


def rotation_tables(length, head_dim, heads):
    half = ROT // 2
    inverse = jnp.exp(-(jnp.arange(half).astype(F32) * 2.0 / ROT) * BASE_LOG)
    angles = jnp.arange(length).astype(F32)[:, None] * inverse[None, :]
    cos, sin = jnp.cos(angles), jnp.sin(angles)
    zero = jnp.zeros_like(sin)
    rest = jnp.zeros((length, head_dim - ROT), F32)
    one_head = (
        jnp.concatenate([cos, cos, rest + 1.0], 1),
        jnp.concatenate([-sin, zero, rest], 1),
        jnp.concatenate([zero, sin, rest], 1),
    )
    return tuple(jnp.tile(t, (1, heads)) for t in one_head)


def attention_kernel(
    heads, head_dim, block, chunks, chunk,
    seq, place, qkv_in, g_in, cos_ref, neg_ref, pos_ref,
    o_out, dqkv_out, bias_out,
    stage, q, k, v, g, kt, vt, gt, dk, dv, dq, o, scores, in_sem, out_sem,
):
    length, width = q.shape
    half = ROT // 2
    scale = head_dim ** (-0.5)
    count = length // block
    loads = []
    for r in range(chunks):
        rows = pl.ds(pl.multiple_of(place[r] * chunk, chunk), chunk)
        for n in range(3):
            src = qkv_in.at[n, seq, pl.ds(r * chunk, chunk), :]
            loads.append(pltpu.make_async_copy(src, stage.at[n, rows, :], in_sem.at[r, n]))
        loads.append(pltpu.make_async_copy(g_in.at[seq, pl.ds(r * chunk, chunk), :], g.at[rows, :], in_sem.at[r, 3]))
    for c in loads:
        c.start()
    for c in loads:
        c.wait()

    def prepare(at, _):
        rows = pl.ds(pl.multiple_of(at * block, block), block)
        cos, neg, pos = cos_ref[rows, :], neg_ref[rows, :], pos_ref[rows, :]

        def rotate(x):
            return x * cos + pltpu.roll(x, width - half, 1) * neg + pltpu.roll(x, half, 1) * pos

        q[rows, :] = rotate(stage[0, rows, :]).astype(BF16) * scale
        kb = rotate(stage[1, rows, :]).astype(BF16)
        vb = stage[2, rows, :].astype(BF16)
        k[rows, :] = kb
        v[rows, :] = vb
        kt[:, rows] = kb.T
        vt[:, rows] = vb.T
        gt[:, rows] = g[rows, :].T
        dk[rows, :] = jnp.zeros((block, width), F32)
        dv[rows, :] = jnp.zeros((block, width), F32)
        return 0

    lax.fori_loop(0, count, prepare, 0)
    lane = lax.broadcasted_iota(jnp.int32, (block, width), 1)

    def only(x, h):
        if heads == 1:
            return x
        keep = (lane >= h * head_dim) & (lane < (h + 1) * head_dim)
        return jnp.where(keep, x.astype(F32), 0.0).astype(BF16)

    def one_block(i, _):
        mine = pl.ds(pl.multiple_of(i * block, block), block)
        qi, gi = q[mine, :], g[mine, :]
        ob = jnp.zeros((width, block), F32)
        dqb = jnp.zeros((width, block), F32)
        row = lax.broadcasted_iota(jnp.int32, (width, block), 0)
        for h in range(heads):
            qh, gh = only(qi, h), only(gi, h)

            def first(j, top):
                cols = pl.ds(pl.multiple_of(j * block, block), block)
                s = dot_nt(k[cols, :], qh)
                scores[cols, :] = s
                return jnp.maximum(top, jnp.max(s, 0, keepdims=True))

            top = lax.fori_loop(0, i, first, jnp.full((1, block), -1e30, F32))
            s = dot_nt(k[mine, :], qh)
            key_at = lax.broadcasted_iota(jnp.int32, (block, block), 0)
            query_at = lax.broadcasted_iota(jnp.int32, (block, block), 1)
            s = jnp.where(key_at <= query_at, s, -1e30)
            scores[mine, :] = s
            top = jnp.maximum(top, jnp.max(s, 0, keepdims=True))

            def second(j, carry):
                total, acc = carry
                cols = pl.ds(pl.multiple_of(j * block, block), block)
                e = jnp.exp(scores[cols, :] - top)
                scores[cols, :] = e
                return total + jnp.sum(e, 0, keepdims=True), acc + dot_nn(vt[:, cols], e.astype(BF16))

            total, acc = lax.fori_loop(
                0, i + 1, second, (jnp.zeros((1, block), F32), jnp.zeros((width, block), F32))
            )
            inv = 1.0 / total
            acc = (acc * inv).astype(BF16).astype(F32)
            here = (row >= h * head_dim) & (row < (h + 1) * head_dim)
            acc = jnp.where(here, acc, 0.0)
            delta = jnp.sum(acc * gt[:, mine].astype(F32), 0, keepdims=True)
            ob = ob + acc

            def third(j, acc_q):
                cols = pl.ds(pl.multiple_of(j * block, block), block)
                p = scores[cols, :] * inv
                dv[cols, :] += dot_nn(p.astype(BF16), gh)
                dp = dot_nt(v[cols, :], gh)
                ds = (p * (dp - delta)).astype(BF16)
                dk[cols, :] += dot_nn(ds, qh)
                return acc_q + dot_nn(kt[:, cols], ds)

            acc_q = lax.fori_loop(0, i + 1, third, jnp.zeros((width, block), F32))
            dqb = dqb + jnp.where(here, acc_q, 0.0)
        o[mine, :] = ob.T.astype(BF16)
        dq[mine, :] = dqb.T * scale
        return 0

    lax.fori_loop(0, count, one_block, 0)

    def finish(at, sums):
        rows = pl.ds(pl.multiple_of(at * block, block), block)
        cos, neg, pos = cos_ref[rows, :], neg_ref[rows, :], pos_ref[rows, :]

        def unrotate(x):
            return x * cos - pltpu.roll(x, width - half, 1) * neg - pltpu.roll(x, half, 1) * pos

        a = unrotate(dq[rows, :].astype(BF16).astype(F32))
        b = unrotate(dk[rows, :].astype(BF16).astype(F32))
        c = dv[rows, :].astype(BF16).astype(F32)
        q[rows, :] = a.astype(BF16)
        k[rows, :] = b.astype(BF16)
        v[rows, :] = c.astype(BF16)
        return tuple(s + jnp.sum(x, 0, keepdims=True) for s, x in zip(sums, (a, b, c)))

    sums = lax.fori_loop(0, count, finish, tuple(jnp.zeros((1, width), F32) for _ in range(3)))
    bias_out[...] = jnp.concatenate(list(sums), 0)
    stores = []
    for r in range(chunks):
        rows = pl.ds(pl.multiple_of(place[r] * chunk, chunk), chunk)
        place_out = pl.ds(r * chunk, chunk)
        for n, src in enumerate((q, k, v)):
            stores.append(pltpu.make_async_copy(src.at[rows, :], dqkv_out.at[n, place_out, :], out_sem.at[r, n]))
        stores.append(pltpu.make_async_copy(o.at[rows, :], o_out.at[place_out, :], out_sem.at[r, 3]))
    for c in stores:
        c.start()
    for c in stores:
        c.wait()


def attention(qkv, grad, seq, tables, place, heads, head_dim):
    length, width = qkv.shape[2:]
    block = min(512, length)
    chunks = place.shape[0]
    chunk = length // chunks
    hbm = pl.BlockSpec(memory_space=pl.ANY)
    vmem = pl.BlockSpec(memory_space=pltpu.VMEM)
    pairs = heads * length * (length + block) // 2
    low = [pltpu.VMEM((length, width), BF16)] * 4 + [pltpu.VMEM((width, length), BF16)] * 3
    return pl.pallas_call(
        functools.partial(attention_kernel, heads, head_dim, block, chunks, chunk, seq),
        out_shape=(
            jax.ShapeDtypeStruct((length, width), BF16),
            jax.ShapeDtypeStruct((3, length, width), BF16),
            jax.ShapeDtypeStruct((3, width), F32),
        ),
        in_specs=[pl.BlockSpec(memory_space=pltpu.SMEM)] + [hbm] * 2 + [vmem] * 3,
        out_specs=(hbm, hbm, vmem),
        scratch_shapes=[pltpu.VMEM((3, length, width), F32)]
        + low
        + [pltpu.VMEM((length, width), F32)] * 3
        + [
            pltpu.VMEM((length, width), BF16),
            pltpu.VMEM((length, block), F32),
            pltpu.SemaphoreType.DMA((chunks, 4)),
            pltpu.SemaphoreType.DMA((chunks, 4)),
        ],
        compiler_params=pltpu.CompilerParams(vmem_limit_bytes=48 << 20),
        cost_estimate=pl.CostEstimate(flops=pairs * 4 * 6 * 128, bytes_accessed=length * width * 24, transcendentals=pairs),
        name="attention",
    )(place, qkv, grad, *tables)


def front_kernel(
    ways, spread,
    tok_own, cot_own, qkv_own, dense_own, w1_own, w2_own, gain, shift, qkv_b, w1_b,
    tok_all, cot_all, normed_all, qkv_all, g_all, ap_all, wqkv_out, dense_out, w1_out, w2_out, b1_out,
    wqkv, dense, w1, w2, xb, nb, qb, gb, apb,
    row_send, row_recv, far_send, far_recv, w_send, w_recv, w_local, load_sem, out_sem, w_out_sem,
):
    half = spread // 2
    steps = ways.bit_length() - 1
    orders = bit_orders(ways)
    hb = tok_own.shape[0] // 2
    part = dense.shape[0]
    shard = part // half
    me, f = lax.axis_index("seq"), lax.axis_index("fsdp")
    g = f % half
    base = f - g

    def near(b):
        bit = 1 << b
        return {"seq": me + bit - 2 * bit * ((me // bit) % 2)}

    far = {"fsdp": (f + half) % spread}
    peers = [{"fsdp": base + (g + k) % half} for k in range(1, half)]
    everyone = [near(b) for b in range(steps)] + [far] + peers
    barrier = pltpu.get_barrier_semaphore()
    for device in everyone:
        pl.semaphore_signal(barrier, inc=1, device_id=device, device_id_type=MESH)
    pl.semaphore_wait(barrier, len(everyone))

    own, everything = (tok_own, cot_own), (tok_all, cot_all)

    def span(h, p):
        start = (h * ways + p) * hb
        return pl.ds(start if isinstance(start, int) else pl.multiple_of(start, hb), hb)

    def source(s, a, h, p):
        if s == 0 and p == 0:
            return own[a].at[pl.ds(h * hb, hb), :]
        return everything[a].at[s, span(h, p), :]

    def row_copy(s, a, h, p, t):
        q = p + (1 << t)
        return pltpu.make_async_remote_copy(
            src_ref=source(s, a, h, p),
            dst_ref=everything[a].at[s, span(h, q), :],
            send_sem=row_send.at[s, a, h, q],
            recv_sem=row_recv.at[s, a, h, q],
            device_id=near(orders[h][t]),
            device_id_type=MESH,
        )

    def forward(s, a, h, p):
        for t in range(p.bit_length(), steps):
            row_copy(s, a, h, p, t).start()

    def arrived(s, a, h, p):
        t = p.bit_length() - 1
        row_copy(s, a, h, p - (1 << t), t).wait_recv()

    def far_copy(a, h):
        return pltpu.make_async_remote_copy(
            src_ref=source(0, a, h, 0),
            dst_ref=everything[a].at[1, span(h, 0), :],
            send_sem=far_send.at[a, h],
            recv_sem=far_recv.at[a, h],
            device_id=far,
            device_id_type=MESH,
        )

    rows_of = pl.ds(pl.multiple_of(g * shard, shard), shard)
    slabs = (
        (qkv_own, wqkv.at[:, rows_of, :]),
        (w1_own, w1.at[g]),
        (w2_own, w2.at[g]),
        (dense_own, dense.at[rows_of, :]),
    )

    def weight_copy(k, n):
        return pltpu.make_async_remote_copy(
            src_ref=slabs[n][0],
            dst_ref=slabs[n][1],
            send_sem=w_send.at[k - 1, n],
            recv_sem=w_recv.at[k - 1, n],
            device_id=peers[k - 1],
            device_id_type=MESH,
        )

    for n in range(4):
        for k in range(1, half):
            weight_copy(k, n).start()
    for a in range(2):
        for h in range(2):
            forward(0, a, h, 0)
    for a in range(2):
        for h in range(2):
            far_copy(a, h).start()
    local_w = [pltpu.make_async_copy(s, d, w_local.at[n]) for n, (s, d) in enumerate(slabs)]
    for c in local_w:
        c.start()

    order = [j for p in range(ways // 2) for j in (p, p + ways // 2)]
    total = 2 * ways

    def load(n, slot):
        s, j = n // ways, order[n % ways]
        for a in range(2):
            for h in range(2):
                pltpu.make_async_copy(
                    source(s, a, h, j), xb.at[slot, a, pl.ds(h * hb, hb), :], load_sem.at[slot, a, h]
                ).start()

    def outputs(slot, s, j):
        copies = []
        for h in range(2):
            rows, at = pl.ds(h * hb, hb), span(h, j)
            pairs = (
                (nb.at[slot, rows, :], normed_all.at[s, at, :]),
                (qb.at[slot, :, rows, :], qkv_all.at[:, s, at, :]),
                (gb.at[slot, rows, :], g_all.at[s, at, :]),
                (apb.at[slot, :, :, rows, :], ap_all.at[:, :, s, at, :]),
            )
            for n, (x, y) in enumerate(pairs):
                copies.append(pltpu.make_async_copy(x, y, out_sem.at[slot, h, n]))
        return copies

    load(0, 0)
    for p in range(1, ways // 2):
        for a in range(2):
            for h in range(2):
                arrived(0, a, h, p)
                forward(0, a, h, p)
    for c in local_w:
        c.wait()
    for n in range(4):
        for k in range(1, half):
            weight_copy(k, n).wait_recv()
    weights_out = [
        pltpu.make_async_copy(x, y, w_out_sem.at[n])
        for n, (x, y) in enumerate(((wqkv, wqkv_out), (dense, dense_out), (w1, w1_out), (w2, w2_out)))
    ]
    for c in weights_out:
        c.start()
    b1_out[...] = jnp.zeros_like(b1_out)

    def block(k, _):
        slot = k % 2
        s = k // ways
        j = (k % ways) // 2 + (k % 2) * (ways // 2)
        for a in range(2):
            @pl.when(k == (ways // 2 if a == 0 else ways - 1))
            def _():
                for h in range(2):
                    far_copy(a, h).wait_recv()
                    forward(1, a, h, 0)

        for n in range(1, total):
            @pl.when(k + 1 == n)
            def _():
                t, p = n // ways, order[n % ways]
                if p and (t or p >= ways // 2):
                    for a in range(2):
                        for h in range(2):
                            arrived(t, a, h, p)
                            forward(t, a, h, p)
                load(n, n % 2)

        for a in range(2):
            for h in range(2):
                pltpu.make_async_copy(
                    own[a].at[pl.ds(h * hb, hb), :], xb.at[slot, a, pl.ds(h * hb, hb), :], load_sem.at[slot, a, h]
                ).wait()

        @pl.when(k >= 2)
        def _():
            for c in outputs(slot, s, j):
                c.wait()

        x = xb[slot, 0].astype(F32)
        centred = x - jnp.mean(x, -1, keepdims=True)
        inv = lax.rsqrt(jnp.mean(centred * centred, -1, keepdims=True) + EPSILON)
        nb[slot] = (centred * inv * gain[...] + shift[...]).astype(BF16)
        normed = nb[slot]
        if part % 128 == 0:
            flat = dot_nt(normed, wqkv[...].reshape(3 * part, wqkv.shape[2]))
            thirds = [flat[:, n * part : (n + 1) * part] for n in range(3)]
        else:
            thirds = [dot_nt(normed, wqkv[n]) for n in range(3)]
        for n in range(3):
            qb[slot, n] = thirds[n] + qkv_b[n : n + 1, :]
        cot = xb[slot, 1]
        gb[slot] = dot_nt(cot, dense[...]).astype(BF16)
        for n in range(half):
            act, slope = gelu_pair(dot_nn(normed, w1[n]) + w1_b[n : n + 1, :])
            apb[slot, 0, n] = act.astype(BF16)
            grad = dot_nt(cot, w2[n]) * slope
            b1_out[n : n + 1, :] += jnp.sum(grad, 0, keepdims=True)
            apb[slot, 1, n] = grad.astype(BF16)
        for c in outputs(slot, s, j):
            c.start()

        @pl.when(k == 0)
        def _():
            copies = [
                pltpu.make_async_copy(
                    xb.at[0, 1, pl.ds(h * hb, hb), :], cot_all.at[0, span(h, 0), :], load_sem.at[0, 1, h]
                )
                for h in range(2)
            ]
            for c in copies:
                c.start()
            for c in copies:
                c.wait()

        return 0

    lax.fori_loop(0, total, block, 0)
    for slot in range(2):
        for c in outputs(slot, 1, order[ways - 2 + slot]):
            c.wait()
    for c in weights_out:
        c.wait()
    for n in range(4):
        for k in range(1, half):
            weight_copy(k, n).wait_send()
    for a in range(2):
        for h in range(2):
            far_copy(a, h).wait_send()
            for s in range(2):
                for p in range(ways):
                    for t in range(p.bit_length(), steps):
                        row_copy(s, a, h, p, t).wait_send()


def front(ways, spread, tok, cot, qkv_w, dense_w, w1, w2, gain, shift, qkv_b, w1_b):
    rows, width = tok.shape
    half = spread // 2
    length = rows * ways
    part = dense_w.shape[0] * half
    hidden = w1.shape[1]
    hbm = pl.BlockSpec(memory_space=pl.ANY)
    vmem = pl.BlockSpec(memory_space=pltpu.VMEM)
    shape = jax.ShapeDtypeStruct
    dma = pltpu.SemaphoreType.DMA
    return pl.pallas_call(
        functools.partial(front_kernel, ways, spread),
        out_shape=(
            shape((2, length, width), BF16),
            shape((2, length, width), BF16),
            shape((2, length, width), BF16),
            shape((3, 2, length, part), F32),
            shape((2, length, part), BF16),
            shape((2, half, 2, length, hidden), BF16),
            shape((3, part, width), BF16),
            shape((part, width), BF16),
            shape((half, width, hidden), BF16),
            shape((half, hidden, width), BF16),
            shape((half, hidden), F32),
        ),
        in_specs=[hbm] * 6 + [vmem] * 4,
        out_specs=(hbm,) * 10 + (vmem,),
        scratch_shapes=[
            pltpu.VMEM((3, part, width), BF16),
            pltpu.VMEM((part, width), BF16),
            pltpu.VMEM((half, width, hidden), BF16),
            pltpu.VMEM((half, hidden, width), BF16),
            pltpu.VMEM((2, 2, rows, width), BF16),
            pltpu.VMEM((2, rows, width), BF16),
            pltpu.VMEM((2, 3, rows, part), F32),
            pltpu.VMEM((2, rows, part), BF16),
            pltpu.VMEM((2, 2, half, rows, hidden), BF16),
            dma((2, 2, 2, ways)),
            dma((2, 2, 2, ways)),
            dma((2, 2)),
            dma((2, 2)),
            dma((max(half - 1, 1), 4)),
            dma((max(half - 1, 1), 4)),
            dma((4,)),
            dma((2, 2, 2)),
            dma((2, 2, 4)),
            dma((4,)),
        ],
        compiler_params=pltpu.CompilerParams(collective_id=1, has_side_effects=True, vmem_limit_bytes=56 << 20),
        name="front",
    )(tok, cot, qkv_w, dense_w, w1, w2, gain, shift, qkv_b, w1_b)


def back_kernel(count, o, ap, dqkv, wqkv, dense, w1, w2, *outs):
    at = pl.program_id(0)
    half = w1.shape[0]
    out = dot_nn(o[...], dense[...])
    grad = dot_nn(dqkv[0], wqkv[0])
    for n in range(1, 3):
        grad = grad + dot_nn(dqkv[n], wqkv[n])
    for n in range(half):
        out = out + dot_nn(ap[0, n, 0], w2[n])
        grad = grad + dot_nt(ap[1, n, 0], w1[n])
    out, grad = out.astype(BF16), grad.astype(BF16)
    for q in range(4):
        @pl.when(at // count == q)
        def _():
            outs[q][...] = out
            outs[4 + q][...] = grad


def back(o, ap, seq, dqkv, wqkv, dense, w1, w2):
    length, part = o.shape
    width = wqkv.shape[2]
    half, hidden = ap.shape[1], ap.shape[4]
    rows = min(256, length // 4)
    count = length // 4 // rows
    once = pl.Buffered(1)

    def group(q):
        return pl.BlockSpec((rows, width), lambda i: (jnp.clip(i - q * count, 0, count - 1), 0))

    whole = lambda x: pl.BlockSpec(x.shape, lambda i: (0,) * x.ndim, pipeline_mode=once)
    macs = length * width * (4 * part + 2 * half * hidden)
    return pl.pallas_call(
        functools.partial(back_kernel, count),
        grid=(4 * count,),
        out_shape=[jax.ShapeDtypeStruct((length // 4, width), BF16)] * 8,
        in_specs=[
            pl.BlockSpec((rows, part), lambda i: (i, 0)),
            pl.BlockSpec((2, half, 1, rows, hidden), lambda i: (0, 0, seq, i, 0)),
            pl.BlockSpec((3, rows, part), lambda i: (0, i, 0)),
            whole(wqkv), whole(dense), whole(w1), whole(w2),
        ],
        out_specs=[group(q % 4) for q in range(8)],
        compiler_params=pltpu.CompilerParams(vmem_limit_bytes=48 << 20),
        cost_estimate=pl.CostEstimate(flops=2 * macs, bytes_accessed=length * width * 6, transcendentals=0),
        name="back",
    )(o, ap, dqkv, wqkv, dense, w1, w2)


def normalize(rows):
    mean = jnp.mean(rows, -1, keepdims=True)
    centred = rows - mean
    inv = lax.rsqrt(jnp.mean(centred * centred, -1, keepdims=True) + EPSILON)
    return centred * inv, inv


def tie(*trees):
    return lax.optimization_barrier(trees)


def add_split(keep, came):
    n = keep.shape[0] // 2
    low = lambda a, b: (a.astype(F32) + b.astype(F32)).astype(BF16)
    return low(keep[:n], came[:n]), low(keep[n:], came[n:])


def local(
    tokens, layer_norm_gain, layer_norm_bias, qkv_weight, qkv_bias, dense_weight, dense_bias,
    fc1_weight, fc1_bias, fc2_weight, fc2_bias, cotangent,
):
    shape = tokens.shape
    rows, width = shape[0] * shape[1], shape[2]
    head_dim = width // HEADS
    ways = lax.axis_size("seq")
    spread = lax.axis_size("fsdp")
    half = spread // 2
    length = rows * ways
    heads = HEADS // (2 * ways)
    part = heads * head_dim
    hidden = fc1_weight.shape[1]
    orders = bit_orders(ways)
    masks = [masks_of(o) for o in orders]
    me = lax.axis_index("seq")
    group = lax.rem(lax.axis_index("fsdp"), half)
    place = jnp.stack([2 * (me ^ m) + h for h in range(2) for m in masks[h]]).astype(jnp.int32)

    small = gather_small(jnp.stack([layer_norm_gain, layer_norm_bias, dense_bias, fc2_bias])).astype(F32)
    gain, shift = small[0], small[1]

    def absolute(parts):
        stacked = jnp.stack(parts, 0)
        return stacked[jnp.arange(half) ^ group] if half > 1 else stacked

    qkv_b = absolute(group_gather(qkv_bias, 1, half)).transpose(1, 0, 2).reshape(3, part).astype(F32)
    fc1_b = absolute(group_gather(fc1_bias, 0, half)).astype(F32)
    tables = rotation_tables(length, head_dim, heads)
    tok, cot = tokens.reshape(rows, width), cotangent.reshape(rows, width)
    (
        _, cot_all, normed_all, qkv_all, g_all, ap_all, wqkv, dense, w1, w2, b1_sum,
    ) = front(
        ways, spread, tok, cot, qkv_weight.transpose(1, 2, 0), dense_weight, fc1_weight, fc2_weight,
        small[0:1], small[1:2], qkv_b, fc1_b,
    )

    def first_step(parts, n):
        return [swap(parts[4 * n + 2 * h + 1], "seq", 1 << orders[h][-1]) for h in range(2)]

    o0, dqkv0, bias0 = attention(qkv_all, g_all, 0, tables, place, heads, head_dim)
    parts0 = back(o0, ap_all, 0, dqkv0, wqkv, dense, w1, w2)
    came0 = [first_step(parts0, n) for n in range(2)]
    qkv_all, parts0 = tie(qkv_all, parts0)
    o1, dqkv1, bias1 = attention(qkv_all, g_all, 1, tables, place, heads, head_dim)
    parts1 = back(o1, ap_all, 1, dqkv1, wqkv, dense, w1, w2)
    came1 = [first_step(parts1, n) for n in range(2)]

    def finish(parts, came, n):
        done = []
        for h in range(2):
            x, keep = came[n][h], parts[4 * n + 2 * h]
            for at, b in enumerate(reversed(orders[h][:-1])):
                low, high = add_split(keep, x)
                keep, x = low, swap(high, "seq", 1 << b)
            done.append(keep.astype(F32) + x.astype(F32))
        return jnp.concatenate(done, 0)

    out0, grad0 = (finish(parts0, came0, n) for n in range(2))
    out1, grad1 = (finish(parts1, came1, n) for n in range(2))
    out_far = swap(out1.astype(BF16), "fsdp", half).astype(F32)
    grad_far = swap(grad1.astype(BF16), "fsdp", half).astype(F32)

    flat = lambda x: x.reshape(2 * length, x.shape[-1])
    normed_flat, cot_flat = flat(normed_all), flat(cot_all)
    dqkv = jnp.stack([dqkv0, dqkv1], 1).reshape(3, 2 * length, part)
    fc1_w_sum = [dot_tn(normed_flat, flat(ap_all[1, n])) for n in range(half)]
    fc2_w_sum = [dot_tn(flat(ap_all[0, n]), cot_flat) for n in range(half)]
    qkv_w_sum = [dot_tn(normed_flat, dqkv[n]) for n in range(3)]
    dense_w_sum = dot_tn(jnp.concatenate([o0, o1], 0), cot_flat)

    def returned(parts):
        pieces = jnp.stack(parts, 0)[jnp.arange(half) ^ group] if half > 1 else jnp.stack(parts, 0)
        total = pieces[0]
        for k in range(1, half):
            total = total + swap(pieces[k].astype(BF16), "fsdp", k).astype(F32)
        return total

    shard = part // half
    cut = lambda x, axis: [lax.slice_in_dim(x, n * shard, (n + 1) * shard, axis=axis) for n in range(half)]
    qkv_w_grad = returned(cut(jnp.stack(qkv_w_sum, 1), 2))
    qkv_b_grad = returned(cut(bias0 + bias1, 1))
    dense_w_grad = returned(cut(dense_w_sum, 0))
    fc1_w_grad = returned(fc1_w_sum)
    fc1_b_grad = returned([b1_sum[n] for n in range(half)])
    fc2_w_grad = returned(fc2_w_sum)

    rows_f32, cot_f32 = tok.astype(F32), cot.astype(F32)
    output = (rows_f32 + out0 + out_far + small[2] + small[3]).astype(BF16).reshape(shape)
    normed_grad = grad0 + grad_far
    xhat, inv = normalize(rows_f32)
    scaled = normed_grad * gain
    inner = inv * (
        scaled
        - jnp.mean(scaled, -1, keepdims=True)
        - xhat * jnp.mean(scaled * xhat, -1, keepdims=True)
    )
    tokens_grad = (cot_f32 + inner).astype(BF16).reshape(shape)
    vectors = jnp.stack([jnp.sum(normed_grad * xhat, 0), jnp.sum(normed_grad, 0), jnp.sum(cot_f32, 0)])
    vectors = scatter_small(vectors)
    return (
        output, tokens_grad, vectors[0], vectors[1], qkv_w_grad, qkv_b_grad, dense_w_grad, vectors[2],
        fc1_w_grad, fc1_b_grad, fc2_w_grad, vectors[2],
    )


def solution(mesh):
    both = ("seq", "fsdp")
    rows = P("fsdp", "seq", None)
    return jax.shard_map(
        local,
        mesh=mesh,
        in_specs=(
            rows, P(both), P(both), P(None, None, both), P(None, both), P(both, None), P(both),
            P(None, both), P(both), P(both, None), P(both), rows,
        ),
        out_specs=(
            rows, rows, P(both), P(both), P(None, None, both), P(None, both), P(both, None), P(both),
            P(None, both), P(both), P(both, None), P(both),
        ),
        check_vma=False,
    )
```

```python
import functools
import math

import jax
import jax.numpy as jnp
from jax import lax
from jax.experimental import pallas as pl
from jax.experimental.pallas import tpu as pltpu
from jax.sharding import PartitionSpec as P

HEADS = 32
ROT = 32
EPSILON = 1e-05
GELU_C = math.sqrt(2.0 / math.pi)
BASE_LOG = math.log(10000.0)
F32 = jnp.float32
BF16 = jnp.bfloat16
MESH = pl.DeviceIdType.MESH


def dot_nn(left, right):
    return lax.dot_general(left, right, (((1,), (0,)), ((), ())), preferred_element_type=F32)


def dot_nt(left, right):
    return lax.dot_general(left, right, (((1,), (1,)), ((), ())), preferred_element_type=F32)


def dot_tn(left, right):
    return lax.dot_general(left, right, (((0,), (0,)), ((), ())), preferred_element_type=F32)


def gelu_pair(pre):
    t = jnp.tanh(GELU_C * (pre + 0.044715 * pre * pre * pre))
    value = 0.5 * pre * (1.0 + t)
    slope = 0.5 * (1.0 + t) + 0.5 * pre * (1.0 - t * t) * GELU_C * (1.0 + 3.0 * 0.044715 * pre * pre)
    return value, slope


def xor_perm(size, mask):
    return [(i, i ^ mask) for i in range(size)]


def swap(x, axis, mask):
    return lax.ppermute(x, axis, xor_perm(lax.axis_size(axis), mask))


def bit_orders(ways):
    upper = list(range(1, ways.bit_length() - 1))
    last = [0] if ways > 1 else []
    return upper + last, upper[::-1] + last


def masks_of(order):
    masks = [0]
    for b in order:
        masks = masks + [m ^ (1 << b) for m in masks]
    return masks


def scatter_small(x):
    for axis in ("seq", "fsdp"):
        ways = lax.axis_size(axis)
        place = lax.axis_index(axis)
        for b in reversed(range(ways.bit_length() - 1)):
            n = x.shape[1] // 2
            mine_high = (place >> b) & 1
            keep = jnp.where(mine_high == 1, x[:, n:], x[:, :n])
            send = jnp.where(mine_high == 1, x[:, :n], x[:, n:])
            x = keep + swap(send, axis, 1 << b)
    return x


def rotation_tables(length, head_dim, heads):
    half = ROT // 2
    inverse = jnp.exp(-(jnp.arange(half).astype(F32) * 2.0 / ROT) * BASE_LOG)
    angles = jnp.arange(length).astype(F32)[:, None] * inverse[None, :]
    cos, sin = jnp.cos(angles), jnp.sin(angles)
    zero = jnp.zeros_like(sin)
    rest = jnp.zeros((length, head_dim - ROT), F32)
    one_head = (
        jnp.concatenate([cos, cos, rest + 1.0], 1),
        jnp.concatenate([-sin, zero, rest], 1),
        jnp.concatenate([zero, sin, rest], 1),
    )
    return tuple(jnp.tile(t, (1, heads)) for t in one_head)


def flip(place, bit):
    return place + bit - 2 * bit * ((place // bit) % 2)


class Layout:
    def __init__(self, ways, spread):
        self.ways, self.spread, self.half = ways, spread, spread // 2
        self.steps = ways.bit_length() - 1
        self.orders = bit_orders(ways)
        self.masks = [masks_of(o) for o in self.orders]
        self.me, self.f = lax.axis_index("seq"), lax.axis_index("fsdp")
        self.g = self.f % self.half
        self.base = self.f - self.g
        self.far = {"fsdp": (self.f + self.half) % spread}
        self.peer_at = [(self.g + k) % self.half for k in range(1, self.half)]
        self.peers = [{"fsdp": self.base + p} for p in self.peer_at]

    def near(self, b):
        return {"seq": flip(self.me, 1 << b)}

    def device_of(self, h, p):
        place = self.me
        for b in range(self.steps):
            if (self.masks[h][p] >> b) & 1:
                place = flip(place, 1 << b)
        return place

    def meet(self):
        everyone = [self.near(b) for b in range(self.steps)] + [self.far] + self.peers
        barrier = pltpu.get_barrier_semaphore()
        for device in everyone:
            pl.semaphore_signal(barrier, inc=1, device_id=device, device_id_type=MESH)
        pl.semaphore_wait(barrier, len(everyone))


def remote(src, dst, send, recv, device):
    return pltpu.make_async_remote_copy(
        src_ref=src, dst_ref=dst, send_sem=send, recv_sem=recv, device_id=device, device_id_type=MESH
    )


def aligned(start, size, first=0):
    if isinstance(start, int):
        return pl.ds(first + start, size)
    return pl.ds(pl.multiple_of(first + start, math.gcd(first, size)), size)


def wide(x, w, cuts):
    if all(c % 128 == 0 for c in cuts):
        y = dot_nt(x, w[...])
        return [y[:, a:b] for a, b in zip(cuts, cuts[1:])]
    return [dot_nt(x, w[a:b, :]) for a, b in zip(cuts, cuts[1:])]


def front_kernel(
    ways, spread, heads,
    tok_own, cot_own, qkv_own, w1_own, dense_own, w2_own, vectors, biases,
    tok_all, cot_all, normed_all, qkv_all, g_all, ap_all, wg_out, wo_out, b1_out, vectors_out,
    wg, wo, xb, nb, qb, gb, apb, vec, vec_in, bias_in,
    row_send, row_recv, far_send, far_recv, w_send, w_recv, w_local, load_sem, out_sem, w_out_sem,
    vec_send, vec_recv, bias_send, bias_recv,
):
    at = Layout(ways, spread)
    half, steps, orders = at.half, at.steps, at.orders
    hb = tok_own.shape[0] // 2
    shard, hidden = dense_own.shape[0], w2_own.shape[0]
    part, units = half * shard, half * hidden
    own, everything = (tok_own, cot_own), (tok_all, cot_all)
    at.meet()

    def span(h, p):
        return aligned((h * ways + p) * hb, hb)

    def source(s, a, h, p):
        if s == 0 and p == 0:
            return own[a].at[pl.ds(h * hb, hb), :]
        return everything[a].at[s, span(h, p), :]

    def row_copy(s, a, h, p, t):
        q = p + (1 << t)
        return remote(
            source(s, a, h, p), everything[a].at[s, span(h, q), :],
            row_send.at[s, a, h, q], row_recv.at[s, a, h, q], at.near(orders[h][t]),
        )

    def forward(s, a, h, p):
        for t in range(p.bit_length(), steps):
            row_copy(s, a, h, p, t).start()

    def arrived(s, a, h, p):
        t = p.bit_length() - 1
        row_copy(s, a, h, p - (1 << t), t).wait_recv()

    def relay(s, p):
        for a in range(2):
            for h in range(2):
                arrived(s, a, h, p)
                forward(s, a, h, p)

    def far_copy(a, h):
        return remote(
            source(0, a, h, 0), everything[a].at[1, span(h, 0), :], far_send.at[a, h], far_recv.at[a, h], at.far
        )

    slabs = [(qkv_own.at[n], wg.at[aligned(at.g * shard, shard, n * part), :]) for n in range(3)]
    slabs.append((w1_own, wg.at[aligned(at.g * hidden, hidden, 3 * part), :]))
    slabs.append((w2_own, wo.at[aligned(at.g * hidden, hidden, part), :]))
    slabs.append((dense_own, wo.at[aligned(at.g * shard, shard), :]))

    def weight_copy(k, n):
        return remote(slabs[n][0], slabs[n][1], w_send.at[k - 1, n], w_recv.at[k - 1, n], at.peers[k - 1])

    weight_copies = [(k, n) for n in range(6) for k in range(1, half)]

    def bias_copy(k):
        return remote(biases, bias_in.at[k - 1], bias_send.at[k - 1], bias_recv.at[k - 1], at.peers[k - 1])

    spread_bits = spread.bit_length() - 1
    partners = [{"fsdp": flip(at.f, 1 << b)} for b in range(spread_bits)] + [at.near(b) for b in range(steps)]

    def vector_copy(b):
        return remote(vec.at[b], vec_in.at[b], vec_send.at[b], vec_recv.at[b], partners[b])

    def vector_step(b):
        vector_copy(b).wait_recv()
        vec[b + 1] = vec[b] + vec_in[b]
        if b + 1 < len(partners):
            vector_copy(b + 1).start()

    for a in range(2):
        for h in range(2):
            forward(0, a, h, 0)
    vec[0] = vectors[...]
    vector_copy(0).start()
    for k in range(1, half):
        bias_copy(k).start()
    for b in range(spread_bits):
        vector_step(b)
    inner = (at.f * 4 >= spread) & (at.f * 4 < 3 * spread)

    @pl.when(jnp.logical_not(inner))
    def _():
        for a in range(2):
            for h in range(2):
                far_copy(a, h).start()

    for k, n in weight_copies:
        weight_copy(k, n).start()
    local_w = [pltpu.make_async_copy(s, d, w_local.at[n]) for n, (s, d) in enumerate(slabs)]
    for c in local_w:
        c.start()

    order = [j for p in range(ways // 2) for j in (p, p + ways // 2)]
    total = 2 * ways

    def load(n, slot):
        s, j = n // ways, order[n % ways]
        for a in range(2):
            for h in range(2):
                pltpu.make_async_copy(
                    source(s, a, h, j), xb.at[slot, a, pl.ds(h * hb, hb), :], load_sem.at[slot, a, h]
                ).start()

    def outputs(slot, s, j):
        copies = []
        for h in range(2):
            rows, to = pl.ds(h * hb, hb), span(h, j)
            pairs = (
                (nb.at[slot, rows, :], normed_all.at[s, to, :]),
                (qb.at[slot, :, rows, :], qkv_all.at[:, s, to, :]),
                (gb.at[slot, rows, :], g_all.at[s, to, :]),
                (apb.at[slot, :, rows, :], ap_all.at[:, s, to, :]),
            )
            for n, (x, y) in enumerate(pairs):
                copies.append(pltpu.make_async_copy(x, y, out_sem.at[slot, h, n]))
        return copies

    load(0, 0)
    vector_step(spread_bits)
    relay(0, 1)

    @pl.when(inner)
    def _():
        for a in range(2):
            for h in range(2):
                far_copy(a, h).wait_recv()
        for a in range(2):
            for h in range(2):
                far_copy(a, h).start()

    for p in range(2, ways // 2):
        relay(0, p)
    for b in range(spread_bits + 1, len(partners)):
        vector_step(b)
    vectors_out[...] = vec[len(partners)]

    @pl.when(jnp.logical_not(inner))
    def _():
        for a in range(2):
            for h in range(2):
                far_copy(a, h).wait_recv()

    for a in range(2):
        for h in range(2):
            forward(1, a, h, 0)
    relay(1, 1)
    for c in local_w:
        c.wait()
    for k, n in weight_copies:
        weight_copy(k, n).wait_recv()
    weights_out = [pltpu.make_async_copy(x, y, w_out_sem.at[n]) for n, (x, y) in enumerate(((wg, wg_out), (wo, wo_out)))]
    for c in weights_out:
        c.start()
    for k in range(1, half):
        bias_copy(k).wait_recv()
    bias = biases[...]
    for k in range(1, half):
        bias = bias + bias_in[k - 1]
    gain, shift = vec[len(partners), 0:1, :], vec[len(partners), 1:2, :]
    b1_out[...] = jnp.zeros_like(b1_out)

    def block(k, _):
        slot = k % 2
        s = k // ways
        j = (k % ways) // 2 + (k % 2) * (ways // 2)
        for p in range(2, ways // 2):
            @pl.when(k == 2 * p - 1)
            def _():
                relay(1, p)

        for n in range(1, total):
            @pl.when(k + 1 == n)
            def _():
                t, p = n // ways, order[n % ways]
                if p >= ways // 2:
                    for a in range(2):
                        for h in range(2):
                            arrived(t, a, h, p)
                load(n, n % 2)

        for a in range(2):
            for h in range(2):
                pltpu.make_async_copy(
                    own[a].at[pl.ds(h * hb, hb), :], xb.at[slot, a, pl.ds(h * hb, hb), :], load_sem.at[slot, a, h]
                ).wait()

        @pl.when(k >= 2)
        def _():
            for c in outputs(slot, s, j):
                c.wait()

        x = xb[slot, 0].astype(F32)
        centred = x - jnp.mean(x, -1, keepdims=True)
        inv = lax.rsqrt(jnp.mean(centred * centred, -1, keepdims=True) + EPSILON)
        nb[slot] = (centred * inv * gain + shift).astype(BF16)
        normed = nb[slot]
        q, kk, v, pre = wide(normed, wg, [0, part, 2 * part, 3 * part, 3 * part + units])
        for n, y in enumerate((q, kk, v)):
            qb[slot, n] = y + bias[n : n + 1, :part]
        grad_heads, grad = wide(xb[slot, 1], wo, [0, part, part + units])
        gb[slot] = grad_heads.astype(BF16)
        act, slope = gelu_pair(pre + bias[3:4, :units])
        apb[slot, 0] = act.astype(BF16)
        grad = grad * slope
        b1_out[...] += jnp.sum(grad, 0, keepdims=True)
        apb[slot, 1] = grad.astype(BF16)
        for c in outputs(slot, s, j):
            c.start()

        @pl.when(k == 0)
        def _():
            copies = [
                pltpu.make_async_copy(
                    xb.at[0, 1, pl.ds(h * hb, hb), :], cot_all.at[0, span(h, 0), :], load_sem.at[0, 1, h]
                )
                for h in range(2)
            ]
            for c in copies:
                c.start()
            for c in copies:
                c.wait()

        return 0

    lax.fori_loop(0, total, block, 0)
    for slot in range(2):
        for c in outputs(slot, 1, order[ways - 2 + slot]):
            c.wait()
    for c in weights_out:
        c.wait()
    for k, n in weight_copies:
        weight_copy(k, n).wait_send()
    for k in range(1, half):
        bias_copy(k).wait_send()
    for b in range(len(partners)):
        vector_copy(b).wait_send()
    for a in range(2):
        for h in range(2):
            far_copy(a, h).wait_send()
            for s in range(2):
                for p in range(ways):
                    for t in range(p.bit_length(), steps):
                        row_copy(s, a, h, p, t).wait_send()


def front(ways, spread, heads, tok, cot, qkv_w, w1, dense_w, w2, vectors, biases):
    rows, width = tok.shape
    half = spread // 2
    length = rows * ways
    part, units = dense_w.shape[0] * half, w2.shape[0] * half
    hops = (spread * ways).bit_length() - 1
    hbm = pl.BlockSpec(memory_space=pl.ANY)
    vmem = pl.BlockSpec(memory_space=pltpu.VMEM)
    shape = jax.ShapeDtypeStruct
    dma = pltpu.SemaphoreType.DMA
    return pl.pallas_call(
        functools.partial(front_kernel, ways, spread, heads),
        out_shape=(
            shape((2, length, width), BF16),
            shape((2, length, width), BF16),
            shape((2, length, width), BF16),
            shape((3, 2, length, part), F32),
            shape((2, length, part), BF16),
            shape((2, 2, length, units), BF16),
            shape((3 * part + units, width), BF16),
            shape((part + units, width), BF16),
            shape((1, units), F32),
            shape(vectors.shape, F32),
        ),
        in_specs=[hbm] * 6 + [vmem] * 2,
        out_specs=(hbm,) * 8 + (vmem,) * 2,
        scratch_shapes=[
            pltpu.VMEM((3 * part + units, width), BF16),
            pltpu.VMEM((part + units, width), BF16),
            pltpu.VMEM((2, 2, rows, width), BF16),
            pltpu.VMEM((2, rows, width), BF16),
            pltpu.VMEM((2, 3, rows, part), F32),
            pltpu.VMEM((2, rows, part), BF16),
            pltpu.VMEM((2, 2, rows, units), BF16),
            pltpu.VMEM((hops + 1,) + vectors.shape, F32),
            pltpu.VMEM((hops,) + vectors.shape, F32),
            pltpu.VMEM((max(half - 1, 1),) + biases.shape, F32),
            dma((2, 2, 2, ways)),
            dma((2, 2, 2, ways)),
            dma((2, 2)),
            dma((2, 2)),
            dma((max(half - 1, 1), 6)),
            dma((max(half - 1, 1), 6)),
            dma((6,)),
            dma((2, 2, 2)),
            dma((2, 2, 4)),
            dma((2,)),
            dma((hops,)),
            dma((hops,)),
            dma((max(half - 1, 1),)),
            dma((max(half - 1, 1),)),
        ],
        compiler_params=pltpu.CompilerParams(collective_id=1, has_side_effects=True, vmem_limit_bytes=56 << 20),
        name="front",
    )(tok, cot, qkv_w, w1, dense_w, w2, vectors, biases)


def attention_core(
    heads, head_dim, block, chunks, seq, qkv_in, g_in, cos_ref, neg_ref, pos_ref, o_out, dqkv_out, bias_out,
    stage, q, k, v, g, kt, vt, gt, dk, dv, dq, o, scores, in_sem, out_sem,
):
    length, width = q.shape
    half = ROT // 2
    scale = head_dim ** (-0.5)
    count = length // block
    chunk = length // len(chunks)
    loads = []
    for r, start in enumerate(chunks):
        rows, here = pl.ds(start, chunk), pl.ds(r * chunk, chunk)
        loads.append(pltpu.make_async_copy(qkv_in.at[:, seq, here, :], stage.at[:, rows, :], in_sem.at[r, 0]))
        loads.append(pltpu.make_async_copy(g_in.at[seq, here, :], g.at[rows, :], in_sem.at[r, 1]))
    for c in loads:
        c.start()
    for c in loads:
        c.wait()

    def prepare(at, _):
        rows = aligned(at * block, block)
        cos, neg, pos = cos_ref[rows, :], neg_ref[rows, :], pos_ref[rows, :]

        def rotate(x):
            return x * cos + pltpu.roll(x, width - half, 1) * neg + pltpu.roll(x, half, 1) * pos

        q[rows, :] = rotate(stage[0, rows, :]).astype(BF16) * scale
        kb = rotate(stage[1, rows, :]).astype(BF16)
        vb = stage[2, rows, :].astype(BF16)
        k[rows, :] = kb
        v[rows, :] = vb
        kt[:, rows] = kb.T
        vt[:, rows] = vb.T
        gt[:, rows] = g[rows, :].T
        dk[rows, :] = jnp.zeros((block, width), F32)
        dv[rows, :] = jnp.zeros((block, width), F32)
        return 0

    lax.fori_loop(0, count, prepare, 0)
    lane = lax.broadcasted_iota(jnp.int32, (block, width), 1)

    def only(x, h):
        if heads == 1:
            return x
        keep = (lane >= h * head_dim) & (lane < (h + 1) * head_dim)
        return jnp.where(keep, x.astype(F32), 0.0).astype(BF16)

    def one_block(i, _):
        mine = aligned(i * block, block)
        qi, gi = q[mine, :], g[mine, :]
        ob = jnp.zeros((width, block), F32)
        dqb = jnp.zeros((width, block), F32)
        row = lax.broadcasted_iota(jnp.int32, (width, block), 0)
        for h in range(heads):
            qh, gh = only(qi, h), only(gi, h)

            def first(j, top):
                cols = aligned(j * block, block)
                s = dot_nt(k[cols, :], qh)
                scores[cols, :] = s
                return jnp.maximum(top, jnp.max(s, 0, keepdims=True))

            top = lax.fori_loop(0, i, first, jnp.full((1, block), -1e30, F32))
            s = dot_nt(k[mine, :], qh)
            key_at = lax.broadcasted_iota(jnp.int32, (block, block), 0)
            query_at = lax.broadcasted_iota(jnp.int32, (block, block), 1)
            s = jnp.where(key_at <= query_at, s, -1e30)
            scores[mine, :] = s
            top = jnp.maximum(top, jnp.max(s, 0, keepdims=True))

            def second(j, carry):
                total, acc = carry
                cols = aligned(j * block, block)
                e = jnp.exp(scores[cols, :] - top)
                scores[cols, :] = e
                return total + jnp.sum(e, 0, keepdims=True), acc + dot_nn(vt[:, cols], e.astype(BF16))

            total, acc = lax.fori_loop(
                0, i + 1, second, (jnp.zeros((1, block), F32), jnp.zeros((width, block), F32))
            )
            inv = 1.0 / total
            acc = (acc * inv).astype(BF16).astype(F32)
            here = (row >= h * head_dim) & (row < (h + 1) * head_dim)
            acc = jnp.where(here, acc, 0.0)
            delta = jnp.sum(acc * gt[:, mine].astype(F32), 0, keepdims=True)
            ob = ob + acc

            def third(j, acc_q):
                cols = aligned(j * block, block)
                p = scores[cols, :] * inv
                dv[cols, :] += dot_nn(p.astype(BF16), gh)
                dp = dot_nt(v[cols, :], gh)
                ds = (p * (dp - delta)).astype(BF16)
                dk[cols, :] += dot_nn(ds, qh)
                return acc_q + dot_nn(kt[:, cols], ds)

            acc_q = lax.fori_loop(0, i + 1, third, jnp.zeros((width, block), F32))
            dqb = dqb + jnp.where(here, acc_q, 0.0)
        o[mine, :] = ob.T.astype(BF16)
        dq[mine, :] = dqb.T * scale
        return 0

    lax.fori_loop(0, count, one_block, 0)

    def finish(at, sums):
        rows = aligned(at * block, block)
        cos, neg, pos = cos_ref[rows, :], neg_ref[rows, :], pos_ref[rows, :]

        def unrotate(x):
            return x * cos - pltpu.roll(x, width - half, 1) * neg - pltpu.roll(x, half, 1) * pos

        a = unrotate(dq[rows, :].astype(BF16).astype(F32))
        b = unrotate(dk[rows, :].astype(BF16).astype(F32))
        c = dv[rows, :].astype(BF16).astype(F32)
        q[rows, :] = a.astype(BF16)
        k[rows, :] = b.astype(BF16)
        v[rows, :] = c.astype(BF16)
        return tuple(s + jnp.sum(x, 0, keepdims=True) for s, x in zip(sums, (a, b, c)))

    sums = lax.fori_loop(0, count, finish, tuple(jnp.zeros((1, width), F32) for _ in range(3)))
    bias_out[...] += jnp.concatenate(list(sums), 0)
    stores = []
    for r, start in enumerate(chunks):
        rows, here = pl.ds(start, chunk), pl.ds(r * chunk, chunk)
        for n, src in enumerate((q, k, v)):
            stores.append(pltpu.make_async_copy(src.at[rows, :], dqkv_out.at[n, seq, here, :], out_sem.at[r, n]))
        stores.append(pltpu.make_async_copy(o.at[rows, :], o_out.at[seq, here, :], out_sem.at[r, 3]))
    for c in stores:
        c.start()
    for c in stores:
        c.wait()


def joined(xs, w):
    if all(x.shape[1] % 128 == 0 for x in xs):
        return dot_nn(jnp.concatenate(xs, 1), w[...])
    total, at = None, 0
    for x in xs:
        y = dot_nn(x, w[at : at + x.shape[1], :])
        total, at = (y if total is None else total + y), at + x.shape[1]
    return total


def rest_kernel(
    ways, spread, heads, head_dim,
    qkv_all, g_all, ap_all, normed_all, cot_all, wg_in, wo_in, cos_ref, neg_ref, pos_ref,
    o_all, dqkv_all, recv, own_sum, far_sum, dw_own, dw_recv, bias_out,
    wg, wo, keep, stage_send, stage_recv, ob, db, apb,
    w_sem, load_sem, rs_send, rs_recv, add_sem, own_sem, far_send, far_recv, dw_send, dw_come,
):
    at = Layout(ways, spread)
    half, steps, orders = at.half, at.steps, at.orders
    hb = keep.shape[4]
    length = 2 * ways * hb
    part = g_all.shape[2]
    shard = part // half
    block = min(512, length)
    width = keep.shape[5]
    at.meet()
    loads = [pltpu.make_async_copy(x, y, w_sem.at[n]) for n, (x, y) in enumerate(((wg_in, wg), (wo_in, wo)))]
    for c in loads:
        c.start()
    bias_out[...] = jnp.zeros_like(bias_out)
    chunks = [
        pl.multiple_of((2 * at.device_of(h, p) + h) * hb, hb) for h in range(2) for p in range(ways)
    ]

    def span(h, p):
        return aligned((h * ways + p) * hb, hb)

    def attend(seq):
        f32 = [pltpu.VMEM((length, part), F32)] * 3
        low = [pltpu.VMEM((length, part), BF16)] * 4 + [pltpu.VMEM((part, length), BF16)] * 3
        pl.run_scoped(
            lambda *scratch: attention_core(
                heads, head_dim, block, chunks, seq, qkv_all, g_all, cos_ref, neg_ref, pos_ref,
                o_all, dqkv_all, bias_out, *scratch,
            ),
            pltpu.VMEM((3, length, part), F32), *low, *f32,
            pltpu.VMEM((length, part), BF16), pltpu.VMEM((length, block), F32),
            pltpu.SemaphoreType.DMA((len(chunks), 4)), pltpu.SemaphoreType.DMA((len(chunks), 4)),
        )

    def sent(s, t, h, q, src):
        level = q.bit_length() - 1 if isinstance(q, int) else steps - 1
        return remote(src, recv.at[s, t, h, q], rs_send.at[s, t, h, q], rs_recv.at[s, t, h, q], at.near(orders[h][level]))

    def partial_sums(s):
        def place(i):
            return jnp.where(i < ways // 2, ways // 2 + i, ways - 1 - i)

        def copies(i):
            slot, p = i % 2, place(i)
            out = []
            for h in range(2):
                rows = pl.ds(h * hb, hb)
                out.append(pltpu.make_async_copy(o_all.at[s, span(h, p), :], ob.at[slot, rows, :], load_sem.at[slot, h, 0]))
                out.append(pltpu.make_async_copy(dqkv_all.at[:, s, span(h, p), :], db.at[slot, :, rows, :], load_sem.at[slot, h, 1]))
                out.append(pltpu.make_async_copy(ap_all.at[:, s, span(h, p), :], apb.at[slot, :, rows, :], load_sem.at[slot, h, 2]))
            return out

        def sends(i):
            return [sent(s, t, h, place(i), stage_send.at[i % 2, t, h]) for t in range(2) for h in range(2)]

        for c in copies(0):
            c.start()

        def one(i, _):
            slot = i % 2
            for c in copies(i):
                c.wait()

            @pl.when(i + 1 < ways)
            def _():
                for c in copies(i + 1):
                    c.start()

            @pl.when((i >= 2) & (i < ways // 2 + 2))
            def _():
                for c in sends(i - 2):
                    c.wait_send()

            out = joined([ob[slot], apb[slot, 0]], wo).astype(BF16)
            grad = joined([db[slot, 0], db[slot, 1], db[slot, 2], apb[slot, 1]], wg).astype(BF16)

            @pl.when(i < ways // 2)
            def _():
                for t, x in enumerate((grad, out)):
                    for h in range(2):
                        stage_send[slot, t, h] = x[h * hb : (h + 1) * hb, :]
                for c in sends(i):
                    c.start()

            @pl.when(i >= ways // 2)
            def _():
                for t, x in enumerate((grad, out)):
                    for h in range(2):
                        keep[s, t, h, ways - 1 - i] = x[h * hb : (h + 1) * hb, :]

            return 0

        lax.fori_loop(0, ways, one, 0)

    def far_copy(t, h):
        return remote(keep.at[1, t, h, 0], far_sum.at[t, h], far_send.at[t, h], far_recv.at[t, h], at.far)

    def own_copy(t, h):
        return pltpu.make_async_copy(keep.at[0, t, h, 0], own_sum.at[t, h], own_sem.at[t, h])

    def serve(s, q):
        level = q.bit_length() - 1
        p = q - (1 << level)
        pairs = [(t, h) for t in range(2) for h in range(2)]
        come = [pltpu.make_async_copy(recv.at[s, t, h, q], stage_recv.at[t, h], add_sem.at[t, h]) for t, h in pairs]
        for (t, h), c in zip(pairs, come):
            sent(s, t, h, q, stage_recv.at[t, h]).wait_recv()
            c.start()
        for (t, h), c in zip(pairs, come):
            c.wait()
            keep[s, t, h, p] = (keep[s, t, h, p].astype(F32) + stage_recv[t, h].astype(F32)).astype(BF16)
            if p and p.bit_length() == level:
                sent(s, t, h, p, keep.at[s, t, h, p]).start()
            if q == 1:
                (own_copy if s == 0 else far_copy)(t, h).start()

    def weight_sums():
        rows = min(512, length)
        per = length // rows

        def body(nbuf, cbuf, dbuf, obuf, acc, low, sems, dw_sem):
            def copies(i):
                slot, s, here = i % 2, i // per, aligned((i % per) * rows, rows)
                return [
                    pltpu.make_async_copy(normed_all.at[s, here, :], nbuf.at[slot], sems.at[slot, 0]),
                    pltpu.make_async_copy(cot_all.at[s, here, :], cbuf.at[slot], sems.at[slot, 1]),
                    pltpu.make_async_copy(dqkv_all.at[:, s, here, :], dbuf.at[slot], sems.at[slot, 2]),
                    pltpu.make_async_copy(o_all.at[s, here, :], obuf.at[slot], sems.at[slot, 3]),
                ]

            for c in copies(0):
                c.start()
            acc[...] = jnp.zeros_like(acc)

            def one(i, _):
                slot = i % 2
                for c in copies(i):
                    c.wait()

                @pl.when(i + 1 < 2 * per)
                def _():
                    for c in copies(i + 1):
                        c.start()

                normed = nbuf[slot]
                if part % 128 == 0:
                    y = dot_tn(jnp.concatenate([dbuf[slot, n] for n in range(3)], 1), normed)
                    for n in range(3):
                        acc[n] += y[n * part : (n + 1) * part, :]
                else:
                    for n in range(3):
                        acc[n] += dot_tn(dbuf[slot, n], normed)
                acc[3] += dot_tn(obuf[slot], cbuf[slot])
                return 0

            lax.fori_loop(0, 2 * per, one, 0)
            low[...] = acc[...].astype(BF16)

            def copy(k):
                mine = aligned(at.peer_at[k - 1] * shard, shard)
                return remote(low.at[:, mine, :], dw_recv.at[k - 1], dw_send.at[k - 1], dw_come.at[k - 1], at.peers[k - 1])

            for k in range(1, half):
                copy(k).start()
            out = pltpu.make_async_copy(acc.at[:, aligned(at.g * shard, shard), :], dw_own, dw_sem)
            out.start()
            for q in range(ways // 2 - 1, 0, -1):
                serve(0, q)
            out.wait()
            for k in range(1, half):
                copy(k).wait()

        pl.run_scoped(
            body,
            pltpu.VMEM((2, rows, width), BF16), pltpu.VMEM((2, rows, width), BF16),
            pltpu.VMEM((2, 3, rows, part), BF16), pltpu.VMEM((2, rows, part), BF16),
            pltpu.VMEM((4, part, width), F32), pltpu.VMEM((4, part, width), BF16),
            pltpu.SemaphoreType.DMA((2, 4)), pltpu.SemaphoreType.DMA,
        )

    def one_sequence(turn, _):
        s = 1 - turn
        attend(s)

        @pl.when(turn == 0)
        def _():
            for c in loads:
                c.wait()

        @pl.when(turn == 1)
        def _():
            for q in range(ways // 2 - 1, 1, -1):
                serve(1, q)

        partial_sums(s)

        @pl.when(turn == 0)
        def _():
            for q in range(ways - 1, ways // 2 - 1, -1):
                serve(1, q)

        return 0

    lax.fori_loop(0, 2, one_sequence, 0)
    for q in range(ways - 1, ways // 2 - 1, -1):
        serve(0, q)
    serve(1, 1)
    weight_sums()
    for t in range(2):
        for h in range(2):
            far_copy(t, h).wait()
            own_copy(t, h).wait()
            for s in range(2):
                for p in range(1, ways // 2):
                    sent(s, t, h, p, keep.at[s, t, h, p]).wait_send()


def rest(ways, spread, heads, head_dim, qkv_all, g_all, ap_all, normed_all, cot_all, wg, wo, tables):
    _, length, width = normed_all.shape
    half = spread // 2
    part, units = g_all.shape[2], ap_all.shape[3]
    hb = length // ways // 2
    shard = part // half
    rows = 2 * hb
    hbm = pl.BlockSpec(memory_space=pl.ANY)
    vmem = pl.BlockSpec(memory_space=pltpu.VMEM)
    shape = jax.ShapeDtypeStruct
    dma = pltpu.SemaphoreType.DMA
    return pl.pallas_call(
        functools.partial(rest_kernel, ways, spread, heads, head_dim),
        out_shape=(
            shape((2, length, part), BF16),
            shape((3, 2, length, part), BF16),
            shape((2, 2, 2, ways, hb, width), BF16),
            shape((2, 2, hb, width), BF16),
            shape((2, 2, hb, width), BF16),
            shape((4, shard, width), F32),
            shape((max(half - 1, 1), 4, shard, width), BF16),
            shape((3, part), F32),
        ),
        in_specs=[hbm] * 7 + [vmem] * 3,
        out_specs=(hbm,) * 7 + (vmem,),
        scratch_shapes=[
            pltpu.VMEM(wg.shape, BF16),
            pltpu.VMEM(wo.shape, BF16),
            pltpu.VMEM((2, 2, 2, ways // 2, hb, width), BF16),
            pltpu.VMEM((2, 2, 2, hb, width), BF16),
            pltpu.VMEM((2, 2, hb, width), BF16),
            pltpu.VMEM((2, rows, part), BF16),
            pltpu.VMEM((2, 3, rows, part), BF16),
            pltpu.VMEM((2, 2, rows, units), BF16),
            dma((2,)),
            dma((2, 2, 3)),
            dma((2, 2, 2, ways)),
            dma((2, 2, 2, ways)),
            dma((2, 2)),
            dma((2, 2)),
            dma((2, 2)),
            dma((2, 2)),
            dma((max(half - 1, 1),)),
            dma((max(half - 1, 1),)),
        ],
        compiler_params=pltpu.CompilerParams(collective_id=2, has_side_effects=True, vmem_limit_bytes=63 << 20),
        name="rest",
    )(qkv_all, g_all, ap_all, normed_all, cot_all, wg, wo, *tables)


def normalize(rows):
    mean = jnp.mean(rows, -1, keepdims=True)
    centred = rows - mean
    inv = lax.rsqrt(jnp.mean(centred * centred, -1, keepdims=True) + EPSILON)
    return centred * inv, inv


def local(
    tokens, layer_norm_gain, layer_norm_bias, qkv_weight, qkv_bias, dense_weight, dense_bias,
    fc1_weight, fc1_bias, fc2_weight, fc2_bias, cotangent,
):
    shape = tokens.shape
    rows, width = shape[0] * shape[1], shape[2]
    head_dim = width // HEADS
    ways = lax.axis_size("seq")
    spread = lax.axis_size("fsdp")
    half = spread // 2
    length = rows * ways
    heads = HEADS // (2 * ways)
    shard, hidden = dense_weight.shape[0], fc2_weight.shape[0]
    part, units = shard * half, hidden * half
    me, f = lax.axis_index("seq"), lax.axis_index("fsdp")
    group = lax.rem(f, half)

    mine = jnp.stack([layer_norm_gain, layer_norm_bias, dense_bias, fc2_bias]).astype(F32)
    vectors = lax.dynamic_update_slice(jnp.zeros((8, width), F32), mine, (0, (me * spread + f) * mine.shape[1]))
    biases = jnp.zeros((8, max(part, units)), F32)
    biases = lax.dynamic_update_slice(biases, qkv_bias.astype(F32), (0, group * shard))
    biases = lax.dynamic_update_slice(biases, fc1_bias.astype(F32)[None], (3, group * hidden))
    tok, cot = tokens.reshape(rows, width), cotangent.reshape(rows, width)
    _, cot_all, normed_all, qkv_all, g_all, ap_all, wg, wo, b1_sum, small = front(
        ways, spread, heads, tok, cot, qkv_weight.transpose(1, 2, 0), fc1_weight.transpose(1, 0), dense_weight,
        fc2_weight, vectors, biases,
    )

    def to_peer(x, k):
        pairs = [(i, i - i % half + (i % half + k) % half) for i in range(spread)]
        return lax.ppermute(x, "fsdp", pairs)

    def cut(x, at, size, axis):
        return lax.dynamic_slice_in_dim(x, at * size, size, axis)

    flat = lambda x: x.reshape(2 * length, x.shape[-1])
    fc1_sum = dot_tn(flat(normed_all), flat(ap_all[1]))
    fc2_sum = dot_tn(flat(ap_all[0]), flat(cot_all))
    peers = [(k, lax.rem(group + k, half)) for k in range(1, half)]
    fc1_out = [cut(fc1_sum, p, hidden, 1).astype(BF16) for _, p in peers]
    fc2_out = [cut(fc2_sum, p, hidden, 0).astype(BF16) for _, p in peers]
    fc1_grad, fc2_grad = cut(fc1_sum, group, hidden, 1), cut(fc2_sum, group, hidden, 0)
    b1_out = [cut(b1_sum, p, hidden, 1).astype(BF16) for _, p in peers]
    fc1_in = [to_peer(x, k) for (k, _), x in zip(peers, fc1_out)]
    fc2_in = [to_peer(x, k) for (k, _), x in zip(peers, fc2_out)]
    b1_in = [to_peer(x, k) for (k, _), x in zip(peers, b1_out)]
    g_all, fc1_out, fc2_out, fc1_grad, fc2_grad = lax.optimization_barrier((g_all, fc1_out, fc2_out, fc1_grad, fc2_grad))

    tables = rotation_tables(length, head_dim, heads)
    _, _, _, own_sum, far_sum, dw_own, dw_in, qkv_b_sum = rest(
        ways, spread, heads, head_dim, qkv_all, g_all, ap_all, normed_all, cot_all, wg, wo, tables
    )
    total = lambda own, come: functools.reduce(lambda a, b: a + b.astype(F32), come, own)
    fc1_w_grad, fc2_w_grad = total(fc1_grad, fc1_in), total(fc2_grad, fc2_in)
    fc1_b_grad = total(cut(b1_sum, group, hidden, 1), b1_in)[0]
    b_in = [to_peer(cut(qkv_b_sum, p, shard, 1).astype(BF16), k) for k, p in peers]
    qkv_b_grad = total(cut(qkv_b_sum, group, shard, 1), b_in)
    dw = total(dw_own, [dw_in[k] for k in range(half - 1)])
    qkv_w_grad, dense_w_grad = dw[:3].transpose(2, 0, 1), dw[3]

    rows_f32, cot_f32 = tok.astype(F32), cot.astype(F32)
    sums = (own_sum.astype(F32) + far_sum.astype(F32)).reshape(2, rows, width)
    normed_grad = sums[0]
    output = (rows_f32 + sums[1] + small[2] + small[3]).astype(BF16).reshape(shape)
    xhat, inv = normalize(rows_f32)
    scaled = normed_grad * small[0]
    inner = inv * (
        scaled
        - jnp.mean(scaled, -1, keepdims=True)
        - xhat * jnp.mean(scaled * xhat, -1, keepdims=True)
    )
    tokens_grad = (cot_f32 + inner).astype(BF16).reshape(shape)
    sums = jnp.stack([jnp.sum(normed_grad * xhat, 0), jnp.sum(normed_grad, 0), jnp.sum(cot_f32, 0)])
    sums = scatter_small(sums)
    return (
        output, tokens_grad, sums[0], sums[1], qkv_w_grad, qkv_b_grad, dense_w_grad, sums[2],
        fc1_w_grad, fc1_b_grad, fc2_w_grad, sums[2],
    )


def solution(mesh):
    both = ("seq", "fsdp")
    rows = P("fsdp", "seq", None)
    return jax.shard_map(
        local,
        mesh=mesh,
        in_specs=(
            rows, P(both), P(both), P(None, None, both), P(None, both), P(both, None), P(both),
            P(None, both), P(both), P(both, None), P(both), rows,
        ),
        out_specs=(
            rows, rows, P(both), P(both), P(None, None, both), P(None, both), P(both, None), P(both),
            P(None, both), P(both), P(both, None), P(both),
        ),
        check_vma=False,
    )
```

```python
import functools
import math

import jax
import jax.numpy as jnp
from jax import lax
from jax.experimental import pallas as pl
from jax.experimental.pallas import tpu as pltpu
from jax.sharding import PartitionSpec as P

HEADS = 32
ROT = 32
EPSILON = 1e-05
GELU_C = math.sqrt(2.0 / math.pi)
BASE_LOG = math.log(10000.0)
F32 = jnp.float32
BF16 = jnp.bfloat16
MESH = pl.DeviceIdType.MESH


def dot_nn(left, right):
    return lax.dot_general(left, right, (((1,), (0,)), ((), ())), preferred_element_type=F32)


def dot_nt(left, right):
    return lax.dot_general(left, right, (((1,), (1,)), ((), ())), preferred_element_type=F32)


def dot_tn(left, right):
    return lax.dot_general(left, right, (((0,), (0,)), ((), ())), preferred_element_type=F32)


def gelu_pair(pre):
    t = jnp.tanh(GELU_C * (pre + 0.044715 * pre * pre * pre))
    value = 0.5 * pre * (1.0 + t)
    slope = 0.5 * (1.0 + t) + 0.5 * pre * (1.0 - t * t) * GELU_C * (1.0 + 3.0 * 0.044715 * pre * pre)
    return value, slope


def xor_perm(size, mask):
    return [(i, i ^ mask) for i in range(size)]


def swap(x, axis, mask):
    return lax.ppermute(x, axis, xor_perm(lax.axis_size(axis), mask))


def bit_orders(ways):
    upper = list(range(1, ways.bit_length() - 1))
    last = [0] if ways > 1 else []
    return upper + last, upper[::-1] + last


def masks_of(order):
    masks = [0]
    for b in order:
        masks = masks + [m ^ (1 << b) for m in masks]
    return masks


def scatter_small(x):
    for axis in ("seq", "fsdp"):
        ways = lax.axis_size(axis)
        place = lax.axis_index(axis)
        for b in reversed(range(ways.bit_length() - 1)):
            n = x.shape[1] // 2
            mine_high = (place >> b) & 1
            keep = jnp.where(mine_high == 1, x[:, n:], x[:, :n])
            send = jnp.where(mine_high == 1, x[:, :n], x[:, n:])
            x = keep + swap(send, axis, 1 << b)
    return x


def rotation_tables(length, head_dim, heads):
    half = ROT // 2
    inverse = jnp.exp(-(jnp.arange(half).astype(F32) * 2.0 / ROT) * BASE_LOG)
    angles = jnp.arange(length).astype(F32)[:, None] * inverse[None, :]
    cos, sin = jnp.cos(angles), jnp.sin(angles)
    zero = jnp.zeros_like(sin)
    rest = jnp.zeros((length, head_dim - ROT), F32)
    one_head = (
        jnp.concatenate([cos, cos, rest + 1.0], 1),
        jnp.concatenate([-sin, zero, rest], 1),
        jnp.concatenate([zero, sin, rest], 1),
    )
    return tuple(jnp.tile(t, (1, heads)) for t in one_head)


def flip(place, bit):
    return place + bit - 2 * bit * ((place // bit) % 2)


class Layout:
    def __init__(self, ways, spread):
        self.ways, self.spread, self.half = ways, spread, spread // 2
        self.steps = ways.bit_length() - 1
        self.orders = bit_orders(ways)
        self.masks = [masks_of(o) for o in self.orders]
        self.me, self.f = lax.axis_index("seq"), lax.axis_index("fsdp")
        self.g = self.f % self.half
        self.base = self.f - self.g
        self.far = {"fsdp": (self.f + self.half) % spread}
        self.peer_at = [(self.g + k) % self.half for k in range(1, self.half)]
        self.peers = [{"fsdp": self.base + p} for p in self.peer_at]

    def near(self, b):
        return {"seq": flip(self.me, 1 << b)}

    def device_of(self, h, p):
        place = self.me
        for b in range(self.steps):
            if (self.masks[h][p] >> b) & 1:
                place = flip(place, 1 << b)
        return place

    def meet(self):
        everyone = [self.near(b) for b in range(self.steps)] + [self.far] + self.peers
        barrier = pltpu.get_barrier_semaphore()
        for device in everyone:
            pl.semaphore_signal(barrier, inc=1, device_id=device, device_id_type=MESH)
        pl.semaphore_wait(barrier, len(everyone))


def remote(src, dst, send, recv, device):
    return pltpu.make_async_remote_copy(
        src_ref=src, dst_ref=dst, send_sem=send, recv_sem=recv, device_id=device, device_id_type=MESH
    )


def aligned(start, size, first=0):
    if isinstance(start, int):
        return pl.ds(first + start, size)
    return pl.ds(pl.multiple_of(first + start, math.gcd(first, size)), size)


def wide(x, w, cuts):
    if all(c % 128 == 0 for c in cuts):
        y = dot_nt(x, w[...])
        return [y[:, a:b] for a, b in zip(cuts, cuts[1:])]
    return [dot_nt(x, w[a:b, :]) for a, b in zip(cuts, cuts[1:])]


def shard_of(arrays, r, s, rows):
    if len(arrays) > 1:
        return arrays[r].at[s, rows, :]
    half = lax.axis_size("fsdp") // 2
    hidden = arrays[0].shape[2] // half
    return arrays[0].at[s, rows, pl.ds(r * hidden, hidden)]


def front_kernel(
    ways, spread, heads, head_dim,
    tok_own, cot_own, qkv_own, w1_own, dense_own, w2_own, vectors, biases, cos_ref, neg_ref, pos_ref,
    tok_all, cot_all, normed_all, qkv_all, g_all, wg_out, wo_out, o_out, dqkv_out, b1_out, vectors_out, bias_out, *more,
):
    at = Layout(ways, spread)
    half, steps, orders = at.half, at.steps, at.orders
    arrays = 1 if w2_own.shape[0] % 128 == 0 else half
    acts, pres = more[:arrays], more[arrays : 2 * arrays]
    (
        wg, wo, xb, nb, qb, gb, apb, vec, vec_in, bias_in,
        row_send, row_recv, far_send, far_recv, w_send, w_recv, w_local, load_sem, out_sem, w_out_sem,
        vec_send, vec_recv, bias_send, bias_recv,
    ) = more[2 * arrays :]
    hb = tok_own.shape[0] // 2
    shard, hidden = dense_own.shape[0], w2_own.shape[0]
    part, units = half * shard, half * hidden
    own, everything = (tok_own, cot_own), (tok_all, cot_all)
    at.meet()

    def span(h, p, size=1):
        start = (h * ways + p) * hb
        return pl.ds(start if isinstance(start, int) else pl.multiple_of(start, hb), hb * size)

    def source(s, a, h, p):
        if s == 0 and p == 0:
            return own[a].at[pl.ds(h * hb, hb), :]
        return everything[a].at[s, span(h, p), :]

    def row_copy(s, a, h, p, t):
        q = p + (1 << t)
        return remote(
            source(s, a, h, p), everything[a].at[s, span(h, q), :],
            row_send.at[s, a, h, q], row_recv.at[s, a, h, q], at.near(orders[h][t]),
        )

    def forward(s, a, h, p):
        for t in range(p.bit_length(), steps):
            row_copy(s, a, h, p, t).start()

    def arrived(s, a, h, p):
        t = p.bit_length() - 1
        row_copy(s, a, h, p - (1 << t), t).wait_recv()

    def relay(s, p, kinds=(0, 1)):
        for a in kinds:
            for h in range(2):
                arrived(s, a, h, p)
                forward(s, a, h, p)

    def far_copy(a, h):
        return remote(
            source(0, a, h, 0), everything[a].at[1, span(h, 0), :], far_send.at[a, h], far_recv.at[a, h], at.far
        )

    heads_at = aligned(at.g * shard, shard)

    def slab(n, r):
        if n < 3:
            return qkv_own.at[n], wg.at[aligned(at.g * shard, shard, n * part), :]
        if n == 3:
            return w1_own, wg.at[pl.ds(3 * part + r * hidden, hidden), :]
        if n == 4:
            return w2_own, wo.at[pl.ds(part + r * hidden, hidden), :]
        return dense_own, wo.at[heads_at, :]

    def weight_copy(k, n):
        src, dst = slab(n, half - k)
        return remote(src, dst, w_send.at[k - 1, n], w_recv.at[k - 1, n], at.peers[k - 1])

    weight_copies = [(k, n) for n in range(6) for k in range(1, half)]

    def bias_copy(k):
        return remote(biases, bias_in.at[k - 1], bias_send.at[k - 1], bias_recv.at[k - 1], at.peers[k - 1])

    spread_bits = spread.bit_length() - 1
    partners = [{"fsdp": flip(at.f, 1 << b)} for b in range(spread_bits)] + [at.near(b) for b in range(steps)]

    def vector_copy(b):
        return remote(vec.at[b], vec_in.at[b], vec_send.at[b], vec_recv.at[b], partners[b])

    def vector_step(b):
        vector_copy(b).wait_recv()
        vec[b + 1] = vec[b] + vec_in[b]
        if b + 1 < len(partners):
            vector_copy(b + 1).start()

    inner = (at.f * 4 >= spread) & (at.f * 4 < 3 * spread)
    outer = jnp.logical_not(inner)

    def send_weights(items):
        for n in items:
            for k in range(1, half):
                weight_copy(k, n).start()

    def own_weights(items):
        for n in items:
            local_w[n].wait()

    def far_weights(items):
        for n in items:
            for k in range(1, half):
                weight_copy(k, n).wait_recv()

    def far(a, what):
        for h in range(2):
            getattr(far_copy(a, h), what)()

    attention_part, mlp_part = (0, 1, 2, 5), (3, 4)
    local_w = [pltpu.make_async_copy(s, d, w_local.at[n]) for n, (s, d) in enumerate(slab(n, 0) for n in range(6))]
    for h in range(2):
        forward(0, 0, h, 0)
    vec[0] = vectors[...]
    vector_copy(0).start()
    for k in range(1, half):
        bias_copy(k).start()
    for c in local_w:
        c.start()
    for b in range(spread_bits):
        vector_step(b)

    @pl.when(outer)
    def _():
        far(0, "start")
        send_weights(attention_part)
        far(1, "start")
        send_weights(mlp_part)

    @pl.when(inner)
    def _():
        send_weights(attention_part)

    vector_step(spread_bits)
    for h in range(2):
        forward(0, 1, h, 0)

    order = [j for p in range(ways // 2) for j in (p, p + ways // 2)]

    def load(s, n, first):
        slot, j = n % 2, order[n]
        for a in range(2):
            for h in range(2):
                if first:
                    src = source(s, a, h, j)
                else:
                    src = (normed_all, cot_all)[a].at[s, span(h, j), :]
                pltpu.make_async_copy(src, xb.at[slot, a, pl.ds(h * hb, hb), :], load_sem.at[slot, a, h]).start()

    def outputs(slot, s, j, first, units_of, size=1):
        copies = []
        for h in range(2):
            rows, to = pl.ds(h * hb * size, hb * size), span(h, j, size)
            pairs = []
            if first:
                pairs += [
                    (nb.at[slot, rows, :], normed_all.at[s, to, :]),
                    (qb.at[slot, :, rows, :], qkv_all.at[:, s, to, :]),
                    (gb.at[slot, rows, :], g_all.at[s, to, :]),
                ]
            for r in units_of:
                pairs.append((apb.at[slot, 0, r, rows, :], shard_of(acts, r, s, to)))
                pairs.append((apb.at[slot, 1, r, rows, :], shard_of(pres, r, s, to)))
            for n, (x, y) in enumerate(pairs):
                copies.append(pltpu.make_async_copy(x, y, out_sem.at[slot, h, n]))
        return copies

    def attention_rows(slot):
        x = xb[slot, 0, : 2 * hb].astype(F32)
        centred = x - jnp.mean(x, -1, keepdims=True)
        inv = lax.rsqrt(jnp.mean(centred * centred, -1, keepdims=True) + EPSILON)
        nb[slot] = (centred * inv * gain() + shift()).astype(BF16)
        thirds = wide(nb[slot], wg.at[0 : 3 * part], [0, part, 2 * part, 3 * part])
        for n, y in enumerate(thirds):
            qb[slot, n] = y + bias[n : n + 1, :part]
        gb[slot] = dot_nt(xb[slot, 1, : 2 * hb], wo[0:part, :]).astype(BF16)

    def mlp_rows(slot, normed, cot, r, count):
        b1 = biases if r == 0 else bias_in.at[half - r - 1]
        pre = dot_nt(normed, wg[3 * part + r * hidden : 3 * part + (r + 1) * hidden, :]) + b1[3:4, :hidden]
        act, slope = gelu_pair(pre)
        apb[slot, 0, r, :count] = act.astype(BF16)
        grad = dot_nt(cot, wo[part + r * hidden : part + (r + 1) * hidden, :]) * slope
        b1_out[r : r + 1, :] += jnp.sum(grad, 0, keepdims=True)
        apb[slot, 1, r, :count] = grad.astype(BF16)

    def loaded(slot):
        for a in range(2):
            for h in range(2):
                pltpu.make_async_copy(
                    own[a].at[pl.ds(h * hb, hb), :], xb.at[slot, a, pl.ds(h * hb, hb), :], load_sem.at[slot, a, h]
                ).wait()

    def run(s, units_of, before_load):
        before_load(0)
        load(s, 0, True)

        def block(k, _):
            slot = k % 2
            j = k // 2 + (k % 2) * (ways // 2)
            for n in range(1, ways):
                @pl.when(k + 1 == n)
                def _():
                    before_load(n)
                    load(s, n, True)

            loaded(slot)

            @pl.when(k >= 2)
            def _():
                for c in outputs(slot, s, j, True, units_of):
                    c.wait()

            attention_rows(slot)
            for r in units_of:
                mlp_rows(slot, nb[slot], xb[slot, 1, : 2 * hb], r, 2 * hb)
            for c in outputs(slot, s, j, True, units_of):
                c.start()
            if s == 0:
                @pl.when(k == 0)
                def _():
                    copies = [
                        pltpu.make_async_copy(
                            xb.at[0, 1, pl.ds(h * hb, hb), :], cot_all.at[0, span(h, 0), :], load_sem.at[0, 1, h]
                        )
                        for h in range(2)
                    ]
                    for c in copies:
                        c.start()
                    for c in copies:
                        c.wait()

            return 0

        lax.fori_loop(0, ways, block, 0)
        for slot in range(2):
            for c in outputs(slot, s, order[ways - 2 + slot], True, units_of):
                c.wait()

    def rerun(first, count, units_of):
        per = ways // 2

        def copies(k):
            s, p, slot = k // per, 2 * (k % per), k % 2
            return [
                pltpu.make_async_copy(
                    x.at[s, span(h, p, 2), :], xb.at[slot, a, pl.ds(2 * h * hb, 2 * hb), :], load_sem.at[slot, a, h]
                )
                for a, x in enumerate((normed_all, cot_all))
                for h in range(2)
            ]

        def stores(k):
            return outputs(k % 2, k // per, 2 * (k % per), False, units_of, 2)

        for c in copies(first):
            c.start()

        def block(k, _):
            slot = k % 2
            for c in copies(k):
                c.wait()

            @pl.when(k + 1 < first + count)
            def _():
                for c in copies(k + 1):
                    c.start()

            @pl.when(k >= first + 2)
            def _():
                for c in stores(k):
                    c.wait()

            for r in units_of:
                mlp_rows(slot, xb[slot, 0], xb[slot, 1], r, 4 * hb)
            for c in stores(k):
                c.start()
            return 0

        lax.fori_loop(first, first + count, block, 0)
        for k in range(first + count - 2, first + count):
            for c in stores(k):
                c.wait()

    vector_step(spread_bits + 1)
    relay(0, 1)

    @pl.when(inner)
    def _():
        far(0, "wait_recv")
        far(0, "start")

    for b in range(spread_bits + 2, len(partners)):
        vector_step(b)
    vectors_out[...] = vec[len(partners)]
    gain = lambda: vec[len(partners), 0:1, :]
    shift = lambda: vec[len(partners), 1:2, :]
    for k in range(1, half):
        bias_copy(k).wait_recv()
    bias = biases[...]
    for k in range(1, half):
        bias = bias + bias_in[k - 1]
    own_weights(attention_part + mlp_part)
    far_weights(attention_part)
    b1_out[...] = jnp.zeros_like(b1_out)

    def rows_of_own(n):
        p = order[n]
        if p >= ways // 2:
            for a in range(2):
                for h in range(2):
                    arrived(0, a, h, p)
        elif p >= 2:
            relay(0, p)
        if p == 2:
            @pl.when(inner)
            def _():
                far(1, "wait_recv")
                far(1, "start")

        if p == ways // 2 - 1:
            @pl.when(outer)
            def _():
                far(0, "wait_recv")

            for h in range(2):
                forward(1, 0, h, 0)

            @pl.when(inner)
            def _():
                for h in range(2):
                    forward(1, 1, h, 0)

    run(0, (), rows_of_own)

    def hook(i, count):
        @pl.when(i == count // 2)
        def _():
            @pl.when(inner)
            def _():
                far(1, "wait_send")
                send_weights(mlp_part)

            @pl.when(outer)
            def _():
                far(1, "wait_recv")
                for h in range(2):
                    forward(1, 1, h, 0)

        @pl.when(i == count - 1)
        def _():
            relay(1, 1, (0,))

    bias_out[...] = jnp.zeros_like(bias_out)
    length = 2 * ways * hb
    block_rows = min(512, length)
    chunks = [pl.multiple_of((2 * at.device_of(h, p) + h) * hb, hb) for h in range(2) for p in range(ways)]
    pl.run_scoped(
        lambda *scratch: attention_core(
            heads, head_dim, block_rows, chunks, 0, qkv_all, g_all, cos_ref, neg_ref, pos_ref,
            o_out, dqkv_out, bias_out, hook, *scratch,
        ),
        *attention_scratch(length, part, block_rows, len(chunks)),
    )
    rerun(0, ways // 2, (0,))
    relay(1, 1, (1,))

    def rows_of_partner(n):
        p = order[n]
        if p >= ways // 2:
            for a in range(2):
                for h in range(2):
                    arrived(1, a, h, p)
        elif p >= 2:
            relay(1, p)

    run(1, (0,), rows_of_partner)
    far_weights(mlp_part)
    weights_out = [pltpu.make_async_copy(x, y, w_out_sem.at[n]) for n, (x, y) in enumerate(((wg, wg_out), (wo, wo_out)))]
    for c in weights_out:
        c.start()
    rerun(0, ways, tuple(range(1, half)))
    for c in weights_out:
        c.wait()
    for k, n in weight_copies:
        weight_copy(k, n).wait_send()
    for k in range(1, half):
        bias_copy(k).wait_send()
    for b in range(len(partners)):
        vector_copy(b).wait_send()

    @pl.when(outer)
    def _():
        far(0, "wait_send")
        far(1, "wait_send")

    @pl.when(inner)
    def _():
        far(0, "wait_send")

    for a in range(2):
        for h in range(2):
            for s in range(2):
                for p in range(ways):
                    for t in range(p.bit_length(), steps):
                        row_copy(s, a, h, p, t).wait_send()


def front(ways, spread, heads, head_dim, tok, cot, qkv_w, w1, dense_w, w2, vectors, biases, tables):
    rows, width = tok.shape
    half = spread // 2
    length = rows * ways
    part, units = dense_w.shape[0] * half, w2.shape[0] * half
    arrays = 1 if w2.shape[0] % 128 == 0 else half
    hops = (spread * ways).bit_length() - 1
    hbm = pl.BlockSpec(memory_space=pl.ANY)
    vmem = pl.BlockSpec(memory_space=pltpu.VMEM)
    shape = jax.ShapeDtypeStruct
    dma = pltpu.SemaphoreType.DMA
    return pl.pallas_call(
        functools.partial(front_kernel, ways, spread, heads, head_dim),
        out_shape=(
            shape((2, length, width), BF16),
            shape((2, length, width), BF16),
            shape((2, length, width), BF16),
            shape((3, 2, length, part), F32),
            shape((2, length, part), BF16),
            shape((3 * part + units, width), BF16),
            shape((part + units, width), BF16),
            shape((1, length, part), BF16),
            shape((3, 1, length, part), BF16),
            shape((half, units // half), F32),
            shape(vectors.shape, F32),
            shape((3, part), F32),
        )
        + (shape((2, length, units // arrays), BF16),) * (2 * arrays),
        in_specs=[hbm] * 6 + [vmem] * 5,
        out_specs=(hbm,) * 9 + (vmem,) * 3 + (hbm,) * (2 * arrays),
        scratch_shapes=[
            pltpu.VMEM((3 * part + units, width), BF16),
            pltpu.VMEM((part + units, width), BF16),
            pltpu.VMEM((2, 2, 2 * rows, width), BF16),
            pltpu.VMEM((2, rows, width), BF16),
            pltpu.VMEM((2, 3, rows, part), F32),
            pltpu.VMEM((2, rows, part), BF16),
            pltpu.VMEM((2, 2, half, 2 * rows, units // half), BF16),
            pltpu.VMEM((hops + 1,) + vectors.shape, F32),
            pltpu.VMEM((hops,) + vectors.shape, F32),
            pltpu.VMEM((max(half - 1, 1),) + biases.shape, F32),
            dma((2, 2, 2, ways)),
            dma((2, 2, 2, ways)),
            dma((2, 2)),
            dma((2, 2)),
            dma((max(half - 1, 1), 6)),
            dma((max(half - 1, 1), 6)),
            dma((6,)),
            dma((2, 2, 2)),
            dma((2, 2, 3 + 2 * half)),
            dma((2,)),
            dma((hops,)),
            dma((hops,)),
            dma((max(half - 1, 1),)),
            dma((max(half - 1, 1),)),
        ],
        compiler_params=pltpu.CompilerParams(collective_id=1, has_side_effects=True, vmem_limit_bytes=60 << 20),
        name="front",
    )(tok, cot, qkv_w, w1, dense_w, w2, vectors, biases, *tables)


def attention_core(
    heads, head_dim, block, chunks, seq, qkv_in, g_in, cos_ref, neg_ref, pos_ref, o_out, dqkv_out, bias_out,
    hook, stage, q, k, v, g, kt, vt, gt, dk, dv, dq, o, scores, in_sem, out_sem,
):
    length, width = q.shape
    half = ROT // 2
    scale = head_dim ** (-0.5)
    count = length // block
    chunk = length // len(chunks)
    loads = []
    for r, start in enumerate(chunks):
        rows, here = pl.ds(start, chunk), pl.ds(r * chunk, chunk)
        loads.append(pltpu.make_async_copy(qkv_in.at[:, seq, here, :], stage.at[:, rows, :], in_sem.at[r, 0]))
        loads.append(pltpu.make_async_copy(g_in.at[seq, here, :], g.at[rows, :], in_sem.at[r, 1]))
    for c in loads:
        c.start()
    for c in loads:
        c.wait()

    def prepare(at, _):
        rows = aligned(at * block, block)
        cos, neg, pos = cos_ref[rows, :], neg_ref[rows, :], pos_ref[rows, :]

        def rotate(x):
            return x * cos + pltpu.roll(x, width - half, 1) * neg + pltpu.roll(x, half, 1) * pos

        q[rows, :] = rotate(stage[0, rows, :]).astype(BF16) * scale
        kb = rotate(stage[1, rows, :]).astype(BF16)
        vb = stage[2, rows, :].astype(BF16)
        k[rows, :] = kb
        v[rows, :] = vb
        kt[:, rows] = kb.T
        vt[:, rows] = vb.T
        gt[:, rows] = g[rows, :].T
        dk[rows, :] = jnp.zeros((block, width), F32)
        dv[rows, :] = jnp.zeros((block, width), F32)
        return 0

    lax.fori_loop(0, count, prepare, 0)
    lane = lax.broadcasted_iota(jnp.int32, (block, width), 1)

    def only(x, h):
        if heads == 1:
            return x
        keep = (lane >= h * head_dim) & (lane < (h + 1) * head_dim)
        return jnp.where(keep, x.astype(F32), 0.0).astype(BF16)

    def one_block(i, _):
        hook(i, count)
        mine = aligned(i * block, block)
        qi, gi = q[mine, :], g[mine, :]
        ob = jnp.zeros((width, block), F32)
        dqb = jnp.zeros((width, block), F32)
        row = lax.broadcasted_iota(jnp.int32, (width, block), 0)
        for h in range(heads):
            qh, gh = only(qi, h), only(gi, h)

            def first(j, top):
                cols = aligned(j * block, block)
                s = dot_nt(k[cols, :], qh)
                scores[cols, :] = s
                return jnp.maximum(top, jnp.max(s, 0, keepdims=True))

            top = lax.fori_loop(0, i, first, jnp.full((1, block), -1e30, F32))
            s = dot_nt(k[mine, :], qh)
            key_at = lax.broadcasted_iota(jnp.int32, (block, block), 0)
            query_at = lax.broadcasted_iota(jnp.int32, (block, block), 1)
            s = jnp.where(key_at <= query_at, s, -1e30)
            scores[mine, :] = s
            top = jnp.maximum(top, jnp.max(s, 0, keepdims=True))

            def second(j, carry):
                total, acc = carry
                cols = aligned(j * block, block)
                e = jnp.exp(scores[cols, :] - top)
                scores[cols, :] = e
                return total + jnp.sum(e, 0, keepdims=True), acc + dot_nn(vt[:, cols], e.astype(BF16))

            total, acc = lax.fori_loop(
                0, i + 1, second, (jnp.zeros((1, block), F32), jnp.zeros((width, block), F32))
            )
            inv = 1.0 / total
            acc = (acc * inv).astype(BF16).astype(F32)
            here = (row >= h * head_dim) & (row < (h + 1) * head_dim)
            acc = jnp.where(here, acc, 0.0)
            delta = jnp.sum(acc * gt[:, mine].astype(F32), 0, keepdims=True)
            ob = ob + acc

            def third(j, acc_q):
                cols = aligned(j * block, block)
                p = scores[cols, :] * inv
                dv[cols, :] += dot_nn(p.astype(BF16), gh)
                dp = dot_nt(v[cols, :], gh)
                ds = (p * (dp - delta)).astype(BF16)
                dk[cols, :] += dot_nn(ds, qh)
                return acc_q + dot_nn(kt[:, cols], ds)

            acc_q = lax.fori_loop(0, i + 1, third, jnp.zeros((width, block), F32))
            dqb = dqb + jnp.where(here, acc_q, 0.0)
        o[mine, :] = ob.T.astype(BF16)
        dq[mine, :] = dqb.T * scale
        return 0

    lax.fori_loop(0, count, one_block, 0)

    def finish(at, sums):
        rows = aligned(at * block, block)
        cos, neg, pos = cos_ref[rows, :], neg_ref[rows, :], pos_ref[rows, :]

        def unrotate(x):
            return x * cos - pltpu.roll(x, width - half, 1) * neg - pltpu.roll(x, half, 1) * pos

        a = unrotate(dq[rows, :].astype(BF16).astype(F32))
        b = unrotate(dk[rows, :].astype(BF16).astype(F32))
        c = dv[rows, :].astype(BF16).astype(F32)
        q[rows, :] = a.astype(BF16)
        k[rows, :] = b.astype(BF16)
        v[rows, :] = c.astype(BF16)
        return tuple(s + jnp.sum(x, 0, keepdims=True) for s, x in zip(sums, (a, b, c)))

    sums = lax.fori_loop(0, count, finish, tuple(jnp.zeros((1, width), F32) for _ in range(3)))
    bias_out[...] += jnp.concatenate(list(sums), 0)
    stores = []
    for r, start in enumerate(chunks):
        rows, here = pl.ds(start, chunk), pl.ds(r * chunk, chunk)
        for n, src in enumerate((q, k, v)):
            stores.append(pltpu.make_async_copy(src.at[rows, :], dqkv_out.at[n, 0, here, :], out_sem.at[r, n]))
        stores.append(pltpu.make_async_copy(o.at[rows, :], o_out.at[0, here, :], out_sem.at[r, 3]))
    for c in stores:
        c.start()
    for c in stores:
        c.wait()


def attention_scratch(length, part, block, chunks):
    return (
        [pltpu.VMEM((3, length, part), F32)]
        + [pltpu.VMEM((length, part), BF16)] * 4
        + [pltpu.VMEM((part, length), BF16)] * 3
        + [pltpu.VMEM((length, part), F32)] * 3
        + [
            pltpu.VMEM((length, part), BF16),
            pltpu.VMEM((length, block), F32),
            pltpu.SemaphoreType.DMA((chunks, 2)),
            pltpu.SemaphoreType.DMA((chunks, 4)),
        ]
    )


def joined(xs, w):
    if all(x.shape[1] % 128 == 0 for x in xs):
        return dot_nn(jnp.concatenate(xs, 1), w[...])
    total, at = None, 0
    for x in xs:
        y = dot_nn(x, w[at : at + x.shape[1], :])
        total, at = (y if total is None else total + y), at + x.shape[1]
    return total


def rest_kernel(
    ways, spread, heads, head_dim,
    qkv_all, g_all, normed_all, cot_all, wg_in, wo_in, o_0, dqkv_0, cos_ref, neg_ref, pos_ref, *more,
):
    at = Layout(ways, spread)
    half, steps, orders = at.half, at.steps, at.orders
    arrays = (len(more) - 27) // 2
    acts, pres = more[:arrays], more[arrays : 2 * arrays]
    (
        o_1, dqkv_1, recv, own_sum, far_sum, dw_own, dw_recv, dw_low, bias_out,
        wg, wo, keep, stage_send, stage_recv, ob, db, apb,
        w_sem, load_sem, rs_send, rs_recv, add_sem, own_sem, far_send, far_recv, dw_send, dw_come,
    ) = more[2 * arrays :]
    hb = keep.shape[4]
    length = 2 * ways * hb
    part = g_all.shape[2]
    shard = part // half
    block = min(512, length)
    width = keep.shape[5]
    at.meet()
    loads = [pltpu.make_async_copy(x, y, w_sem.at[n]) for n, (x, y) in enumerate(((wg_in, wg), (wo_in, wo)))]
    for c in loads:
        c.start()
    bias_out[...] = jnp.zeros_like(bias_out)
    chunks = [
        pl.multiple_of((2 * at.device_of(h, p) + h) * hb, hb) for h in range(2) for p in range(ways)
    ]

    def span(h, p):
        return aligned((h * ways + p) * hb, hb)

    def from_heads(s, pick, o_dst, dqkv_dst, o_sem, dqkv_sem):
        for v, (x, y) in enumerate(((o_0, dqkv_0), (o_1, dqkv_1))):
            @pl.when(s == v)
            def _():
                pltpu.make_async_copy(x.at[0, pick, :], o_dst, o_sem).start()
                pltpu.make_async_copy(y.at[:, 0, pick, :], dqkv_dst, dqkv_sem).start()

    def heads_there(pick, o_dst, dqkv_dst, o_sem, dqkv_sem):
        pltpu.make_async_copy(o_1.at[0, pick, :], o_dst, o_sem).wait()
        pltpu.make_async_copy(dqkv_1.at[:, 0, pick, :], dqkv_dst, dqkv_sem).wait()

    def sent(s, t, h, q, src):
        level = q.bit_length() - 1 if isinstance(q, int) else steps - 1
        return remote(src, recv.at[s, t, h, q], rs_send.at[s, t, h, q], rs_recv.at[s, t, h, q], at.near(orders[h][level]))

    def partial_sums(s):
        def place(i):
            return jnp.where(i < ways // 2, ways // 2 + i, ways - 1 - i)

        def heads_of(i, h):
            slot, rows = i % 2, pl.ds(h * hb, hb)
            return (
                span(h, place(i)), ob.at[slot, rows, :], db.at[slot, :, rows, :],
                load_sem.at[slot, h, 0], load_sem.at[slot, h, 1],
            )

        def act_copies(i, h):
            slot, rows = i % 2, pl.ds(h * hb, hb)
            return [
                pltpu.make_async_copy(
                    shard_of(x, r, s, span(h, place(i))), apb.at[slot, n, r, rows, :], load_sem.at[slot, h, 2 + n * half + r]
                )
                for n, x in enumerate((acts, pres))
                for r in range(half)
            ]

        def fetch(i):
            for h in range(2):
                from_heads(s, *heads_of(i, h))
                for c in act_copies(i, h):
                    c.start()

        def sends(i):
            return [sent(s, t, h, place(i), stage_send.at[i % 2, t, h]) for t in range(2) for h in range(2)]

        fetch(0)

        def one(i, _):
            slot = i % 2
            for h in range(2):
                heads_there(*heads_of(i, h))
                for c in act_copies(i, h):
                    c.wait()

            @pl.when(i + 1 < ways)
            def _():
                fetch(i + 1)

            @pl.when((i == 1) & (s == 0))
            def _():
                for q in range(ways // 2 - 1, ways // 4, -1):
                    serve(1, q, 0)
                send_held(1, 1)

            @pl.when((i >= 2) & (i < ways // 2 + 2))
            def _():
                for c in sends(i - 2):
                    c.wait_send()

            out = joined([ob[slot]] + [apb[slot, 0, r] for r in range(half)], wo).astype(BF16)
            grad = joined([db[slot, n] for n in range(3)] + [apb[slot, 1, r] for r in range(half)], wg).astype(BF16)

            @pl.when(i < ways // 2)
            def _():
                for t, x in enumerate((grad, out)):
                    for h in range(2):
                        stage_send[slot, t, h] = x[h * hb : (h + 1) * hb, :]
                for c in sends(i):
                    c.start()

            @pl.when(i >= ways // 2)
            def _():
                for t, x in enumerate((grad, out)):
                    for h in range(2):
                        keep[s, t, h, ways - 1 - i] = x[h * hb : (h + 1) * hb, :]

            for n in range(ways // 2):
                @pl.when(i == ways // 2 + n)
                def _():
                    for t in range(2):
                        serve(s, ways - 1 - n, t)

            return 0

        lax.fori_loop(0, ways, one, 0)

    def far_copy(t, h):
        return remote(keep.at[1, t, h, 0], far_sum.at[t, h], far_send.at[t, h], far_recv.at[t, h], at.far)

    def own_copy(t, h):
        return pltpu.make_async_copy(keep.at[0, t, h, 0], own_sum.at[t, h], own_sem.at[t, h])

    def serve(s, q, t):
        level = q.bit_length() - 1
        p = q - (1 << level)
        come = [pltpu.make_async_copy(recv.at[s, t, h, q], stage_recv.at[t, h], add_sem.at[t, h]) for h in range(2)]
        for h, c in enumerate(come):
            sent(s, t, h, q, stage_recv.at[t, h]).wait_recv()
            c.start()
        for h, c in enumerate(come):
            c.wait()
            keep[s, t, h, p] = (keep[s, t, h, p].astype(F32) + stage_recv[t, h].astype(F32)).astype(BF16)
            if p and p.bit_length() == level:
                if level == steps - 1:
                    if t == 0:
                        @pl.when(s == 1)
                        def _():
                            sent(s, t, h, p, keep.at[s, t, h, p]).start()
                else:
                    sent(s, t, h, p, keep.at[s, t, h, p]).start()
            if q == 1:
                (own_copy if s == 0 else far_copy)(t, h).start()

    def send_held(s, t):
        for p in range(ways // 2 - 1, ways // 4 - 1, -1):
            for h in range(2):
                sent(s, t, h, p, keep.at[s, t, h, p]).start()

    def shard_copy(k):
        cut = aligned(at.peer_at[k - 1] * shard, shard)
        return remote(dw_low.at[:, cut, :], dw_recv.at[k - 1], dw_send.at[k - 1], dw_come.at[k - 1], at.peers[k - 1])

    def weight_sums(hook):
        rows = min(512, length)
        per = length // rows

        def body(nbuf, cbuf, abuf, acc, rounded, sems, out_sem):
            def heads_of(i):
                slot = i % 2
                return aligned((i % per) * rows, rows), abuf.at[slot, 3], abuf.at[slot, 0:3], sems.at[slot, 3], sems.at[slot, 2]

            def copies(i):
                slot, s, here = i % 2, i // per, aligned((i % per) * rows, rows)
                return [
                    pltpu.make_async_copy(normed_all.at[s, here, :], nbuf.at[slot], sems.at[slot, 0]),
                    pltpu.make_async_copy(cot_all.at[s, here, :], cbuf.at[slot], sems.at[slot, 1]),
                ]

            def fetch(i):
                for c in copies(i):
                    c.start()
                from_heads(i // per, *heads_of(i))

            fetch(0)
            acc[...] = jnp.zeros_like(acc)

            def one(i, _):
                slot = i % 2
                for c in copies(i):
                    c.wait()
                heads_there(*heads_of(i))

                @pl.when(i + 1 < 2 * per)
                def _():
                    fetch(i + 1)

                hook(i, 2 * per)
                normed = nbuf[slot]
                if part % 128 == 0:
                    y = dot_tn(jnp.concatenate([abuf[slot, n] for n in range(3)], 1), normed)
                    for n in range(3):
                        acc[n] += y[n * part : (n + 1) * part, :]
                else:
                    for n in range(3):
                        acc[n] += dot_tn(abuf[slot, n], normed)
                acc[3] += dot_tn(abuf[slot, 3], cbuf[slot])
                return 0

            lax.fori_loop(0, 2 * per, one, 0)
            own = pltpu.make_async_copy(acc.at[:, aligned(at.g * shard, shard), :], dw_own, out_sem.at[0])
            own.start()
            rounded[...] = acc[...].astype(BF16)
            others = pltpu.make_async_copy(rounded, dw_low, out_sem.at[1])
            others.start()
            others.wait()
            own.wait()

        width_of = pltpu.VMEM((2, rows, width), BF16)
        pl.run_scoped(
            body, width_of, width_of, pltpu.VMEM((2, 4, rows, part), BF16),
            pltpu.VMEM((4, part, width), F32), pltpu.VMEM((4, part, width), BF16),
            pltpu.SemaphoreType.DMA((2, 4)), pltpu.SemaphoreType.DMA((2,)),
        )
        for k in range(1, half):
            shard_copy(k).start()

    pl.run_scoped(
        lambda *scratch: attention_core(
            heads, head_dim, block, chunks, 1, qkv_all, g_all, cos_ref, neg_ref, pos_ref,
            o_1, dqkv_1, bias_out, lambda i, count: None, *scratch,
        ),
        *attention_scratch(length, part, block, len(chunks)),
    )
    for c in loads:
        c.wait()

    def one_sequence(turn, _):
        partial_sums(1 - turn)
        return 0

    lax.fori_loop(0, 2, one_sequence, 0)

    for q in range(ways // 4, 0, -1):
        serve(1, q, 0)
    for q in range(ways // 2 - 1, ways // 4, -1):
        serve(1, q, 1)
    for t in range(2):
        send_held(0, t)

    def output_rows_back(i, count):
        @pl.when(i == count // 2)
        def _():
            for q in range(ways // 4, 1, -1):
                serve(1, q, 1)

        @pl.when(i == count - 1)
        def _():
            serve(1, 1, 1)

    weight_sums(output_rows_back)
    for q in range(ways // 2 - 1, 0, -1):
        for t in range(2):
            serve(0, q, t)
    for k in range(1, half):
        shard_copy(k).wait()
    for t in range(2):
        for h in range(2):
            far_copy(t, h).wait()
            own_copy(t, h).wait()
            for s in range(2):
                for p in range(1, ways // 2):
                    sent(s, t, h, p, keep.at[s, t, h, p]).wait_send()


def rest(ways, spread, heads, head_dim, qkv_all, g_all, normed_all, cot_all, wg, wo, o_0, dqkv_0, tables, acts, pres):
    _, length, width = normed_all.shape
    half = spread // 2
    part, hidden = g_all.shape[2], sum(x.shape[2] for x in acts) // half
    hb = length // ways // 2
    shard = part // half
    rows = 2 * hb
    hbm = pl.BlockSpec(memory_space=pl.ANY)
    vmem = pl.BlockSpec(memory_space=pltpu.VMEM)
    shape = jax.ShapeDtypeStruct
    dma = pltpu.SemaphoreType.DMA
    return pl.pallas_call(
        functools.partial(rest_kernel, ways, spread, heads, head_dim),
        out_shape=(
            shape((1, length, part), BF16),
            shape((3, 1, length, part), BF16),
            shape((2, 2, 2, ways, hb, width), BF16),
            shape((2, 2, hb, width), BF16),
            shape((2, 2, hb, width), BF16),
            shape((4, shard, width), F32),
            shape((max(half - 1, 1), 4, shard, width), BF16),
            shape((4, part, width), BF16),
            shape((3, part), F32),
        ),
        in_specs=[hbm] * 8 + [vmem] * 3 + [hbm] * (2 * len(acts)),
        out_specs=(hbm,) * 8 + (vmem,),
        scratch_shapes=[
            pltpu.VMEM(wg.shape, BF16),
            pltpu.VMEM(wo.shape, BF16),
            pltpu.VMEM((2, 2, 2, ways // 2, hb, width), BF16),
            pltpu.VMEM((2, 2, 2, hb, width), BF16),
            pltpu.VMEM((2, 2, hb, width), BF16),
            pltpu.VMEM((2, rows, part), BF16),
            pltpu.VMEM((2, 3, rows, part), BF16),
            pltpu.VMEM((2, 2, half, rows, hidden), BF16),
            dma((2,)),
            dma((2, 2, 2 + 2 * half)),
            dma((2, 2, 2, ways)),
            dma((2, 2, 2, ways)),
            dma((2, 2)),
            dma((2, 2)),
            dma((2, 2)),
            dma((2, 2)),
            dma((max(half - 1, 1),)),
            dma((max(half - 1, 1),)),
        ],
        compiler_params=pltpu.CompilerParams(collective_id=2, has_side_effects=True, vmem_limit_bytes=63 << 20),
        name="rest",
    )(qkv_all, g_all, normed_all, cot_all, wg, wo, o_0, dqkv_0, *tables, *acts, *pres)


def normalize(rows):
    mean = jnp.mean(rows, -1, keepdims=True)
    centred = rows - mean
    inv = lax.rsqrt(jnp.mean(centred * centred, -1, keepdims=True) + EPSILON)
    return centred * inv, inv


def local(
    tokens, layer_norm_gain, layer_norm_bias, qkv_weight, qkv_bias, dense_weight, dense_bias,
    fc1_weight, fc1_bias, fc2_weight, fc2_bias, cotangent,
):
    shape = tokens.shape
    rows, width = shape[0] * shape[1], shape[2]
    head_dim = width // HEADS
    ways = lax.axis_size("seq")
    spread = lax.axis_size("fsdp")
    half = spread // 2
    length = rows * ways
    heads = HEADS // (2 * ways)
    shard, hidden = dense_weight.shape[0], fc2_weight.shape[0]
    part, units = shard * half, hidden * half
    me, f = lax.axis_index("seq"), lax.axis_index("fsdp")
    group = lax.rem(f, half)

    mine = jnp.stack([layer_norm_gain, layer_norm_bias, dense_bias, fc2_bias]).astype(F32)
    vectors = lax.dynamic_update_slice(jnp.zeros((8, width), F32), mine, (0, (me * spread + f) * mine.shape[1]))
    biases = jnp.zeros((8, max(part, units)), F32)
    biases = lax.dynamic_update_slice(biases, qkv_bias.astype(F32), (0, group * shard))
    biases = lax.dynamic_update_slice(biases, fc1_bias.astype(F32)[None], (3, 0))
    tok, cot = tokens.reshape(rows, width), cotangent.reshape(rows, width)
    tables = rotation_tables(length, head_dim, heads)
    _, cot_all, normed_all, qkv_all, g_all, wg, wo, o_0, dqkv_0, b1_sum, small, bias_0, *hidden_rows = front(
        ways, spread, heads, head_dim, tok, cot, qkv_weight.transpose(1, 2, 0), fc1_weight.transpose(1, 0), dense_weight,
        fc2_weight, vectors, biases, tables,
    )

    def to_peer(x, k):
        pairs = [(i, i - i % half + (i % half + k) % half) for i in range(spread)]
        return lax.ppermute(x, "fsdp", pairs)

    def cut(x, at, size, axis):
        return lax.dynamic_slice_in_dim(x, at * size, size, axis)

    arrays = len(hidden_rows) // 2
    acts, pres = hidden_rows[:arrays], hidden_rows[arrays:]
    flat = lambda x: x.reshape(2 * length, x.shape[-1])
    shard_at = lambda sums, r, axis: (
        sums[r] if len(sums) > 1 else lax.slice_in_dim(sums[0], r * hidden, (r + 1) * hidden, axis=axis)
    )
    fc1_sums = [dot_tn(flat(normed_all), flat(x)) for x in pres]
    fc2_sums = [dot_tn(flat(x), flat(cot_all)) for x in acts]
    peers = [(k, lax.rem(group + k, half)) for k in range(1, half)]
    fc1_out = [shard_at(fc1_sums, k, 1).astype(BF16) for k in range(1, half)]
    fc2_out = [shard_at(fc2_sums, k, 0).astype(BF16) for k in range(1, half)]
    fc1_in = [to_peer(x, k) for (k, _), x in zip(peers, fc1_out)]
    fc2_in = [to_peer(x, k) for (k, _), x in zip(peers, fc2_out)]
    b1_in = [to_peer(b1_sum[k].astype(BF16), k) for k, _ in peers]
    g_all, fc1_out, fc2_out, fc1_sums, fc2_sums = lax.optimization_barrier((g_all, fc1_out, fc2_out, fc1_sums, fc2_sums))
    _, _, _, own_sum, far_sum, dw_own, dw_in, _, bias_1 = rest(
        ways, spread, heads, head_dim, qkv_all, g_all, normed_all, cot_all, wg, wo, o_0, dqkv_0, tables, acts, pres
    )
    qkv_b_sum = bias_0 + bias_1
    total = lambda own, come: functools.reduce(lambda a, b: a + b.astype(F32), come, own)
    fc1_w_grad, fc2_w_grad = total(shard_at(fc1_sums, 0, 1), fc1_in), total(shard_at(fc2_sums, 0, 0), fc2_in)
    fc1_b_grad = total(b1_sum[0], b1_in)
    b_in = [to_peer(cut(qkv_b_sum, p, shard, 1).astype(BF16), k) for k, p in peers]
    qkv_b_grad = total(cut(qkv_b_sum, group, shard, 1), b_in)
    dw = total(dw_own, [dw_in[k] for k in range(half - 1)])
    qkv_w_grad, dense_w_grad = dw[:3].transpose(2, 0, 1), dw[3]

    rows_f32, cot_f32 = tok.astype(F32), cot.astype(F32)
    sums = (own_sum.astype(F32) + far_sum.astype(F32)).reshape(2, rows, width)
    normed_grad = sums[0]
    output = (rows_f32 + sums[1] + small[2] + small[3]).astype(BF16).reshape(shape)
    xhat, inv = normalize(rows_f32)
    scaled = normed_grad * small[0]
    inner = inv * (
        scaled
        - jnp.mean(scaled, -1, keepdims=True)
        - xhat * jnp.mean(scaled * xhat, -1, keepdims=True)
    )
    tokens_grad = (cot_f32 + inner).astype(BF16).reshape(shape)
    sums = jnp.stack([jnp.sum(normed_grad * xhat, 0), jnp.sum(normed_grad, 0), jnp.sum(cot_f32, 0)])
    sums = scatter_small(sums)
    return (
        output, tokens_grad, sums[0], sums[1], qkv_w_grad, qkv_b_grad, dense_w_grad, sums[2],
        fc1_w_grad, fc1_b_grad, fc2_w_grad, sums[2],
    )


def solution(mesh):
    both = ("seq", "fsdp")
    rows = P("fsdp", "seq", None)
    return jax.shard_map(
        local,
        mesh=mesh,
        in_specs=(
            rows, P(both), P(both), P(None, None, both), P(None, both), P(both, None), P(both),
            P(None, both), P(both), P(both, None), P(both), rows,
        ),
        out_specs=(
            rows, rows, P(both), P(both), P(None, None, both), P(None, both), P(both, None), P(both),
            P(None, both), P(both), P(both, None), P(both),
        ),
        check_vma=False,
    )
```

```python
import functools
import math

import jax
import jax.numpy as jnp
from jax import lax
from jax.experimental import pallas as pl
from jax.experimental.pallas import tpu as pltpu
from jax.sharding import PartitionSpec as P

HEADS = 32
ROT = 32
EPSILON = 1e-05
GELU_C = math.sqrt(2.0 / math.pi)
BASE_LOG = math.log(10000.0)
F32 = jnp.float32
BF16 = jnp.bfloat16
MESH = pl.DeviceIdType.MESH


def dot_nn(left, right):
    return lax.dot_general(left, right, (((1,), (0,)), ((), ())), preferred_element_type=F32)


def dot_nt(left, right):
    return lax.dot_general(left, right, (((1,), (1,)), ((), ())), preferred_element_type=F32)


def dot_tn(left, right):
    return lax.dot_general(left, right, (((0,), (0,)), ((), ())), preferred_element_type=F32)


def gelu_pair(pre):
    t = jnp.tanh(GELU_C * (pre + 0.044715 * pre * pre * pre))
    value = 0.5 * pre * (1.0 + t)
    slope = 0.5 * (1.0 + t) + 0.5 * pre * (1.0 - t * t) * GELU_C * (1.0 + 3.0 * 0.044715 * pre * pre)
    return value, slope


def xor_perm(size, mask):
    return [(i, i ^ mask) for i in range(size)]


def swap(x, axis, mask):
    return lax.ppermute(x, axis, xor_perm(lax.axis_size(axis), mask))


def bit_orders(ways):
    upper = list(range(1, ways.bit_length() - 1))
    last = [0] if ways > 1 else []
    return upper + last, upper[::-1] + last


def masks_of(order):
    masks = [0]
    for b in order:
        masks = masks + [m ^ (1 << b) for m in masks]
    return masks


def rotation_tables(length, head_dim, heads):
    half = ROT // 2
    inverse = jnp.exp(-(jnp.arange(half).astype(F32) * 2.0 / ROT) * BASE_LOG)
    angles = jnp.arange(length).astype(F32)[:, None] * inverse[None, :]
    cos, sin = jnp.cos(angles), jnp.sin(angles)
    zero = jnp.zeros_like(sin)
    rest = jnp.zeros((length, head_dim - ROT), F32)
    one_head = (
        jnp.concatenate([cos, cos, rest + 1.0], 1),
        jnp.concatenate([-sin, zero, rest], 1),
        jnp.concatenate([zero, sin, rest], 1),
    )
    return tuple(jnp.tile(t, (1, heads)) for t in one_head)


def flip(place, bit):
    return place + bit - 2 * bit * ((place // bit) % 2)


class Layout:
    def __init__(self, ways, spread):
        self.ways, self.spread, self.half = ways, spread, spread // 2
        self.steps = ways.bit_length() - 1
        self.orders = bit_orders(ways)
        self.masks = [masks_of(o) for o in self.orders]
        self.me, self.f = lax.axis_index("seq"), lax.axis_index("fsdp")
        self.g = self.f % self.half
        self.base = self.f - self.g
        self.far = {"fsdp": (self.f + self.half) % spread}
        self.peer_at = [(self.g + k) % self.half for k in range(1, self.half)]
        self.peers = [{"fsdp": self.base + p} for p in self.peer_at]

    def near(self, b):
        return {"seq": flip(self.me, 1 << b)}

    def device_of(self, h, p):
        place = self.me
        for b in range(self.steps):
            if (self.masks[h][p] >> b) & 1:
                place = flip(place, 1 << b)
        return place

    def meet(self):
        everyone = [self.near(b) for b in range(self.steps)] + [self.far] + self.peers
        barrier = pltpu.get_barrier_semaphore()
        for device in everyone:
            pl.semaphore_signal(barrier, inc=1, device_id=device, device_id_type=MESH)
        pl.semaphore_wait(barrier, len(everyone))


def remote(src, dst, send, recv, device):
    return pltpu.make_async_remote_copy(
        src_ref=src, dst_ref=dst, send_sem=send, recv_sem=recv, device_id=device, device_id_type=MESH
    )


def aligned(start, size, first=0):
    if isinstance(start, int):
        return pl.ds(first + start, size)
    return pl.ds(pl.multiple_of(first + start, math.gcd(first, size)), size)


def wide(x, w, cuts):
    if all(c % 128 == 0 for c in cuts):
        y = dot_nt(x, w[...])
        return [y[:, a:b] for a, b in zip(cuts, cuts[1:])]
    return [dot_nt(x, w[a:b, :]) for a, b in zip(cuts, cuts[1:])]


def shard_of(arrays, r, s, rows):
    if len(arrays) > 1:
        return arrays[r].at[s, rows, :]
    half = lax.axis_size("fsdp") // 2
    hidden = arrays[0].shape[2] // half
    return arrays[0].at[s, rows, pl.ds(r * hidden, hidden)]


def front_kernel(
    ways, spread, heads, head_dim,
    tok_own, cot_own, qkv_own, w1_own, dense_own, w2_own, vectors, biases, cos_ref, neg_ref, pos_ref,
    tok_all, cot_all, normed_all, qkv_all, g_all, wg_out, wo_out, o_out, dqkv_out, b1_out, vectors_out, bias_out, *more,
):
    at = Layout(ways, spread)
    half, steps, orders = at.half, at.steps, at.orders
    arrays = 1 if w2_own.shape[0] % 128 == 0 else half
    acts, pres = more[:arrays], more[arrays : 2 * arrays]
    (
        wg, wo, xb, nb, qb, gb, apb, vec, vec_in, bias_in,
        row_send, row_recv, far_send, far_recv, w_send, w_recv, w_local, load_sem, out_sem, w_out_sem,
        vec_send, vec_recv, bias_send, bias_recv,
    ) = more[2 * arrays :]
    hb = tok_own.shape[0] // 2
    shard, hidden = dense_own.shape[0], w2_own.shape[0]
    part, units = half * shard, half * hidden
    own, everything = (tok_own, cot_own), (tok_all, cot_all)
    at.meet()

    def span(h, p, size=1):
        start = (h * ways + p) * hb
        return pl.ds(start if isinstance(start, int) else pl.multiple_of(start, hb), hb * size)

    def source(s, a, h, p):
        if s == 0 and p == 0:
            return own[a].at[pl.ds(h * hb, hb), :]
        return everything[a].at[s, span(h, p), :]

    def row_copy(s, a, h, p, t):
        q = p + (1 << t)
        return remote(
            source(s, a, h, p), everything[a].at[s, span(h, q), :],
            row_send.at[s, a, h, q], row_recv.at[s, a, h, q], at.near(orders[h][t]),
        )

    def forward(s, a, h, p):
        for t in range(p.bit_length(), steps):
            row_copy(s, a, h, p, t).start()

    def arrived(s, a, h, p):
        t = p.bit_length() - 1
        row_copy(s, a, h, p - (1 << t), t).wait_recv()

    def relay(s, p, kinds=(0, 1)):
        for a in kinds:
            for h in range(2):
                arrived(s, a, h, p)
                forward(s, a, h, p)

    def far_copy(a, h):
        return remote(
            source(0, a, h, 0), everything[a].at[1, span(h, 0), :], far_send.at[a, h], far_recv.at[a, h], at.far
        )

    heads_at = aligned(at.g * shard, shard)

    def slab(n, r):
        if n < 3:
            return qkv_own.at[n], wg.at[aligned(at.g * shard, shard, n * part), :]
        if n == 3:
            return w1_own, wg.at[pl.ds(3 * part + r * hidden, hidden), :]
        if n == 4:
            return w2_own, wo.at[pl.ds(part + r * hidden, hidden), :]
        return dense_own, wo.at[heads_at, :]

    def weight_copy(k, n):
        src, dst = slab(n, half - k)
        return remote(src, dst, w_send.at[k - 1, n], w_recv.at[k - 1, n], at.peers[k - 1])

    weight_copies = [(k, n) for n in range(6) for k in range(1, half)]

    def bias_copy(k):
        return remote(biases, bias_in.at[k - 1], bias_send.at[k - 1], bias_recv.at[k - 1], at.peers[k - 1])

    spread_bits = spread.bit_length() - 1
    partners = [{"fsdp": flip(at.f, 1 << b)} for b in range(spread_bits)] + [at.near(b) for b in range(steps)]

    def vector_copy(b):
        return remote(vec.at[b], vec_in.at[b], vec_send.at[b], vec_recv.at[b], partners[b])

    def vector_step(b):
        vector_copy(b).wait_recv()
        vec[b + 1] = vec[b] + vec_in[b]
        if b + 1 < len(partners):
            vector_copy(b + 1).start()

    def send_weights(items):
        for n in items:
            for k in range(1, half):
                weight_copy(k, n).start()

    def own_weights(items):
        for n in items:
            local_w[n].wait()

    def far_weights(items):
        for n in items:
            for k in range(1, half):
                weight_copy(k, n).wait_recv()

    def far(a, what):
        for h in range(2):
            getattr(far_copy(a, h), what)()

    attention_part, mlp_part = (0, 1, 2, 5), (3, 4)
    local_w = [pltpu.make_async_copy(s, d, w_local.at[n]) for n, (s, d) in enumerate(slab(n, 0) for n in range(6))]
    for h in range(2):
        forward(0, 0, h, 0)
    vec[0] = vectors[...]
    vector_copy(0).start()
    for k in range(1, half):
        bias_copy(k).start()
    for c in local_w:
        c.start()
    for b in range(spread_bits):
        vector_step(b)

    send_weights(attention_part)
    far(0, "start")
    far(1, "start")
    send_weights(mlp_part)
    vector_step(spread_bits)
    for h in range(2):
        forward(0, 1, h, 0)

    order = [j for p in range(ways // 2) for j in (p, p + ways // 2)]

    def load(s, n, first):
        slot, j = n % 2, order[n]
        for a in range(2):
            for h in range(2):
                if first:
                    src = source(s, a, h, j)
                else:
                    src = (normed_all, cot_all)[a].at[s, span(h, j), :]
                pltpu.make_async_copy(src, xb.at[slot, a, pl.ds(h * hb, hb), :], load_sem.at[slot, a, h]).start()

    def outputs(slot, s, j, first, units_of, size=1):
        copies = []
        for h in range(2):
            rows, to = pl.ds(h * hb * size, hb * size), span(h, j, size)
            pairs = []
            if first:
                pairs += [
                    (nb.at[slot, rows, :], normed_all.at[s, to, :]),
                    (qb.at[slot, :, rows, :], qkv_all.at[:, s, to, :]),
                    (gb.at[slot, rows, :], g_all.at[s, to, :]),
                ]
            for r in units_of:
                pairs.append((apb.at[slot, 0, r, rows, :], shard_of(acts, r, s, to)))
                pairs.append((apb.at[slot, 1, r, rows, :], shard_of(pres, r, s, to)))
            for n, (x, y) in enumerate(pairs):
                copies.append(pltpu.make_async_copy(x, y, out_sem.at[slot, h, n]))
        return copies

    def attention_rows(slot):
        x = xb[slot, 0, : 2 * hb].astype(F32)
        centred = x - jnp.mean(x, -1, keepdims=True)
        inv = lax.rsqrt(jnp.mean(centred * centred, -1, keepdims=True) + EPSILON)
        nb[slot] = (centred * inv * gain() + shift()).astype(BF16)
        thirds = wide(nb[slot], wg.at[0 : 3 * part], [0, part, 2 * part, 3 * part])
        for n, y in enumerate(thirds):
            qb[slot, n] = y + bias[n : n + 1, :part]
        gb[slot] = dot_nt(xb[slot, 1, : 2 * hb], wo[0:part, :]).astype(BF16)

    def mlp_rows(slot, normed, cot, r, count):
        b1 = biases if r == 0 else bias_in.at[half - r - 1]
        pre = dot_nt(normed, wg[3 * part + r * hidden : 3 * part + (r + 1) * hidden, :]) + b1[3:4, :hidden]
        act, slope = gelu_pair(pre)
        apb[slot, 0, r, :count] = act.astype(BF16)
        grad = dot_nt(cot, wo[part + r * hidden : part + (r + 1) * hidden, :]) * slope
        b1_out[r : r + 1, :] += jnp.sum(grad, 0, keepdims=True)
        apb[slot, 1, r, :count] = grad.astype(BF16)

    def loaded(slot):
        for a in range(2):
            for h in range(2):
                pltpu.make_async_copy(
                    own[a].at[pl.ds(h * hb, hb), :], xb.at[slot, a, pl.ds(h * hb, hb), :], load_sem.at[slot, a, h]
                ).wait()

    def run(s, units_of, before_load):
        before_load(0)
        load(s, 0, True)

        def block(k, _):
            slot = k % 2
            j = k // 2 + (k % 2) * (ways // 2)
            for n in range(1, ways):
                @pl.when(k + 1 == n)
                def _():
                    before_load(n)
                    load(s, n, True)

            loaded(slot)

            @pl.when(k >= 2)
            def _():
                for c in outputs(slot, s, j, True, units_of):
                    c.wait()

            attention_rows(slot)
            for r in units_of:
                mlp_rows(slot, nb[slot], xb[slot, 1, : 2 * hb], r, 2 * hb)
            for c in outputs(slot, s, j, True, units_of):
                c.start()
            if s == 0:
                @pl.when(k == 0)
                def _():
                    copies = [
                        pltpu.make_async_copy(
                            xb.at[0, 1, pl.ds(h * hb, hb), :], cot_all.at[0, span(h, 0), :], load_sem.at[0, 1, h]
                        )
                        for h in range(2)
                    ]
                    for c in copies:
                        c.start()
                    for c in copies:
                        c.wait()

            return 0

        lax.fori_loop(0, ways, block, 0)
        for slot in range(2):
            for c in outputs(slot, s, order[ways - 2 + slot], True, units_of):
                c.wait()

    def rerun(first, count, units_of):
        per = ways // 2

        def copies(k):
            s, p, slot = k // per, 2 * (k % per), k % 2
            return [
                pltpu.make_async_copy(
                    x.at[s, span(h, p, 2), :], xb.at[slot, a, pl.ds(2 * h * hb, 2 * hb), :], load_sem.at[slot, a, h]
                )
                for a, x in enumerate((normed_all, cot_all))
                for h in range(2)
            ]

        def stores(k):
            return outputs(k % 2, k // per, 2 * (k % per), False, units_of, 2)

        for c in copies(first):
            c.start()

        def block(k, _):
            slot = k % 2
            for c in copies(k):
                c.wait()

            @pl.when(k + 1 < first + count)
            def _():
                for c in copies(k + 1):
                    c.start()

            @pl.when(k >= first + 2)
            def _():
                for c in stores(k):
                    c.wait()

            for r in units_of:
                mlp_rows(slot, xb[slot, 0], xb[slot, 1], r, 4 * hb)
            for c in stores(k):
                c.start()
            return 0

        lax.fori_loop(first, first + count, block, 0)
        for k in range(first + count - 2, first + count):
            for c in stores(k):
                c.wait()

    vector_step(spread_bits + 1)
    relay(0, 1)

    for b in range(spread_bits + 2, len(partners)):
        vector_step(b)
    vectors_out[...] = vec[len(partners)]
    gain = lambda: vec[len(partners), 0:1, :]
    shift = lambda: vec[len(partners), 1:2, :]
    for k in range(1, half):
        bias_copy(k).wait_recv()
    bias = biases[...]
    for k in range(1, half):
        bias = bias + bias_in[k - 1]
    own_weights(attention_part + mlp_part)
    far_weights(attention_part)
    b1_out[...] = jnp.zeros_like(b1_out)

    def rows_of_own(n):
        p = order[n]
        if p >= ways // 2:
            for a in range(2):
                for h in range(2):
                    arrived(0, a, h, p)
        elif p >= 2:
            relay(0, p)
        if p == ways // 2 - 1:
            far(0, "wait_recv")
            for h in range(2):
                forward(1, 0, h, 0)

    run(0, (), rows_of_own)

    def hook(i, count):
        @pl.when(i == count // 2)
        def _():
            far(1, "wait_recv")
            for h in range(2):
                forward(1, 1, h, 0)

        @pl.when(i == count - 1)
        def _():
            relay(1, 1, (0,))

    bias_out[...] = jnp.zeros_like(bias_out)
    length = 2 * ways * hb
    block_rows = min(512, length)
    chunks = [pl.multiple_of((2 * at.device_of(h, p) + h) * hb, hb) for h in range(2) for p in range(ways)]
    pl.run_scoped(
        lambda *scratch: attention_core(
            heads, head_dim, block_rows, chunks, 0, qkv_all, g_all, cos_ref, neg_ref, pos_ref,
            o_out, dqkv_out, bias_out, hook, *scratch,
        ),
        *attention_scratch(heads, length, part, block_rows, len(chunks)),
    )
    rerun(0, ways // 2, (0,))
    relay(1, 1, (1,))

    def rows_of_partner(n):
        p = order[n]
        if p >= ways // 2:
            for a in range(2):
                for h in range(2):
                    arrived(1, a, h, p)
        elif p >= 2:
            relay(1, p)

    run(1, (0,), rows_of_partner)
    far_weights(mlp_part)
    weights_out = [pltpu.make_async_copy(x, y, w_out_sem.at[n]) for n, (x, y) in enumerate(((wg, wg_out), (wo, wo_out)))]
    for c in weights_out:
        c.start()
    rerun(0, ways, tuple(range(1, half)))
    for c in weights_out:
        c.wait()
    for k, n in weight_copies:
        weight_copy(k, n).wait_send()
    for k in range(1, half):
        bias_copy(k).wait_send()
    for b in range(len(partners)):
        vector_copy(b).wait_send()

    for a in range(2):
        far(a, "wait_send")
    for a in range(2):
        for h in range(2):
            for s in range(2):
                for p in range(ways):
                    for t in range(p.bit_length(), steps):
                        row_copy(s, a, h, p, t).wait_send()


def front(ways, spread, heads, head_dim, tok, cot, qkv_w, w1, dense_w, w2, vectors, biases, tables):
    rows, width = tok.shape
    half = spread // 2
    length = rows * ways
    part, units = dense_w.shape[0] * half, w2.shape[0] * half
    arrays = 1 if w2.shape[0] % 128 == 0 else half
    hops = (spread * ways).bit_length() - 1
    hbm = pl.BlockSpec(memory_space=pl.ANY)
    vmem = pl.BlockSpec(memory_space=pltpu.VMEM)
    shape = jax.ShapeDtypeStruct
    dma = pltpu.SemaphoreType.DMA
    return pl.pallas_call(
        functools.partial(front_kernel, ways, spread, heads, head_dim),
        out_shape=(
            shape((2, length, width), BF16),
            shape((2, length, width), BF16),
            shape((2, length, width), BF16),
            shape((3, 2, length, part), F32),
            shape((2, length, part), BF16),
            shape((3 * part + units, width), BF16),
            shape((part + units, width), BF16),
            shape((1, length, part), BF16),
            shape((3, 1, length, part), BF16),
            shape((half, units // half), F32),
            shape(vectors.shape, F32),
            shape((3, part), F32),
        )
        + (shape((2, length, units // arrays), BF16),) * (2 * arrays),
        in_specs=[hbm] * 6 + [vmem] * 5,
        out_specs=(hbm,) * 9 + (vmem,) * 3 + (hbm,) * (2 * arrays),
        scratch_shapes=[
            pltpu.VMEM((3 * part + units, width), BF16),
            pltpu.VMEM((part + units, width), BF16),
            pltpu.VMEM((2, 2, 2 * rows, width), BF16),
            pltpu.VMEM((2, rows, width), BF16),
            pltpu.VMEM((2, 3, rows, part), F32),
            pltpu.VMEM((2, rows, part), BF16),
            pltpu.VMEM((2, 2, half, 2 * rows, units // half), BF16),
            pltpu.VMEM((hops + 1,) + vectors.shape, F32),
            pltpu.VMEM((hops,) + vectors.shape, F32),
            pltpu.VMEM((max(half - 1, 1),) + biases.shape, F32),
            dma((2, 2, 2, ways)),
            dma((2, 2, 2, ways)),
            dma((2, 2)),
            dma((2, 2)),
            dma((max(half - 1, 1), 6)),
            dma((max(half - 1, 1), 6)),
            dma((6,)),
            dma((2, 2, 2)),
            dma((2, 2, 3 + 2 * half)),
            dma((2,)),
            dma((hops,)),
            dma((hops,)),
            dma((max(half - 1, 1),)),
            dma((max(half - 1, 1),)),
        ],
        compiler_params=pltpu.CompilerParams(collective_id=1, has_side_effects=True, vmem_limit_bytes=60 << 20),
        name="front",
    )(tok, cot, qkv_w, w1, dense_w, w2, vectors, biases, *tables)


def attention_core(
    heads, head_dim, block, chunks, seq, qkv_in, g_in, cos_ref, neg_ref, pos_ref, o_out, dqkv_out, bias_out,
    hook, stage, q, k, v, g, kt, vt, gt, dk, dv, dq, o, scores, in_sem, out_sem,
):
    length, width = q.shape
    half = ROT // 2
    scale = head_dim ** (-0.5)
    count = length // block
    chunk = length // len(chunks)
    loads = []
    for r, start in enumerate(chunks):
        rows, here = pl.ds(start, chunk), pl.ds(r * chunk, chunk)
        loads.append(pltpu.make_async_copy(qkv_in.at[:, seq, here, :], stage.at[:, rows, :], in_sem.at[r, 0]))
        loads.append(pltpu.make_async_copy(g_in.at[seq, here, :], g.at[rows, :], in_sem.at[r, 1]))
    for c in loads:
        c.start()
    for c in loads:
        c.wait()

    def prepare(at, _):
        rows = aligned(at * block, block)
        cos, neg, pos = cos_ref[rows, :], neg_ref[rows, :], pos_ref[rows, :]

        def rotate(x):
            return x * cos + pltpu.roll(x, width - half, 1) * neg + pltpu.roll(x, half, 1) * pos

        q[rows, :] = rotate(stage[0, rows, :]).astype(BF16) * scale
        kb = rotate(stage[1, rows, :]).astype(BF16)
        vb = stage[2, rows, :].astype(BF16)
        k[rows, :] = kb
        v[rows, :] = vb
        kt[:, rows] = kb.T
        vt[:, rows] = vb.T
        gt[:, rows] = g[rows, :].T
        dk[rows, :] = jnp.zeros((block, width), F32)
        dv[rows, :] = jnp.zeros((block, width), F32)
        return 0

    lax.fori_loop(0, count, prepare, 0)
    lane = lax.broadcasted_iota(jnp.int32, (block, width), 1)

    def only(x, h):
        if heads == 1:
            return x
        keep = (lane >= h * head_dim) & (lane < (h + 1) * head_dim)
        return jnp.where(keep, x.astype(F32), 0.0).astype(BF16)

    def one_block(i, _):
        hook(i, count)
        mine = aligned(i * block, block)
        qi, gi = q[mine, :], g[mine, :]
        qh, gh = [only(qi, h) for h in range(heads)], [only(gi, h) for h in range(heads)]
        row = lax.broadcasted_iota(jnp.int32, (width, block), 0)
        every = range(heads)

        def first(j, tops):
            cols = aligned(j * block, block)
            s = [dot_nt(k[cols, :], qh[h]) for h in every]
            for h in every:
                scores[h, cols, :] = s[h]
            return tuple(jnp.maximum(tops[h], jnp.max(s[h], 0, keepdims=True)) for h in every)

        tops = lax.fori_loop(0, i, first, tuple(jnp.full((1, block), -1e30, F32) for h in every))
        key_at = lax.broadcasted_iota(jnp.int32, (block, block), 0)
        query_at = lax.broadcasted_iota(jnp.int32, (block, block), 1)
        last = [jnp.where(key_at <= query_at, dot_nt(k[mine, :], qh[h]), -1e30) for h in every]
        for h in every:
            scores[h, mine, :] = last[h]
        tops = [jnp.maximum(tops[h], jnp.max(last[h], 0, keepdims=True)) for h in every]

        def second(j, carry):
            totals, accs = carry
            cols = aligned(j * block, block)
            e = [jnp.exp(scores[h, cols, :] - tops[h]) for h in every]
            for h in every:
                scores[h, cols, :] = e[h]
            return (
                tuple(totals[h] + jnp.sum(e[h], 0, keepdims=True) for h in every),
                tuple(accs[h] + dot_nn(vt[:, cols], e[h].astype(BF16)) for h in every),
            )

        nothing = tuple(jnp.zeros((width, block), F32) for h in every)
        totals, accs = lax.fori_loop(
            0, i + 1, second, (tuple(jnp.zeros((1, block), F32) for h in every), nothing)
        )
        inv = [1.0 / totals[h] for h in every]
        here = [(row >= h * head_dim) & (row < (h + 1) * head_dim) for h in every]
        accs = [jnp.where(here[h], (accs[h] * inv[h]).astype(BF16).astype(F32), 0.0) for h in every]
        gti = gt[:, mine].astype(F32)
        delta = [jnp.sum(accs[h] * gti, 0, keepdims=True) for h in every]
        ob = functools.reduce(jnp.add, accs)

        def third(j, acc_q):
            cols = aligned(j * block, block)
            p = [scores[h, cols, :] * inv[h] for h in every]
            dp = [dot_nt(v[cols, :], gh[h]) for h in every]
            dv[cols, :] += functools.reduce(jnp.add, [dot_nn(p[h].astype(BF16), gh[h]) for h in every])
            ds = [(p[h] * (dp[h] - delta[h])).astype(BF16) for h in every]
            dk[cols, :] += functools.reduce(jnp.add, [dot_nn(ds[h], qh[h]) for h in every])
            return tuple(acc_q[h] + dot_nn(kt[:, cols], ds[h]) for h in every)

        acc_q = lax.fori_loop(0, i + 1, third, nothing)
        dqb = functools.reduce(jnp.add, [jnp.where(here[h], acc_q[h], 0.0) for h in every])
        o[mine, :] = ob.T.astype(BF16)
        dq[mine, :] = dqb.T * scale
        return 0

    lax.fori_loop(0, count, one_block, 0)

    def finish(at, sums):
        rows = aligned(at * block, block)
        cos, neg, pos = cos_ref[rows, :], neg_ref[rows, :], pos_ref[rows, :]

        def unrotate(x):
            return x * cos - pltpu.roll(x, width - half, 1) * neg - pltpu.roll(x, half, 1) * pos

        a = unrotate(dq[rows, :].astype(BF16).astype(F32))
        b = unrotate(dk[rows, :].astype(BF16).astype(F32))
        c = dv[rows, :].astype(BF16).astype(F32)
        q[rows, :] = a.astype(BF16)
        k[rows, :] = b.astype(BF16)
        v[rows, :] = c.astype(BF16)
        return tuple(s + jnp.sum(x, 0, keepdims=True) for s, x in zip(sums, (a, b, c)))

    sums = lax.fori_loop(0, count, finish, tuple(jnp.zeros((1, width), F32) for _ in range(3)))
    bias_out[...] += jnp.concatenate(list(sums), 0)
    stores = []
    for r, start in enumerate(chunks):
        rows, here = pl.ds(start, chunk), pl.ds(r * chunk, chunk)
        for n, src in enumerate((q, k, v)):
            stores.append(pltpu.make_async_copy(src.at[rows, :], dqkv_out.at[n, 0, here, :], out_sem.at[r, n]))
        stores.append(pltpu.make_async_copy(o.at[rows, :], o_out.at[0, here, :], out_sem.at[r, 3]))
    for c in stores:
        c.start()
    for c in stores:
        c.wait()


def attention_scratch(heads, length, part, block, chunks):
    return (
        [pltpu.VMEM((3, length, part), F32)]
        + [pltpu.VMEM((length, part), BF16)] * 4
        + [pltpu.VMEM((part, length), BF16)] * 3
        + [pltpu.VMEM((length, part), F32)] * 3
        + [
            pltpu.VMEM((length, part), BF16),
            pltpu.VMEM((heads, length, block), F32),
            pltpu.SemaphoreType.DMA((chunks, 2)),
            pltpu.SemaphoreType.DMA((chunks, 4)),
        ]
    )


def joined(xs, w):
    if all(x.shape[1] % 128 == 0 for x in xs):
        return dot_nn(jnp.concatenate(xs, 1), w[...])
    total, at = None, 0
    for x in xs:
        y = dot_nn(x, w[at : at + x.shape[1], :])
        total, at = (y if total is None else total + y), at + x.shape[1]
    return total


def rest_kernel(
    ways, spread, heads, head_dim,
    qkv_all, g_all, normed_all, cot_all, wg_in, wo_in, o_0, dqkv_0, tok_own, cot_own, cos_ref, neg_ref, pos_ref, norm_ref, *more,
):
    at = Layout(ways, spread)
    half, steps, orders = at.half, at.steps, at.orders
    arrays = (len(more) - 32) // 2
    acts, pres = more[:arrays], more[arrays : 2 * arrays]
    (
        o_1, dqkv_1, recv, far_sum, dw_own, dw_recv, dw_low, out_rows, grad_rows, bias_out, vec_out,
        wg, wo, keep, stage_send, stage_recv, ob, db, apb, vec, vec_in,
        w_sem, load_sem, rs_send, rs_recv, add_sem, far_send, far_recv, dw_send, dw_come, vec_send, vec_recv,
    ) = more[2 * arrays :]
    hb = keep.shape[4]
    length = 2 * ways * hb
    part = g_all.shape[2]
    shard = part // half
    block = min(512, length)
    width = keep.shape[5]
    at.meet()
    loads = [pltpu.make_async_copy(x, y, w_sem.at[n]) for n, (x, y) in enumerate(((wg_in, wg), (wo_in, wo)))]
    for c in loads:
        c.start()
    bias_out[...] = jnp.zeros_like(bias_out)
    chunks = [
        pl.multiple_of((2 * at.device_of(h, p) + h) * hb, hb) for h in range(2) for p in range(ways)
    ]

    def span(h, p):
        return aligned((h * ways + p) * hb, hb)

    def from_heads(s, pick, o_dst, dqkv_dst, o_sem, dqkv_sem):
        for v, (x, y) in enumerate(((o_0, dqkv_0), (o_1, dqkv_1))):
            @pl.when(s == v)
            def _():
                pltpu.make_async_copy(x.at[0, pick, :], o_dst, o_sem).start()
                pltpu.make_async_copy(y.at[:, 0, pick, :], dqkv_dst, dqkv_sem).start()

    def heads_there(pick, o_dst, dqkv_dst, o_sem, dqkv_sem):
        pltpu.make_async_copy(o_1.at[0, pick, :], o_dst, o_sem).wait()
        pltpu.make_async_copy(dqkv_1.at[:, 0, pick, :], dqkv_dst, dqkv_sem).wait()

    def sent(s, t, h, q, src):
        level = q.bit_length() - 1 if isinstance(q, int) else steps - 1
        return remote(src, recv.at[s, t, h, q], rs_send.at[s, t, h, q], rs_recv.at[s, t, h, q], at.near(orders[h][level]))

    def partial_sums(s):
        def place(i):
            return jnp.where(i < ways // 2, ways // 2 + i, ways - 1 - i)

        def heads_of(i, h):
            slot, rows = i % 2, pl.ds(h * hb, hb)
            return (
                span(h, place(i)), ob.at[slot, rows, :], db.at[slot, :, rows, :],
                load_sem.at[slot, h, 0], load_sem.at[slot, h, 1],
            )

        def act_copies(i, h):
            slot, rows = i % 2, pl.ds(h * hb, hb)
            return [
                pltpu.make_async_copy(
                    shard_of(x, r, s, span(h, place(i))), apb.at[slot, n, r, rows, :], load_sem.at[slot, h, 2 + n * half + r]
                )
                for n, x in enumerate((acts, pres))
                for r in range(half)
            ]

        def fetch(i):
            for h in range(2):
                from_heads(s, *heads_of(i, h))
                for c in act_copies(i, h):
                    c.start()

        def sends(i):
            return [sent(s, t, h, place(i), stage_send.at[i % 2, t, h]) for t in range(2) for h in range(2)]

        fetch(0)

        def one(i, _):
            slot = i % 2
            for h in range(2):
                heads_there(*heads_of(i, h))
                for c in act_copies(i, h):
                    c.wait()

            @pl.when(i + 1 < ways)
            def _():
                fetch(i + 1)

            @pl.when((i == 1) & (s == 0))
            def _():
                for q in range(ways // 2 - 1, ways // 4, -1):
                    serve(1, q, 0)
                send_held(1, 1)

            @pl.when((i >= 2) & (i < ways // 2 + 2))
            def _():
                for c in sends(i - 2):
                    c.wait_send()

            out = joined([ob[slot]] + [apb[slot, 0, r] for r in range(half)], wo).astype(BF16)
            grad = joined([db[slot, n] for n in range(3)] + [apb[slot, 1, r] for r in range(half)], wg).astype(BF16)

            @pl.when(i < ways // 2)
            def _():
                for t, x in enumerate((grad, out)):
                    for h in range(2):
                        stage_send[slot, t, h] = x[h * hb : (h + 1) * hb, :]
                for c in sends(i):
                    c.start()

            @pl.when(i >= ways // 2)
            def _():
                for t, x in enumerate((grad, out)):
                    for h in range(2):
                        keep[s, t, h, ways - 1 - i] = x[h * hb : (h + 1) * hb, :]

            for n in range(ways // 2):
                @pl.when(i == ways // 2 + n)
                def _():
                    serve_both(s, ways - 1 - n)

            return 0

        lax.fori_loop(0, ways, one, 0)

    def far_copy(t, h):
        return remote(keep.at[1, t, h, 0], far_sum.at[t, h], far_send.at[t, h], far_recv.at[t, h], at.far)

    def serve(s, q, t):
        level = q.bit_length() - 1
        p = q - (1 << level)
        come = [pltpu.make_async_copy(recv.at[s, t, h, q], stage_recv.at[t, h], add_sem.at[t, h]) for h in range(2)]
        for h, c in enumerate(come):
            sent(s, t, h, q, stage_recv.at[t, h]).wait_recv()
            c.start()
        for h, c in enumerate(come):
            c.wait()
            keep[s, t, h, p] = (keep[s, t, h, p].astype(F32) + stage_recv[t, h].astype(F32)).astype(BF16)
            if p and p.bit_length() == level:
                if level == steps - 1:
                    @pl.when((s == 1) & (t == 0))
                    def _():
                        sent(s, t, h, p, keep.at[s, t, h, p]).start()
                else:
                    sent(s, t, h, p, keep.at[s, t, h, p]).start()
            if q == 1 and s == 1:
                far_copy(t, h).start()

    def serve_both(s, q):
        def body(t, _):
            serve(s, q, t)
            return 0

        lax.fori_loop(0, 2, body, 0)

    def send_held(s, t):
        for p in range(ways // 2 - 1, ways // 4 - 1, -1):
            for h in range(2):
                sent(s, t, h, p, keep.at[s, t, h, p]).start()

    def shard_copy(k):
        cut = aligned(at.peer_at[k - 1] * shard, shard)
        return remote(dw_low.at[:, cut, :], dw_recv.at[k - 1], dw_send.at[k - 1], dw_come.at[k - 1], at.peers[k - 1])

    def weight_sums(hook):
        rows = min(512, length)
        per = length // rows

        def body(nbuf, cbuf, abuf, acc, rounded, sems, out_sem):
            def heads_of(i):
                slot = i % 2
                return aligned((i % per) * rows, rows), abuf.at[slot, 3], abuf.at[slot, 0:3], sems.at[slot, 3], sems.at[slot, 2]

            def copies(i):
                slot, s, here = i % 2, i // per, aligned((i % per) * rows, rows)
                return [
                    pltpu.make_async_copy(normed_all.at[s, here, :], nbuf.at[slot], sems.at[slot, 0]),
                    pltpu.make_async_copy(cot_all.at[s, here, :], cbuf.at[slot], sems.at[slot, 1]),
                ]

            def fetch(i):
                for c in copies(i):
                    c.start()
                from_heads(i // per, *heads_of(i))

            fetch(0)
            acc[...] = jnp.zeros_like(acc)

            def one(i, _):
                slot = i % 2
                for c in copies(i):
                    c.wait()
                heads_there(*heads_of(i))

                @pl.when(i + 1 < 2 * per)
                def _():
                    fetch(i + 1)

                hook(i, 2 * per)
                normed = nbuf[slot]
                if part % 128 == 0:
                    y = dot_tn(jnp.concatenate([abuf[slot, n] for n in range(3)], 1), normed)
                    for n in range(3):
                        acc[n] += y[n * part : (n + 1) * part, :]
                else:
                    for n in range(3):
                        acc[n] += dot_tn(abuf[slot, n], normed)
                acc[3] += dot_tn(abuf[slot, 3], cbuf[slot])
                return 0

            lax.fori_loop(0, 2 * per, one, 0)
            own = pltpu.make_async_copy(acc.at[:, aligned(at.g * shard, shard), :], dw_own, out_sem.at[0])
            own.start()
            rounded[...] = acc[...].astype(BF16)
            others = pltpu.make_async_copy(rounded, dw_low, out_sem.at[1])
            others.start()
            others.wait()
            own.wait()

        width_of = pltpu.VMEM((2, rows, width), BF16)
        pl.run_scoped(
            body, width_of, width_of, pltpu.VMEM((2, 4, rows, part), BF16),
            pltpu.VMEM((4, part, width), F32), pltpu.VMEM((4, part, width), BF16),
            pltpu.SemaphoreType.DMA((2, 4)), pltpu.SemaphoreType.DMA((2,)),
        )
        for k in range(1, half):
            shard_copy(k).start()

    pl.run_scoped(
        lambda *scratch: attention_core(
            heads, head_dim, block, chunks, 1, qkv_all, g_all, cos_ref, neg_ref, pos_ref,
            o_1, dqkv_1, bias_out, lambda i, count: None, *scratch,
        ),
        *attention_scratch(heads, length, part, block, len(chunks)),
    )
    for c in loads:
        c.wait()

    def one_sequence(turn, _):
        partial_sums(1 - turn)
        return 0

    lax.fori_loop(0, 2, one_sequence, 0)

    for q in range(ways // 4, 0, -1):
        serve(1, q, 0)
    for q in range(ways // 2 - 1, ways // 4, -1):
        serve(1, q, 1)
    for t in range(2):
        send_held(0, t)

    def output_rows_back(i, count):
        @pl.when(i == count // 2)
        def _():
            for q in range(ways // 4, 1, -1):
                serve(1, q, 1)

        @pl.when(i == count - 1)
        def _():
            serve(1, 1, 1)

    weight_sums(output_rows_back)
    for q in range(ways // 2 - 1, 0, -1):
        serve_both(0, q)
    for k in range(1, half):
        shard_copy(k).wait()
    for t in range(2):
        for h in range(2):
            far_copy(t, h).wait()
    partners = [{"fsdp": flip(at.f, 1 << b)} for b in range(spread.bit_length() - 1)] + [at.near(b) for b in range(steps)]

    def vector_copy(b):
        return remote(vec.at[b], vec_in.at[b], vec_send.at[b], vec_recv.at[b], partners[b])

    def norm_backward(far, tok, cot, out_buf, grad_buf, sems):
        loads = [
            pltpu.make_async_copy(far_sum, far, sems.at[0]),
            pltpu.make_async_copy(tok_own, tok, sems.at[1]),
            pltpu.make_async_copy(cot_own, cot, sems.at[2]),
        ]
        for c in loads:
            c.start()
        for c in loads:
            c.wait()
        gain = norm_ref[0:1, :]
        biases = norm_ref[2:3, :] + norm_ref[3:4, :]
        sums = [jnp.zeros((1, width), F32)] * 3
        for h in range(2):
            rows = slice(h * hb, (h + 1) * hb)
            x, c = tok[rows, :].astype(F32), cot[rows, :].astype(F32)
            xhat, inv = normalize(x)
            grad = keep[0, 0, h, 0].astype(F32) + far[0, h].astype(F32)
            out_buf[rows, :] = (x + keep[0, 1, h, 0].astype(F32) + far[1, h].astype(F32) + biases).astype(BF16)
            scaled = grad * gain
            inner = inv * (
                scaled
                - jnp.mean(scaled, -1, keepdims=True)
                - xhat * jnp.mean(scaled * xhat, -1, keepdims=True)
            )
            grad_buf[rows, :] = (c + inner).astype(BF16)
            sums = [a + jnp.sum(b, 0, keepdims=True) for a, b in zip(sums, (grad * xhat, grad, c))]
        eighth = width // 8
        vec[0] = jnp.concatenate(
            [jnp.concatenate([x[:, n * eighth : (n + 1) * eighth] for n in range(8)], 0) for x in sums], 1
        )
        vector_copy(0).start()
        stores = [
            pltpu.make_async_copy(out_buf, out_rows, sems.at[0]), pltpu.make_async_copy(grad_buf, grad_rows, sems.at[1])
        ]
        for c in stores:
            c.start()
        for b in range(len(partners)):
            vector_copy(b).wait_recv()
            vec[b + 1] = vec[b] + vec_in[b]
            if b + 1 < len(partners):
                vector_copy(b + 1).start()
        vec_out[...] = vec[len(partners)]
        for c in stores:
            c.wait()

    buf = pltpu.VMEM((2 * hb, width), BF16)
    pl.run_scoped(norm_backward, pltpu.VMEM((2, 2, hb, width), BF16), buf, buf, buf, buf, pltpu.SemaphoreType.DMA((3,)))
    for b in range(len(partners)):
        vector_copy(b).wait_send()
    for t in range(2):
        for h in range(2):
            for s in range(2):
                for p in range(1, ways // 2):
                    sent(s, t, h, p, keep.at[s, t, h, p]).wait_send()


def rest(ways, spread, heads, head_dim, qkv_all, g_all, normed_all, cot_all, wg, wo, o_0, dqkv_0, tok, cot, tables, norm, acts, pres):
    _, length, width = normed_all.shape
    half = spread // 2
    part, hidden = g_all.shape[2], sum(x.shape[2] for x in acts) // half
    hb = length // ways // 2
    shard = part // half
    rows = 2 * hb
    hops = (spread * ways).bit_length() - 1
    hbm = pl.BlockSpec(memory_space=pl.ANY)
    vmem = pl.BlockSpec(memory_space=pltpu.VMEM)
    shape = jax.ShapeDtypeStruct
    dma = pltpu.SemaphoreType.DMA
    return pl.pallas_call(
        functools.partial(rest_kernel, ways, spread, heads, head_dim),
        out_shape=(
            shape((1, length, part), BF16),
            shape((3, 1, length, part), BF16),
            shape((2, 2, 2, ways, hb, width), BF16),
            shape((2, 2, hb, width), BF16),
            shape((4, shard, width), F32),
            shape((max(half - 1, 1), 4, shard, width), BF16),
            shape((4, part, width), BF16),
            shape((rows, width), BF16),
            shape((rows, width), BF16),
            shape((3, part), F32),
            shape((8, 3 * width // 8), F32),
        ),
        in_specs=[hbm] * 10 + [vmem] * 4 + [hbm] * (2 * len(acts)),
        out_specs=(hbm,) * 9 + (vmem,) * 2,
        scratch_shapes=[
            pltpu.VMEM(wg.shape, BF16),
            pltpu.VMEM(wo.shape, BF16),
            pltpu.VMEM((2, 2, 2, ways // 2, hb, width), BF16),
            pltpu.VMEM((2, 2, 2, hb, width), BF16),
            pltpu.VMEM((2, 2, hb, width), BF16),
            pltpu.VMEM((2, rows, part), BF16),
            pltpu.VMEM((2, 3, rows, part), BF16),
            pltpu.VMEM((2, 2, half, rows, hidden), BF16),
            pltpu.VMEM((hops + 1, 8, 3 * width // 8), F32),
            pltpu.VMEM((hops, 8, 3 * width // 8), F32),
            dma((2,)),
            dma((2, 2, 2 + 2 * half)),
            dma((2, 2, 2, ways)),
            dma((2, 2, 2, ways)),
            dma((2, 2)),
            dma((2, 2)),
            dma((2, 2)),
            dma((max(half - 1, 1),)),
            dma((max(half - 1, 1),)),
            dma((hops,)),
            dma((hops,)),
        ],
        compiler_params=pltpu.CompilerParams(collective_id=2, has_side_effects=True, vmem_limit_bytes=63 << 20),
        name="rest",
    )(qkv_all, g_all, normed_all, cot_all, wg, wo, o_0, dqkv_0, tok, cot, *tables, norm, *acts, *pres)


def normalize(rows):
    mean = jnp.mean(rows, -1, keepdims=True)
    centred = rows - mean
    inv = lax.rsqrt(jnp.mean(centred * centred, -1, keepdims=True) + EPSILON)
    return centred * inv, inv


def local(
    tokens, layer_norm_gain, layer_norm_bias, qkv_weight, qkv_bias, dense_weight, dense_bias,
    fc1_weight, fc1_bias, fc2_weight, fc2_bias, cotangent,
):
    shape = tokens.shape
    rows, width = shape[0] * shape[1], shape[2]
    head_dim = width // HEADS
    ways = lax.axis_size("seq")
    spread = lax.axis_size("fsdp")
    half = spread // 2
    length = rows * ways
    heads = HEADS // (2 * ways)
    shard, hidden = dense_weight.shape[0], fc2_weight.shape[0]
    part, units = shard * half, hidden * half
    me, f = lax.axis_index("seq"), lax.axis_index("fsdp")
    group = lax.rem(f, half)

    mine = jnp.stack([layer_norm_gain, layer_norm_bias, dense_bias, fc2_bias]).astype(F32)
    vectors = lax.dynamic_update_slice(jnp.zeros((8, width), F32), mine, (0, (me * spread + f) * mine.shape[1]))
    biases = jnp.zeros((8, max(part, units)), F32)
    biases = lax.dynamic_update_slice(biases, qkv_bias.astype(F32), (0, group * shard))
    biases = lax.dynamic_update_slice(biases, fc1_bias.astype(F32)[None], (3, 0))
    tok, cot = tokens.reshape(rows, width), cotangent.reshape(rows, width)
    tables = rotation_tables(length, head_dim, heads)
    _, cot_all, normed_all, qkv_all, g_all, wg, wo, o_0, dqkv_0, b1_sum, small, bias_0, *hidden_rows = front(
        ways, spread, heads, head_dim, tok, cot, qkv_weight.transpose(1, 2, 0), fc1_weight.transpose(1, 0), dense_weight,
        fc2_weight, vectors, biases, tables,
    )

    def to_peer(x, k):
        pairs = [(i, i - i % half + (i % half + k) % half) for i in range(spread)]
        return lax.ppermute(x, "fsdp", pairs)

    def cut(x, at, size, axis):
        return lax.dynamic_slice_in_dim(x, at * size, size, axis)

    arrays = len(hidden_rows) // 2
    acts, pres = hidden_rows[:arrays], hidden_rows[arrays:]
    flat = lambda x: x.reshape(2 * length, x.shape[-1])
    shard_at = lambda sums, r, axis: (
        sums[r] if len(sums) > 1 else lax.slice_in_dim(sums[0], r * hidden, (r + 1) * hidden, axis=axis)
    )
    fc1_sums = [dot_tn(flat(normed_all), flat(x)) for x in pres]
    fc2_sums = [dot_tn(flat(x), flat(cot_all)) for x in acts]
    peers = [(k, lax.rem(group + k, half)) for k in range(1, half)]
    fc1_out = [shard_at(fc1_sums, k, 1).astype(BF16) for k in range(1, half)]
    fc2_out = [shard_at(fc2_sums, k, 0).astype(BF16) for k in range(1, half)]
    fc1_in = [to_peer(x, k) for (k, _), x in zip(peers, fc1_out)]
    fc2_in = [to_peer(x, k) for (k, _), x in zip(peers, fc2_out)]
    b1_in = [to_peer(b1_sum[k].astype(BF16), k) for k, _ in peers]
    g_all, fc1_out, fc2_out, fc1_sums, fc2_sums = lax.optimization_barrier((g_all, fc1_out, fc2_out, fc1_sums, fc2_sums))
    _, _, _, _, dw_own, dw_in, _, output, tokens_grad, bias_1, sums = rest(
        ways, spread, heads, head_dim, qkv_all, g_all, normed_all, cot_all, wg, wo, o_0, dqkv_0, tok, cot, tables, small,
        acts, pres,
    )
    qkv_b_sum = bias_0 + bias_1
    total = lambda own, come: functools.reduce(lambda a, b: a + b.astype(F32), come, own)
    fc1_w_grad, fc2_w_grad = total(shard_at(fc1_sums, 0, 1), fc1_in), total(shard_at(fc2_sums, 0, 0), fc2_in)
    fc1_b_grad = total(b1_sum[0], b1_in)
    b_in = [to_peer(cut(qkv_b_sum, p, shard, 1).astype(BF16), k) for k, p in peers]
    qkv_b_grad = total(cut(qkv_b_sum, group, shard, 1), b_in)
    dw = total(dw_own, [dw_in[k] for k in range(half - 1)])
    qkv_w_grad, dense_w_grad = dw[:3].transpose(2, 0, 1), dw[3]

    piece, eighth = width // (ways * spread), width // 8
    first = (me * spread + f) * piece
    sums = lax.dynamic_slice(
        sums.reshape(8, 3, eighth), (first // eighth, 0, lax.rem(first, eighth)), (1, 3, piece)
    )[0]
    output, tokens_grad = output.reshape(shape), tokens_grad.reshape(shape)
    return (
        output, tokens_grad, sums[0], sums[1], qkv_w_grad, qkv_b_grad, dense_w_grad, sums[2],
        fc1_w_grad, fc1_b_grad, fc2_w_grad, sums[2],
    )


def solution(mesh):
    both = ("seq", "fsdp")
    rows = P("fsdp", "seq", None)
    return jax.shard_map(
        local,
        mesh=mesh,
        in_specs=(
            rows, P(both), P(both), P(None, None, both), P(None, both), P(both, None), P(both),
            P(None, both), P(both), P(both, None), P(both), rows,
        ),
        out_specs=(
            rows, rows, P(both), P(both), P(None, None, both), P(None, both), P(both, None), P(both),
            P(None, both), P(both), P(both, None), P(both),
        ),
        check_vma=False,
    )
```

```python
import functools
import math

import jax
import jax.numpy as jnp
from jax import lax
from jax.experimental import pallas as pl
from jax.experimental.pallas import tpu as pltpu
from jax.sharding import PartitionSpec as P

HEADS = 32
ROT = 32
EPSILON = 1e-05
GELU_C = math.sqrt(2.0 / math.pi)
BASE_LOG = math.log(10000.0)
F32 = jnp.float32
BF16 = jnp.bfloat16
MESH = pl.DeviceIdType.MESH


def dot_nn(left, right):
    return lax.dot_general(left, right, (((1,), (0,)), ((), ())), preferred_element_type=F32)


def dot_nt(left, right):
    return lax.dot_general(left, right, (((1,), (1,)), ((), ())), preferred_element_type=F32)


def dot_tn(left, right):
    return lax.dot_general(left, right, (((0,), (0,)), ((), ())), preferred_element_type=F32)


def gelu_pair(pre):
    t = jnp.tanh(GELU_C * (pre + 0.044715 * pre * pre * pre))
    value = 0.5 * pre * (1.0 + t)
    slope = 0.5 * (1.0 + t) + 0.5 * pre * (1.0 - t * t) * GELU_C * (1.0 + 3.0 * 0.044715 * pre * pre)
    return value, slope


def xor_perm(size, mask):
    return [(i, i ^ mask) for i in range(size)]


def swap(x, axis, mask):
    return lax.ppermute(x, axis, xor_perm(lax.axis_size(axis), mask))


def bit_orders(ways):
    upper = list(range(1, ways.bit_length() - 1))
    last = [0] if ways > 1 else []
    return upper + last, upper[::-1] + last


def masks_of(order):
    masks = [0]
    for b in order:
        masks = masks + [m ^ (1 << b) for m in masks]
    return masks


def rotation_tables(length, head_dim, heads):
    half = ROT // 2
    inverse = jnp.exp(-(jnp.arange(half).astype(F32) * 2.0 / ROT) * BASE_LOG)
    angles = jnp.arange(length).astype(F32)[:, None] * inverse[None, :]
    cos, sin = jnp.cos(angles), jnp.sin(angles)
    zero = jnp.zeros_like(sin)
    rest = jnp.zeros((length, head_dim - ROT), F32)
    one_head = (
        jnp.concatenate([cos, cos, rest + 1.0], 1),
        jnp.concatenate([-sin, zero, rest], 1),
        jnp.concatenate([zero, sin, rest], 1),
    )
    return tuple(jnp.tile(t, (1, heads)) for t in one_head)


def flip(place, bit):
    return place + bit - 2 * bit * ((place // bit) % 2)


class Layout:
    def __init__(self, ways, spread):
        self.ways, self.spread, self.half = ways, spread, spread // 2
        self.steps = ways.bit_length() - 1
        self.orders = bit_orders(ways)
        self.masks = [masks_of(o) for o in self.orders]
        self.me, self.f = lax.axis_index("seq"), lax.axis_index("fsdp")
        self.g = self.f % self.half
        self.base = self.f - self.g
        self.far = {"fsdp": (self.f + self.half) % spread}
        self.peer_at = [(self.g + k) % self.half for k in range(1, self.half)]
        self.peers = [{"fsdp": self.base + p} for p in self.peer_at]

    def near(self, b):
        return {"seq": flip(self.me, 1 << b)}

    def device_of(self, h, p):
        place = self.me
        for b in range(self.steps):
            if (self.masks[h][p] >> b) & 1:
                place = flip(place, 1 << b)
        return place

    def meet(self):
        everyone = [self.near(b) for b in range(self.steps)] + [self.far] + self.peers
        barrier = pltpu.get_barrier_semaphore()
        for device in everyone:
            pl.semaphore_signal(barrier, inc=1, device_id=device, device_id_type=MESH)
        pl.semaphore_wait(barrier, len(everyone))


def remote(src, dst, send, recv, device):
    return pltpu.make_async_remote_copy(
        src_ref=src, dst_ref=dst, send_sem=send, recv_sem=recv, device_id=device, device_id_type=MESH
    )


def aligned(start, size, first=0):
    if isinstance(start, int):
        return pl.ds(first + start, size)
    return pl.ds(pl.multiple_of(first + start, math.gcd(first, size)), size)


def wide(x, w, cuts):
    if all(c % 128 == 0 for c in cuts):
        y = dot_nt(x, w[...])
        return [y[:, a:b] for a, b in zip(cuts, cuts[1:])]
    return [dot_nt(x, w[a:b, :]) for a, b in zip(cuts, cuts[1:])]


def shard_of(arrays, r, s, rows):
    if len(arrays) > 1:
        return arrays[r].at[s, rows, :]
    half = lax.axis_size("fsdp") // 2
    hidden = arrays[0].shape[2] // half
    return arrays[0].at[s, rows, pl.ds(r * hidden, hidden)]


def front_kernel(
    ways, spread, heads, head_dim,
    tok_own, cot_own, qkv_own, w1_own, dense_own, w2_own, vectors, biases, cos_ref, neg_ref, pos_ref,
    tok_all, cot_all, normed_all, qkv_all, g_all, wg_out, wo_out, o_out, dqkv_out, b1_out, vectors_out, bias_out, *more,
):
    at = Layout(ways, spread)
    half, steps, orders = at.half, at.steps, at.orders
    arrays = 1 if w2_own.shape[0] % 128 == 0 else half
    acts, pres = more[:arrays], more[arrays : 2 * arrays]
    (
        wg, wo, xb, nb, qb, gb, apb, vec, vec_in, bias_in,
        row_send, row_recv, far_send, far_recv, w_send, w_recv, w_local, load_sem, out_sem, w_out_sem,
        vec_send, vec_recv, bias_send, bias_recv,
    ) = more[2 * arrays :]
    hb = tok_own.shape[0] // 2
    shard, hidden = dense_own.shape[0], w2_own.shape[0]
    part, units = half * shard, half * hidden
    own, everything = (tok_own, cot_own), (tok_all, cot_all)
    at.meet()

    def span(h, p, size=1):
        start = (h * ways + p) * hb
        return pl.ds(start if isinstance(start, int) else pl.multiple_of(start, hb), hb * size)

    def source(s, a, h, p):
        if s == 0 and p == 0:
            return own[a].at[pl.ds(h * hb, hb), :]
        return everything[a].at[s, span(h, p), :]

    def row_copy(s, a, h, p, t):
        q = p + (1 << t)
        return remote(
            source(s, a, h, p), everything[a].at[s, span(h, q), :],
            row_send.at[s, a, h, q], row_recv.at[s, a, h, q], at.near(orders[h][t]),
        )

    def forward(s, a, h, p):
        for t in range(p.bit_length(), steps):
            row_copy(s, a, h, p, t).start()

    def arrived(s, a, h, p):
        t = p.bit_length() - 1
        row_copy(s, a, h, p - (1 << t), t).wait_recv()

    def relay(s, p, kinds=(0, 1)):
        for a in kinds:
            for h in range(2):
                arrived(s, a, h, p)
                forward(s, a, h, p)

    def far_copy(a, h):
        return remote(
            source(0, a, h, 0), everything[a].at[1, span(h, 0), :], far_send.at[a, h], far_recv.at[a, h], at.far
        )

    heads_at = aligned(at.g * shard, shard)

    def slab(n, r):
        if n < 3:
            return qkv_own.at[n], wg.at[aligned(at.g * shard, shard, n * part), :]
        if n == 3:
            return w1_own, wg.at[pl.ds(3 * part + r * hidden, hidden), :]
        if n == 4:
            return w2_own, wo.at[pl.ds(part + r * hidden, hidden), :]
        return dense_own, wo.at[heads_at, :]

    def weight_copy(k, n):
        src, dst = slab(n, half - k)
        return remote(src, dst, w_send.at[k - 1, n], w_recv.at[k - 1, n], at.peers[k - 1])

    weight_copies = [(k, n) for n in range(6) for k in range(1, half)]

    def bias_copy(k):
        return remote(biases, bias_in.at[k - 1], bias_send.at[k - 1], bias_recv.at[k - 1], at.peers[k - 1])

    spread_bits = spread.bit_length() - 1
    partners = [{"fsdp": flip(at.f, 1 << b)} for b in range(spread_bits)] + [at.near(b) for b in range(steps)]

    def vector_copy(b):
        return remote(vec.at[b], vec_in.at[b], vec_send.at[b], vec_recv.at[b], partners[b])

    def vector_step(b):
        vector_copy(b).wait_recv()
        vec[b + 1] = vec[b] + vec_in[b]
        if b + 1 < len(partners):
            vector_copy(b + 1).start()

    def send_weights(items):
        for n in items:
            for k in range(1, half):
                weight_copy(k, n).start()

    def own_weights(items):
        for n in items:
            local_w[n].wait()

    def far_weights(items):
        for n in items:
            for k in range(1, half):
                weight_copy(k, n).wait_recv()

    def far(a, what):
        for h in range(2):
            getattr(far_copy(a, h), what)()

    attention_part, mlp_part = (0, 1, 2, 5), (3, 4)
    local_w = [pltpu.make_async_copy(s, d, w_local.at[n]) for n, (s, d) in enumerate(slab(n, 0) for n in range(6))]
    for h in range(2):
        forward(0, 0, h, 0)
    vec[0] = vectors[...]
    vector_copy(0).start()
    for k in range(1, half):
        bias_copy(k).start()
    for c in local_w:
        c.start()
    for b in range(spread_bits):
        vector_step(b)

    send_weights(attention_part)
    far(0, "start")
    far(1, "start")
    send_weights(mlp_part)
    vector_step(spread_bits)
    for h in range(2):
        forward(0, 1, h, 0)

    order = [j for p in range(ways // 2) for j in (p, p + ways // 2)]

    def load(s, n, first):
        slot, j = n % 2, order[n]
        for a in range(2):
            for h in range(2):
                if first:
                    src = source(s, a, h, j)
                else:
                    src = (normed_all, cot_all)[a].at[s, span(h, j), :]
                pltpu.make_async_copy(src, xb.at[slot, a, pl.ds(h * hb, hb), :], load_sem.at[slot, a, h]).start()

    def outputs(slot, s, j, first, units_of, size=1):
        copies = []
        for h in range(2):
            rows, to = pl.ds(h * hb * size, hb * size), span(h, j, size)
            pairs = []
            if first:
                pairs += [
                    (nb.at[slot, rows, :], normed_all.at[s, to, :]),
                    (qb.at[slot, :, rows, :], qkv_all.at[:, s, to, :]),
                    (gb.at[slot, rows, :], g_all.at[s, to, :]),
                ]
            for r in units_of:
                pairs.append((apb.at[slot, 0, r, rows, :], shard_of(acts, r, s, to)))
                pairs.append((apb.at[slot, 1, r, rows, :], shard_of(pres, r, s, to)))
            for n, (x, y) in enumerate(pairs):
                copies.append(pltpu.make_async_copy(x, y, out_sem.at[slot, h, n]))
        return copies

    def attention_rows(slot):
        x = xb[slot, 0, : 2 * hb].astype(F32)
        centred = x - jnp.mean(x, -1, keepdims=True)
        inv = lax.rsqrt(jnp.mean(centred * centred, -1, keepdims=True) + EPSILON)
        nb[slot] = (centred * inv * gain() + shift()).astype(BF16)
        thirds = wide(nb[slot], wg.at[0 : 3 * part], [0, part, 2 * part, 3 * part])
        for n, y in enumerate(thirds):
            qb[slot, n] = y + bias[n : n + 1, :part]
        gb[slot] = dot_nt(xb[slot, 1, : 2 * hb], wo[0:part, :]).astype(BF16)

    def mlp_rows(slot, normed, cot, r, count):
        b1 = biases if r == 0 else bias_in.at[half - r - 1]
        pre = dot_nt(normed, wg[3 * part + r * hidden : 3 * part + (r + 1) * hidden, :]) + b1[3:4, :hidden]
        act, slope = gelu_pair(pre)
        apb[slot, 0, r, :count] = act.astype(BF16)
        grad = dot_nt(cot, wo[part + r * hidden : part + (r + 1) * hidden, :]) * slope
        b1_out[r : r + 1, :] += jnp.sum(grad, 0, keepdims=True)
        apb[slot, 1, r, :count] = grad.astype(BF16)

    def loaded(slot):
        for a in range(2):
            for h in range(2):
                pltpu.make_async_copy(
                    own[a].at[pl.ds(h * hb, hb), :], xb.at[slot, a, pl.ds(h * hb, hb), :], load_sem.at[slot, a, h]
                ).wait()

    def run(s, units_of, before_load):
        before_load(0)
        load(s, 0, True)

        def block(k, _):
            slot = k % 2
            j = k // 2 + (k % 2) * (ways // 2)
            for n in range(1, ways):
                @pl.when(k + 1 == n)
                def _():
                    before_load(n)
                    load(s, n, True)

            loaded(slot)

            @pl.when(k >= 2)
            def _():
                for c in outputs(slot, s, j, True, units_of):
                    c.wait()

            attention_rows(slot)
            for r in units_of:
                mlp_rows(slot, nb[slot], xb[slot, 1, : 2 * hb], r, 2 * hb)
            for c in outputs(slot, s, j, True, units_of):
                c.start()
            if s == 0:
                @pl.when(k == 0)
                def _():
                    copies = [
                        pltpu.make_async_copy(
                            xb.at[0, 1, pl.ds(h * hb, hb), :], cot_all.at[0, span(h, 0), :], load_sem.at[0, 1, h]
                        )
                        for h in range(2)
                    ]
                    for c in copies:
                        c.start()
                    for c in copies:
                        c.wait()

            return 0

        lax.fori_loop(0, ways, block, 0)
        for slot in range(2):
            for c in outputs(slot, s, order[ways - 2 + slot], True, units_of):
                c.wait()

    def rerun(first, count, units_of):
        per = ways // 2

        def copies(k):
            s, p, slot = k // per, 2 * (k % per), k % 2
            return [
                pltpu.make_async_copy(
                    x.at[s, span(h, p, 2), :], xb.at[slot, a, pl.ds(2 * h * hb, 2 * hb), :], load_sem.at[slot, a, h]
                )
                for a, x in enumerate((normed_all, cot_all))
                for h in range(2)
            ]

        def stores(k):
            return outputs(k % 2, k // per, 2 * (k % per), False, units_of, 2)

        for c in copies(first):
            c.start()

        def block(k, _):
            slot = k % 2
            for c in copies(k):
                c.wait()

            @pl.when(k + 1 < first + count)
            def _():
                for c in copies(k + 1):
                    c.start()

            @pl.when(k >= first + 2)
            def _():
                for c in stores(k):
                    c.wait()

            for r in units_of:
                mlp_rows(slot, xb[slot, 0], xb[slot, 1], r, 4 * hb)
            for c in stores(k):
                c.start()
            return 0

        lax.fori_loop(first, first + count, block, 0)
        for k in range(first + count - 2, first + count):
            for c in stores(k):
                c.wait()

    vector_step(spread_bits + 1)
    relay(0, 1)

    for b in range(spread_bits + 2, len(partners)):
        vector_step(b)
    vectors_out[...] = vec[len(partners)]
    gain = lambda: vec[len(partners), 0:1, :]
    shift = lambda: vec[len(partners), 1:2, :]
    for k in range(1, half):
        bias_copy(k).wait_recv()
    bias = biases[...]
    for k in range(1, half):
        bias = bias + bias_in[k - 1]
    own_weights(attention_part + mlp_part)
    far_weights(attention_part)
    b1_out[...] = jnp.zeros_like(b1_out)

    def rows_of_own(n):
        p = order[n]
        if p >= ways // 2:
            for a in range(2):
                for h in range(2):
                    arrived(0, a, h, p)
        elif p >= 2:
            relay(0, p)
        if p == ways // 2 - 1:
            far(0, "wait_recv")
            for h in range(2):
                forward(1, 0, h, 0)

    run(0, (), rows_of_own)

    def hook(i, count):
        @pl.when(i == count // 2)
        def _():
            far(1, "wait_recv")
            for h in range(2):
                forward(1, 1, h, 0)

        @pl.when(i == count - 1)
        def _():
            relay(1, 1, (0,))

    bias_out[...] = jnp.zeros_like(bias_out)
    length = 2 * ways * hb
    block_rows = min(512, length)
    chunks = [pl.multiple_of((2 * at.device_of(h, p) + h) * hb, hb) for h in range(2) for p in range(ways)]
    pl.run_scoped(
        lambda *scratch: attention_core(
            heads, head_dim, block_rows, chunks, 0, qkv_all, g_all, cos_ref, neg_ref, pos_ref,
            o_out, dqkv_out, bias_out, hook, *scratch,
        ),
        *attention_scratch(heads, length, part, block_rows, len(chunks)),
    )
    rerun(0, ways // 2, (0,))
    relay(1, 1, (1,))

    def rows_of_partner(n):
        p = order[n]
        if p >= ways // 2:
            for a in range(2):
                for h in range(2):
                    arrived(1, a, h, p)
        elif p >= 2:
            relay(1, p)

    run(1, (0,), rows_of_partner)
    far_weights(mlp_part)
    weights_out = [pltpu.make_async_copy(x, y, w_out_sem.at[n]) for n, (x, y) in enumerate(((wg, wg_out), (wo, wo_out)))]
    for c in weights_out:
        c.start()
    rerun(0, ways, tuple(range(1, half)))
    for c in weights_out:
        c.wait()
    for k, n in weight_copies:
        weight_copy(k, n).wait_send()
    for k in range(1, half):
        bias_copy(k).wait_send()
    for b in range(len(partners)):
        vector_copy(b).wait_send()

    for a in range(2):
        far(a, "wait_send")
    for a in range(2):
        for h in range(2):
            for s in range(2):
                for p in range(ways):
                    for t in range(p.bit_length(), steps):
                        row_copy(s, a, h, p, t).wait_send()


def front(ways, spread, heads, head_dim, tok, cot, qkv_w, w1, dense_w, w2, vectors, biases, tables):
    rows, width = tok.shape
    half = spread // 2
    length = rows * ways
    part, units = dense_w.shape[0] * half, w2.shape[0] * half
    arrays = 1 if w2.shape[0] % 128 == 0 else half
    hops = (spread * ways).bit_length() - 1
    hbm = pl.BlockSpec(memory_space=pl.ANY)
    vmem = pl.BlockSpec(memory_space=pltpu.VMEM)
    shape = jax.ShapeDtypeStruct
    dma = pltpu.SemaphoreType.DMA
    return pl.pallas_call(
        functools.partial(front_kernel, ways, spread, heads, head_dim),
        out_shape=(
            shape((2, length, width), BF16),
            shape((2, length, width), BF16),
            shape((2, length, width), BF16),
            shape((3, 2, length, part), F32),
            shape((2, length, part), BF16),
            shape((3 * part + units, width), BF16),
            shape((part + units, width), BF16),
            shape((1, length, part), BF16),
            shape((3, 1, length, part), BF16),
            shape((half, units // half), F32),
            shape(vectors.shape, F32),
            shape((3, part), F32),
        )
        + (shape((2, length, units // arrays), BF16),) * (2 * arrays),
        in_specs=[hbm] * 6 + [vmem] * 5,
        out_specs=(hbm,) * 9 + (vmem,) * 3 + (hbm,) * (2 * arrays),
        scratch_shapes=[
            pltpu.VMEM((3 * part + units, width), BF16),
            pltpu.VMEM((part + units, width), BF16),
            pltpu.VMEM((2, 2, 2 * rows, width), BF16),
            pltpu.VMEM((2, rows, width), BF16),
            pltpu.VMEM((2, 3, rows, part), F32),
            pltpu.VMEM((2, rows, part), BF16),
            pltpu.VMEM((2, 2, half, 2 * rows, units // half), BF16),
            pltpu.VMEM((hops + 1,) + vectors.shape, F32),
            pltpu.VMEM((hops,) + vectors.shape, F32),
            pltpu.VMEM((max(half - 1, 1),) + biases.shape, F32),
            dma((2, 2, 2, ways)),
            dma((2, 2, 2, ways)),
            dma((2, 2)),
            dma((2, 2)),
            dma((max(half - 1, 1), 6)),
            dma((max(half - 1, 1), 6)),
            dma((6,)),
            dma((2, 2, 2)),
            dma((2, 2, 3 + 2 * half)),
            dma((2,)),
            dma((hops,)),
            dma((hops,)),
            dma((max(half - 1, 1),)),
            dma((max(half - 1, 1),)),
        ],
        compiler_params=pltpu.CompilerParams(collective_id=1, has_side_effects=True, vmem_limit_bytes=60 << 20),
        name="front",
    )(tok, cot, qkv_w, w1, dense_w, w2, vectors, biases, *tables)


def attention_core(
    heads, head_dim, block, chunks, seq, qkv_in, g_in, cos_ref, neg_ref, pos_ref, o_out, dqkv_out, bias_out,
    hook, stage, q, k, v, g, kt, vt, gt, dk, dv, dq, o, scores, in_sem, out_sem,
):
    length, width = q.shape
    half = ROT // 2
    scale = head_dim ** (-0.5)
    count = length // block
    chunk = length // len(chunks)
    loads = []
    for r, start in enumerate(chunks):
        rows, here = pl.ds(start, chunk), pl.ds(r * chunk, chunk)
        loads.append(pltpu.make_async_copy(qkv_in.at[:, seq, here, :], stage.at[:, rows, :], in_sem.at[r, 0]))
        loads.append(pltpu.make_async_copy(g_in.at[seq, here, :], g.at[rows, :], in_sem.at[r, 1]))
    for c in loads:
        c.start()
    for c in loads:
        c.wait()

    def prepare(at, _):
        rows = aligned(at * block, block)
        cos, neg, pos = cos_ref[rows, :], neg_ref[rows, :], pos_ref[rows, :]

        def rotate(x):
            return x * cos + pltpu.roll(x, width - half, 1) * neg + pltpu.roll(x, half, 1) * pos

        q[rows, :] = rotate(stage[0, rows, :]).astype(BF16) * scale
        kb = rotate(stage[1, rows, :]).astype(BF16)
        vb = stage[2, rows, :].astype(BF16)
        k[rows, :] = kb
        v[rows, :] = vb
        kt[:, rows] = kb.T
        vt[:, rows] = vb.T
        gt[:, rows] = g[rows, :].T
        dk[rows, :] = jnp.zeros((block, width), F32)
        dv[rows, :] = jnp.zeros((block, width), F32)
        return 0

    lax.fori_loop(0, count, prepare, 0)
    lane = lax.broadcasted_iota(jnp.int32, (block, width), 1)

    def only(x, h):
        if heads == 1:
            return x
        keep = (lane >= h * head_dim) & (lane < (h + 1) * head_dim)
        return jnp.where(keep, x.astype(F32), 0.0).astype(BF16)

    def one_block(i, _):
        hook(i, count)
        mine = aligned(i * block, block)
        qi, gi = q[mine, :], g[mine, :]
        qh, gh = [only(qi, h) for h in range(heads)], [only(gi, h) for h in range(heads)]
        row = lax.broadcasted_iota(jnp.int32, (width, block), 0)
        every = range(heads)

        def first(j, tops):
            cols = aligned(j * block, block)
            s = [dot_nt(k[cols, :], qh[h]) for h in every]
            for h in every:
                scores[h, cols, :] = s[h]
            return tuple(jnp.maximum(tops[h], jnp.max(s[h], 0, keepdims=True)) for h in every)

        tops = lax.fori_loop(0, i, first, tuple(jnp.full((1, block), -1e30, F32) for h in every))
        key_at = lax.broadcasted_iota(jnp.int32, (block, block), 0)
        query_at = lax.broadcasted_iota(jnp.int32, (block, block), 1)
        last = [jnp.where(key_at <= query_at, dot_nt(k[mine, :], qh[h]), -1e30) for h in every]
        for h in every:
            scores[h, mine, :] = last[h]
        tops = [jnp.maximum(tops[h], jnp.max(last[h], 0, keepdims=True)) for h in every]

        def second(j, carry):
            totals, accs = carry
            cols = aligned(j * block, block)
            e = [jnp.exp(scores[h, cols, :] - tops[h]) for h in every]
            for h in every:
                scores[h, cols, :] = e[h]
            return (
                tuple(totals[h] + jnp.sum(e[h], 0, keepdims=True) for h in every),
                tuple(accs[h] + dot_nn(vt[:, cols], e[h].astype(BF16)) for h in every),
            )

        nothing = tuple(jnp.zeros((width, block), F32) for h in every)
        totals, accs = lax.fori_loop(
            0, i + 1, second, (tuple(jnp.zeros((1, block), F32) for h in every), nothing)
        )
        inv = [1.0 / totals[h] for h in every]
        here = [(row >= h * head_dim) & (row < (h + 1) * head_dim) for h in every]
        accs = [jnp.where(here[h], (accs[h] * inv[h]).astype(BF16).astype(F32), 0.0) for h in every]
        gti = gt[:, mine].astype(F32)
        delta = [jnp.sum(accs[h] * gti, 0, keepdims=True) for h in every]
        ob = functools.reduce(jnp.add, accs)

        def third(j, acc_q):
            cols = aligned(j * block, block)
            p = [scores[h, cols, :] * inv[h] for h in every]
            dp = [dot_nt(v[cols, :], gh[h]) for h in every]
            dv[cols, :] += functools.reduce(jnp.add, [dot_nn(p[h].astype(BF16), gh[h]) for h in every])
            ds = [(p[h] * (dp[h] - delta[h])).astype(BF16) for h in every]
            dk[cols, :] += functools.reduce(jnp.add, [dot_nn(ds[h], qh[h]) for h in every])
            return tuple(acc_q[h] + dot_nn(kt[:, cols], ds[h]) for h in every)

        acc_q = lax.fori_loop(0, i + 1, third, nothing)
        dqb = functools.reduce(jnp.add, [jnp.where(here[h], acc_q[h], 0.0) for h in every])
        o[mine, :] = ob.T.astype(BF16)
        dq[mine, :] = dqb.T * scale
        return 0

    lax.fori_loop(0, count, one_block, 0)

    def finish(at, sums):
        rows = aligned(at * block, block)
        cos, neg, pos = cos_ref[rows, :], neg_ref[rows, :], pos_ref[rows, :]

        def unrotate(x):
            return x * cos - pltpu.roll(x, width - half, 1) * neg - pltpu.roll(x, half, 1) * pos

        a = unrotate(dq[rows, :].astype(BF16).astype(F32))
        b = unrotate(dk[rows, :].astype(BF16).astype(F32))
        c = dv[rows, :].astype(BF16).astype(F32)
        q[rows, :] = a.astype(BF16)
        k[rows, :] = b.astype(BF16)
        v[rows, :] = c.astype(BF16)
        return tuple(s + jnp.sum(x, 0, keepdims=True) for s, x in zip(sums, (a, b, c)))

    sums = lax.fori_loop(0, count, finish, tuple(jnp.zeros((1, width), F32) for _ in range(3)))
    bias_out[...] += jnp.concatenate(list(sums), 0)
    stores = []
    for r, start in enumerate(chunks):
        rows, here = pl.ds(start, chunk), pl.ds(r * chunk, chunk)
        for n, src in enumerate((q, k, v)):
            stores.append(pltpu.make_async_copy(src.at[rows, :], dqkv_out.at[n, 0, here, :], out_sem.at[r, n]))
        stores.append(pltpu.make_async_copy(o.at[rows, :], o_out.at[0, here, :], out_sem.at[r, 3]))
    for c in stores:
        c.start()
    for c in stores:
        c.wait()


def attention_scratch(heads, length, part, block, chunks):
    return (
        [pltpu.VMEM((3, length, part), F32)]
        + [pltpu.VMEM((length, part), BF16)] * 4
        + [pltpu.VMEM((part, length), BF16)] * 3
        + [pltpu.VMEM((length, part), F32)] * 3
        + [
            pltpu.VMEM((length, part), BF16),
            pltpu.VMEM((heads, length, block), F32),
            pltpu.SemaphoreType.DMA((chunks, 2)),
            pltpu.SemaphoreType.DMA((chunks, 4)),
        ]
    )


def joined(xs, w):
    if all(x.shape[1] % 128 == 0 for x in xs):
        return dot_nn(jnp.concatenate(xs, 1), w[...])
    total, at = None, 0
    for x in xs:
        y = dot_nn(x, w[at : at + x.shape[1], :])
        total, at = (y if total is None else total + y), at + x.shape[1]
    return total


def rest_kernel(
    ways, spread, heads, head_dim,
    qkv_all, g_all, normed_all, cot_all, wg_in, wo_in, o_0, dqkv_0, tok_own, cot_own, cos_ref, neg_ref, pos_ref, norm_ref, *more,
):
    at = Layout(ways, spread)
    half, steps, orders = at.half, at.steps, at.orders
    arrays = (len(more) - 32) // 2
    acts, pres = more[:arrays], more[arrays : 2 * arrays]
    (
        o_1, dqkv_1, recv, far_sum, dw_own, dw_recv, dw_low, out_rows, grad_rows, bias_out, vec_out,
        wg, wo, keep, stage_send, stage_recv, ob, db, apb, vec, vec_in,
        w_sem, load_sem, rs_send, rs_recv, add_sem, far_send, far_recv, dw_send, dw_come, vec_send, vec_recv,
    ) = more[2 * arrays :]
    hb = keep.shape[4]
    length = 2 * ways * hb
    part = g_all.shape[2]
    shard = part // half
    block = min(512, length)
    width = keep.shape[5]
    at.meet()
    loads = [pltpu.make_async_copy(x, y, w_sem.at[n]) for n, (x, y) in enumerate(((wg_in, wg), (wo_in, wo)))]
    for c in loads:
        c.start()
    bias_out[...] = jnp.zeros_like(bias_out)
    chunks = [
        pl.multiple_of((2 * at.device_of(h, p) + h) * hb, hb) for h in range(2) for p in range(ways)
    ]

    def span(h, p):
        return aligned((h * ways + p) * hb, hb)

    def from_heads(s, pick, o_dst, dqkv_dst, o_sem, dqkv_sem):
        for v, (x, y) in enumerate(((o_0, dqkv_0), (o_1, dqkv_1))):
            @pl.when(s == v)
            def _():
                pltpu.make_async_copy(x.at[0, pick, :], o_dst, o_sem).start()
                pltpu.make_async_copy(y.at[:, 0, pick, :], dqkv_dst, dqkv_sem).start()

    def heads_there(pick, o_dst, dqkv_dst, o_sem, dqkv_sem):
        pltpu.make_async_copy(o_1.at[0, pick, :], o_dst, o_sem).wait()
        pltpu.make_async_copy(dqkv_1.at[:, 0, pick, :], dqkv_dst, dqkv_sem).wait()

    def sent(s, t, h, q, src):
        level = q.bit_length() - 1 if isinstance(q, int) else steps - 1
        return remote(src, recv.at[s, t, h, q], rs_send.at[s, t, h, q], rs_recv.at[s, t, h, q], at.near(orders[h][level]))

    def partial_sums(s):
        def place(i):
            return jnp.where(i < ways // 2, ways // 2 + i, ways - 1 - i)

        def heads_of(i, h):
            slot, rows = i % 2, pl.ds(h * hb, hb)
            return (
                span(h, place(i)), ob.at[slot, rows, :], db.at[slot, :, rows, :],
                load_sem.at[slot, h, 0], load_sem.at[slot, h, 1],
            )

        def act_copies(i, h):
            slot, rows = i % 2, pl.ds(h * hb, hb)
            return [
                pltpu.make_async_copy(
                    shard_of(x, r, s, span(h, place(i))), apb.at[slot, n, r, rows, :], load_sem.at[slot, h, 2 + n * half + r]
                )
                for n, x in enumerate((acts, pres))
                for r in range(half)
            ]

        def fetch(i):
            for h in range(2):
                from_heads(s, *heads_of(i, h))
                for c in act_copies(i, h):
                    c.start()

        def sends(i):
            return [sent(s, t, h, place(i), stage_send.at[i % 2, t, h]) for t in range(2) for h in range(2)]

        fetch(0)

        def one(i, _):
            slot = i % 2
            for h in range(2):
                heads_there(*heads_of(i, h))
                for c in act_copies(i, h):
                    c.wait()

            @pl.when(i + 1 < ways)
            def _():
                fetch(i + 1)

            @pl.when((i == 1) & (s == 0))
            def _():
                for q in range(ways // 2 - 1, ways // 4, -1):
                    serve(1, q, 0)
                send_held(1, 1)

            @pl.when((i >= 2) & (i < ways // 2 + 2))
            def _():
                for c in sends(i - 2):
                    c.wait_send()

            out = joined([ob[slot]] + [apb[slot, 0, r] for r in range(half)], wo).astype(BF16)
            grad = joined([db[slot, n] for n in range(3)] + [apb[slot, 1, r] for r in range(half)], wg).astype(BF16)

            @pl.when(i < ways // 2)
            def _():
                for t, x in enumerate((grad, out)):
                    for h in range(2):
                        stage_send[slot, t, h] = x[h * hb : (h + 1) * hb, :]
                for c in sends(i):
                    c.start()

            @pl.when(i >= ways // 2)
            def _():
                for t, x in enumerate((grad, out)):
                    for h in range(2):
                        keep[s, t, h, ways - 1 - i] = x[h * hb : (h + 1) * hb, :]

            for n in range(ways // 2):
                @pl.when(i == ways // 2 + n)
                def _():
                    serve_both(s, ways - 1 - n)

            return 0

        lax.fori_loop(0, ways, one, 0)

    def far_copy(t, h):
        return remote(keep.at[1, t, h, 0], far_sum.at[t, h], far_send.at[t, h], far_recv.at[t, h], at.far)

    def serve(s, q, t):
        level = q.bit_length() - 1
        p = q - (1 << level)
        come = [pltpu.make_async_copy(recv.at[s, t, h, q], stage_recv.at[t, h], add_sem.at[t, h]) for h in range(2)]
        for h, c in enumerate(come):
            sent(s, t, h, q, stage_recv.at[t, h]).wait_recv()
            c.start()
        for h, c in enumerate(come):
            c.wait()
            keep[s, t, h, p] = (keep[s, t, h, p].astype(F32) + stage_recv[t, h].astype(F32)).astype(BF16)
            if p and p.bit_length() == level:
                if level == steps - 1:
                    @pl.when((s == 1) & (t == 0))
                    def _():
                        sent(s, t, h, p, keep.at[s, t, h, p]).start()
                else:
                    sent(s, t, h, p, keep.at[s, t, h, p]).start()
            if q == 1 and s == 1:
                far_copy(t, h).start()

    def serve_both(s, q):
        def body(t, _):
            serve(s, q, t)
            return 0

        lax.fori_loop(0, 2, body, 0)

    def send_held(s, t):
        for p in range(ways // 2 - 1, ways // 4 - 1, -1):
            for h in range(2):
                sent(s, t, h, p, keep.at[s, t, h, p]).start()

    def shard_copy(k):
        cut = aligned(at.peer_at[k - 1] * shard, shard)
        return remote(dw_low.at[:, cut, :], dw_recv.at[k - 1], dw_send.at[k - 1], dw_come.at[k - 1], at.peers[k - 1])

    def weight_sums(hook):
        rows = min(512, length)
        per = length // rows

        def body(nbuf, cbuf, abuf, acc, rounded, sems, out_sem):
            def heads_of(i):
                slot = i % 2
                return aligned((i % per) * rows, rows), abuf.at[slot, 3], abuf.at[slot, 0:3], sems.at[slot, 3], sems.at[slot, 2]

            def copies(i):
                slot, s, here = i % 2, i // per, aligned((i % per) * rows, rows)
                return [
                    pltpu.make_async_copy(normed_all.at[s, here, :], nbuf.at[slot], sems.at[slot, 0]),
                    pltpu.make_async_copy(cot_all.at[s, here, :], cbuf.at[slot], sems.at[slot, 1]),
                ]

            def fetch(i):
                for c in copies(i):
                    c.start()
                from_heads(i // per, *heads_of(i))

            fetch(0)
            acc[...] = jnp.zeros_like(acc)

            def one(i, _):
                slot = i % 2
                for c in copies(i):
                    c.wait()
                heads_there(*heads_of(i))

                @pl.when(i + 1 < 2 * per)
                def _():
                    fetch(i + 1)

                hook(i, 2 * per)
                normed = nbuf[slot]
                if part % 128 == 0:
                    y = dot_tn(jnp.concatenate([abuf[slot, n] for n in range(3)], 1), normed)
                    for n in range(3):
                        acc[n] += y[n * part : (n + 1) * part, :]
                else:
                    for n in range(3):
                        acc[n] += dot_tn(abuf[slot, n], normed)
                acc[3] += dot_tn(abuf[slot, 3], cbuf[slot])
                return 0

            lax.fori_loop(0, 2 * per, one, 0)
            own = pltpu.make_async_copy(acc.at[:, aligned(at.g * shard, shard), :], dw_own, out_sem.at[0])
            own.start()
            rounded[...] = acc[...].astype(BF16)
            others = pltpu.make_async_copy(rounded, dw_low, out_sem.at[1])
            others.start()
            others.wait()
            own.wait()

        width_of = pltpu.VMEM((2, rows, width), BF16)
        pl.run_scoped(
            body, width_of, width_of, pltpu.VMEM((2, 4, rows, part), BF16),
            pltpu.VMEM((4, part, width), F32), pltpu.VMEM((4, part, width), BF16),
            pltpu.SemaphoreType.DMA((2, 4)), pltpu.SemaphoreType.DMA((2,)),
        )
        for k in range(1, half):
            shard_copy(k).start()

    pl.run_scoped(
        lambda *scratch: attention_core(
            heads, head_dim, block, chunks, 1, qkv_all, g_all, cos_ref, neg_ref, pos_ref,
            o_1, dqkv_1, bias_out, lambda i, count: None, *scratch,
        ),
        *attention_scratch(heads, length, part, block, len(chunks)),
    )
    for c in loads:
        c.wait()

    def one_sequence(turn, _):
        partial_sums(1 - turn)
        return 0

    lax.fori_loop(0, 2, one_sequence, 0)

    for q in range(ways // 4, 0, -1):
        serve(1, q, 0)
    for q in range(ways // 2 - 1, ways // 4, -1):
        serve(1, q, 1)
    for t in range(2):
        send_held(0, t)

    def output_rows_back(i, count):
        @pl.when(i == count // 2)
        def _():
            for q in range(ways // 4, 1, -1):
                serve(1, q, 1)

        @pl.when(i == count - 1)
        def _():
            serve(1, 1, 1)

    weight_sums(output_rows_back)
    for q in range(ways // 2 - 1, 0, -1):
        serve_both(0, q)
    for k in range(1, half):
        shard_copy(k).wait()
    for t in range(2):
        for h in range(2):
            far_copy(t, h).wait()
    partners = [{"fsdp": flip(at.f, 1 << b)} for b in range(spread.bit_length() - 1)] + [at.near(b) for b in range(steps)]

    def vector_copy(b):
        return remote(vec.at[b], vec_in.at[b], vec_send.at[b], vec_recv.at[b], partners[b])

    def norm_backward(far, tok, cot, out_buf, grad_buf, sems):
        loads = [
            pltpu.make_async_copy(far_sum, far, sems.at[0]),
            pltpu.make_async_copy(tok_own, tok, sems.at[1]),
            pltpu.make_async_copy(cot_own, cot, sems.at[2]),
        ]
        for c in loads:
            c.start()
        for c in loads:
            c.wait()
        gain = norm_ref[0:1, :]
        biases = norm_ref[2:3, :] + norm_ref[3:4, :]
        sums = [jnp.zeros((1, width), F32)] * 3
        for h in range(2):
            rows = slice(h * hb, (h + 1) * hb)
            x, c = tok[rows, :].astype(F32), cot[rows, :].astype(F32)
            xhat, inv = normalize(x)
            grad = keep[0, 0, h, 0].astype(F32) + far[0, h].astype(F32)
            out_buf[rows, :] = (x + keep[0, 1, h, 0].astype(F32) + far[1, h].astype(F32) + biases).astype(BF16)
            scaled = grad * gain
            inner = inv * (
                scaled
                - jnp.mean(scaled, -1, keepdims=True)
                - xhat * jnp.mean(scaled * xhat, -1, keepdims=True)
            )
            grad_buf[rows, :] = (c + inner).astype(BF16)
            sums = [a + jnp.sum(b, 0, keepdims=True) for a, b in zip(sums, (grad * xhat, grad, c))]
        eighth = width // 8
        vec[0] = jnp.concatenate(
            [jnp.concatenate([x[:, n * eighth : (n + 1) * eighth] for n in range(8)], 0) for x in sums], 1
        )
        vector_copy(0).start()
        stores = [
            pltpu.make_async_copy(out_buf, out_rows, sems.at[0]), pltpu.make_async_copy(grad_buf, grad_rows, sems.at[1])
        ]
        for c in stores:
            c.start()
        for b in range(len(partners)):
            vector_copy(b).wait_recv()
            vec[b + 1] = vec[b] + vec_in[b]
            if b + 1 < len(partners):
                vector_copy(b + 1).start()
        vec_out[...] = vec[len(partners)]
        for c in stores:
            c.wait()

    buf = pltpu.VMEM((2 * hb, width), BF16)
    pl.run_scoped(norm_backward, pltpu.VMEM((2, 2, hb, width), BF16), buf, buf, buf, buf, pltpu.SemaphoreType.DMA((3,)))
    for b in range(len(partners)):
        vector_copy(b).wait_send()
    for t in range(2):
        for h in range(2):
            for s in range(2):
                for p in range(1, ways // 2):
                    sent(s, t, h, p, keep.at[s, t, h, p]).wait_send()


def rest(ways, spread, heads, head_dim, qkv_all, g_all, normed_all, cot_all, wg, wo, o_0, dqkv_0, tok, cot, tables, norm, acts, pres):
    _, length, width = normed_all.shape
    half = spread // 2
    part, hidden = g_all.shape[2], sum(x.shape[2] for x in acts) // half
    hb = length // ways // 2
    shard = part // half
    rows = 2 * hb
    hops = (spread * ways).bit_length() - 1
    hbm = pl.BlockSpec(memory_space=pl.ANY)
    vmem = pl.BlockSpec(memory_space=pltpu.VMEM)
    shape = jax.ShapeDtypeStruct
    dma = pltpu.SemaphoreType.DMA
    return pl.pallas_call(
        functools.partial(rest_kernel, ways, spread, heads, head_dim),
        out_shape=(
            shape((1, length, part), BF16),
            shape((3, 1, length, part), BF16),
            shape((2, 2, 2, ways, hb, width), BF16),
            shape((2, 2, hb, width), BF16),
            shape((4, shard, width), F32),
            shape((max(half - 1, 1), 4, shard, width), BF16),
            shape((4, part, width), BF16),
            shape((rows, width), BF16),
            shape((rows, width), BF16),
            shape((3, part), F32),
            shape((8, 3 * width // 8), F32),
        ),
        in_specs=[hbm] * 10 + [vmem] * 4 + [hbm] * (2 * len(acts)),
        out_specs=(hbm,) * 9 + (vmem,) * 2,
        scratch_shapes=[
            pltpu.VMEM(wg.shape, BF16),
            pltpu.VMEM(wo.shape, BF16),
            pltpu.VMEM((2, 2, 2, ways // 2, hb, width), BF16),
            pltpu.VMEM((2, 2, 2, hb, width), BF16),
            pltpu.VMEM((2, 2, hb, width), BF16),
            pltpu.VMEM((2, rows, part), BF16),
            pltpu.VMEM((2, 3, rows, part), BF16),
            pltpu.VMEM((2, 2, half, rows, hidden), BF16),
            pltpu.VMEM((hops + 1, 8, 3 * width // 8), F32),
            pltpu.VMEM((hops, 8, 3 * width // 8), F32),
            dma((2,)),
            dma((2, 2, 2 + 2 * half)),
            dma((2, 2, 2, ways)),
            dma((2, 2, 2, ways)),
            dma((2, 2)),
            dma((2, 2)),
            dma((2, 2)),
            dma((max(half - 1, 1),)),
            dma((max(half - 1, 1),)),
            dma((hops,)),
            dma((hops,)),
        ],
        compiler_params=pltpu.CompilerParams(collective_id=2, has_side_effects=True, vmem_limit_bytes=63 << 20),
        name="rest",
    )(qkv_all, g_all, normed_all, cot_all, wg, wo, o_0, dqkv_0, tok, cot, *tables, norm, *acts, *pres)


def normalize(rows):
    mean = jnp.mean(rows, -1, keepdims=True)
    centred = rows - mean
    inv = lax.rsqrt(jnp.mean(centred * centred, -1, keepdims=True) + EPSILON)
    return centred * inv, inv


def local(
    tokens, layer_norm_gain, layer_norm_bias, qkv_weight, qkv_bias, dense_weight, dense_bias,
    fc1_weight, fc1_bias, fc2_weight, fc2_bias, cotangent,
):
    shape = tokens.shape
    rows, width = shape[0] * shape[1], shape[2]
    head_dim = width // HEADS
    ways = lax.axis_size("seq")
    spread = lax.axis_size("fsdp")
    half = spread // 2
    length = rows * ways
    heads = HEADS // (2 * ways)
    shard, hidden = dense_weight.shape[0], fc2_weight.shape[0]
    part, units = shard * half, hidden * half
    me, f = lax.axis_index("seq"), lax.axis_index("fsdp")
    group = lax.rem(f, half)

    mine = jnp.stack([layer_norm_gain, layer_norm_bias, dense_bias, fc2_bias]).astype(F32)
    vectors = lax.dynamic_update_slice(jnp.zeros((8, width), F32), mine, (0, (me * spread + f) * mine.shape[1]))
    biases = jnp.zeros((8, max(part, units)), F32)
    biases = lax.dynamic_update_slice(biases, qkv_bias.astype(F32), (0, group * shard))
    biases = lax.dynamic_update_slice(biases, fc1_bias.astype(F32)[None], (3, 0))
    tok, cot = tokens.reshape(rows, width), cotangent.reshape(rows, width)
    tables = rotation_tables(length, head_dim, heads)
    _, cot_all, normed_all, qkv_all, g_all, wg, wo, o_0, dqkv_0, b1_sum, small, bias_0, *hidden_rows = front(
        ways, spread, heads, head_dim, tok, cot, qkv_weight.transpose(1, 2, 0), fc1_weight.transpose(1, 0), dense_weight,
        fc2_weight, vectors, biases, tables,
    )

    def to_peer(x, k):
        pairs = [(i, i - i % half + (i % half + k) % half) for i in range(spread)]
        return lax.ppermute(x, "fsdp", pairs)

    def cut(x, at, size, axis):
        return lax.dynamic_slice_in_dim(x, at * size, size, axis)

    arrays = len(hidden_rows) // 2
    acts, pres = hidden_rows[:arrays], hidden_rows[arrays:]
    flat = lambda x: x.reshape(2 * length, x.shape[-1])
    shard_at = lambda sums, r, axis: (
        sums[r] if len(sums) > 1 else lax.slice_in_dim(sums[0], r * hidden, (r + 1) * hidden, axis=axis)
    )
    fc1_sums = [dot_tn(flat(x), flat(normed_all)) for x in pres]
    fc2_sums = [dot_tn(flat(x), flat(cot_all)) for x in acts]
    peers = [(k, lax.rem(group + k, half)) for k in range(1, half)]
    fc1_out = [shard_at(fc1_sums, k, 0).astype(BF16) for k in range(1, half)]
    fc2_out = [shard_at(fc2_sums, k, 0).astype(BF16) for k in range(1, half)]
    fc1_in = [to_peer(x, k) for (k, _), x in zip(peers, fc1_out)]
    fc2_in = [to_peer(x, k) for (k, _), x in zip(peers, fc2_out)]
    b1_in = [to_peer(b1_sum[k].astype(BF16), k) for k, _ in peers]
    g_all, fc1_out, fc2_out, fc1_sums, fc2_sums = lax.optimization_barrier((g_all, fc1_out, fc2_out, fc1_sums, fc2_sums))
    _, _, _, _, dw_own, dw_in, _, output, tokens_grad, bias_1, sums = rest(
        ways, spread, heads, head_dim, qkv_all, g_all, normed_all, cot_all, wg, wo, o_0, dqkv_0, tok, cot, tables, small,
        acts, pres,
    )
    qkv_b_sum = bias_0 + bias_1
    total = lambda own, come: functools.reduce(lambda a, b: a + b.astype(F32), come, own)
    fc1_w_grad, fc2_w_grad = total(shard_at(fc1_sums, 0, 0), fc1_in), total(shard_at(fc2_sums, 0, 0), fc2_in)
    fc1_w_grad = fc1_w_grad.transpose(1, 0)
    fc1_b_grad = total(b1_sum[0], b1_in)
    b_in = [to_peer(cut(qkv_b_sum, p, shard, 1).astype(BF16), k) for k, p in peers]
    qkv_b_grad = total(cut(qkv_b_sum, group, shard, 1), b_in)
    dw = total(dw_own, [dw_in[k] for k in range(half - 1)])
    qkv_w_grad, dense_w_grad = dw[:3].transpose(2, 0, 1), dw[3]

    piece, eighth = width // (ways * spread), width // 8
    first = (me * spread + f) * piece
    sums = lax.dynamic_slice(
        sums.reshape(8, 3, eighth), (first // eighth, 0, lax.rem(first, eighth)), (1, 3, piece)
    )[0]
    output, tokens_grad = output.reshape(shape), tokens_grad.reshape(shape)
    return (
        output, tokens_grad, sums[0], sums[1], qkv_w_grad, qkv_b_grad, dense_w_grad, sums[2],
        fc1_w_grad, fc1_b_grad, fc2_w_grad, sums[2],
    )


def solution(mesh):
    both = ("seq", "fsdp")
    rows = P("fsdp", "seq", None)
    return jax.shard_map(
        local,
        mesh=mesh,
        in_specs=(
            rows, P(both), P(both), P(None, None, both), P(None, both), P(both, None), P(both),
            P(None, both), P(both), P(both, None), P(both), rows,
        ),
        out_specs=(
            rows, rows, P(both), P(both), P(None, None, both), P(None, both), P(both, None), P(both),
            P(None, both), P(both), P(both, None), P(both),
        ),
        check_vma=False,
    )
```
